512 devices in a mesh: row: 16 (over y_hi, x, core), col: 32 (over z, y_lo).
Axes of the slice: x: 4, y: 4 (y_hi: 2, y_lo: 2; y = y_hi * 2 + y_lo), z: 16, core: 2. Of those that a mesh axis runs over, the one named last changes fastest.
Arguments:
- specimen: float32 [2, 2048, 8192], P(None, 'row', 'col'), may hold values from -6 to 6
- probe_field: float32 [2, 256, 256], replicated, may hold values from -6 to 6
- scan_offsets: int32 [16, 32, 2, 2], replicated, may hold values from -128 to 128, as said below
- live_counts: int32 [16, 32], replicated, may hold values from 1 to 2, as said below
- magnitudes: float32 [16, 32, 2, 256, 256], P('row', 'col'), may hold values from 0 to 2
Outputs:
- specimen_next: float32 [2, 2048, 8192], P(None, 'row', 'col')
- probe_next: float32 [2, 256, 256], replicated
The draws below stay inside these ranges and needn't reach their ends.
Inputs may be any that keep to these rules, and one draw needn't show every extreme that they name: `scan_offsets`: rows of a patch start within -128 to 0 of the tile's first row, columns within -128 to 128 of its first column. Tile (a, b) owns the positions in its first live_counts[a, b] slots.
All inputs are finite; a program needn't handle non-finite values.
Results may differ from the reference program's by a relative error of at most 0.0003.
Values sent between devices are 32-bit elements; how exact they have to be, the bound alone decides.
A program may use at most 64 MiB of HBM per device.

```python
import jax
import jax.numpy as jnp
from jax import lax

PROBE = 256
TILE_R = 128
TILE_C = 256
POS_DEV = 2
NY = 2048
NX = 8192


def draw_scan_offsets(key, part):
    grid_rows = NY // TILE_R
    grid_cols = NX // TILE_C
    half = PROBE // 2
    key_rows, key_cols, key_pick = jax.random.split(jax.random.fold_in(key, 11), 3)
    shape_here = (grid_rows, grid_cols, POS_DEV)
    row_offsets = jax.random.randint(key_rows, shape_here, -half, TILE_R - half + 1)
    col_offsets = jax.random.randint(key_cols, shape_here, -half, TILE_C - half + 1)
    entries = grid_rows * grid_cols * POS_DEV
    lowest = jax.random.randint(key_pick, (), 0, entries)
    highest = (lowest + 1) % entries
    flat_index = jnp.arange(entries, dtype=jnp.int32).reshape(shape_here)
    row_offsets = jnp.where(flat_index == lowest, -half, jnp.where(flat_index == highest, TILE_R - half, row_offsets))
    col_offsets = jnp.where(flat_index == lowest, -half, jnp.where(flat_index == highest, TILE_C - half, col_offsets))
    return jnp.stack([row_offsets, col_offsets], -1).astype(jnp.int32)


def draw_live_counts(key, part):
    grid_rows = NY // TILE_R
    grid_cols = NX // TILE_C
    key_counts, key_pick = jax.random.split(jax.random.fold_in(key, 23), 2)
    counts = jax.random.randint(key_counts, (grid_rows, grid_cols), 1, POS_DEV + 1)
    entries = grid_rows * grid_cols
    fullest = jax.random.randint(key_pick, (), 0, entries)
    emptiest = (fullest + 1) % entries
    flat_index = jnp.arange(entries, dtype=jnp.int32).reshape((grid_rows, grid_cols))
    counts = jnp.where(flat_index == fullest, POS_DEV, jnp.where(flat_index == emptiest, 1, counts))
    return counts.astype(jnp.int32)


def block_levels(stream_key, dims, cuts, smallest, largest):
    def one(axis_at, shards_of):
        steps = jax.random.uniform(jax.random.fold_in(jax.random.fold_in(stream_key, 6), axis_at), (shards_of,), jnp.float32, smallest / len(cuts), largest / len(cuts))
        return jnp.repeat(jnp.exp(steps), dims[axis_at] // shards_of).reshape((-1,) + (1,) * (len(dims) - axis_at - 1))

    factor_of = one(*cuts[0])
    for cut in cuts[1:]:
        factor_of = factor_of * one(*cut)
    return factor_of


def gaussian(own_key, dims, deviation, bound, cuts=(), kind=jnp.bfloat16):
    factor_of = block_levels(own_key, dims, cuts, -0.22, 0.18) if cuts else 1.0
    values = jax.random.normal(own_key, dims, jnp.float32) * deviation * factor_of
    return jnp.minimum(jnp.maximum(values, -bound), bound).astype(kind)


def setup_inputs(seed: int = 0) -> dict:
    key_list = jax.random.split(jax.random.key(seed), 6)
    specimen = gaussian(key_list[0], (2, NY, NX), 1.0, 6.0, ((1, 16), (2, 32)), jnp.float32)
    probe_field = gaussian(key_list[1], (2, PROBE, PROBE), 1.0, 6.0, (), jnp.float32)
    scan_offsets = draw_scan_offsets(jax.random.fold_in(key_list[5], 71), 0)
    live_counts = draw_live_counts(jax.random.fold_in(key_list[5], 71), 0)
    magnitudes = jnp.clip(2.0 * jax.random.uniform(key_list[4], (NY // TILE_R, NX // TILE_C, POS_DEV, PROBE, PROBE), jnp.float32) ** block_levels(key_list[4], (NY // TILE_R, NX // TILE_C, POS_DEV, PROBE, PROBE), ((0, 16), (1, 32)), -0.2, 0.2), 0.0, 2.0)
    return {"specimen": specimen, "probe_field": probe_field, "scan_offsets": scan_offsets, "live_counts": live_counts, "magnitudes": magnitudes}


modulus_floor = 0.25
object_damping = 0.1
probe_damping = 0.1

def transform(wave_real, wave_imag, inverse):
    field = lax.complex(wave_real, wave_imag)
    if inverse:
        result = jnp.fft.ifft2(field, norm='ortho')
    else:
        result = jnp.fft.fft2(field, norm='ortho')
    return (jnp.real(result), jnp.imag(result))

def reference(specimen, probe_field, scan_offsets, live_counts, magnitudes):
    half = PROBE // 2
    grid_rows = specimen.shape[1] // TILE_R
    grid_cols = specimen.shape[2] // TILE_C
    padded = jnp.pad(specimen, ((0, 0), (half, half), (half, half)))
    probe_real = probe_field[0]
    probe_imag = probe_field[1]
    power = probe_real * probe_real + probe_imag * probe_imag
    slot_ids = jnp.arange(POS_DEV, dtype=jnp.int32)
    zero_index = jnp.zeros((), jnp.int32)

    def tile_step(carry, tile):
        buffer, probe_sums = carry
        tile_row = tile // grid_cols
        tile_col = tile % grid_cols
        offsets_here = scan_offsets[tile_row, tile_col]
        live = (slot_ids < live_counts[tile_row, tile_col]).astype(jnp.float32)[:, None, None]
        row_starts = (tile_row * TILE_R + offsets_here[:, 0] + half).astype(jnp.int32)
        col_starts = (tile_col * TILE_C + offsets_here[:, 1] + half).astype(jnp.int32)

        def extract(row_start, col_start):
            return lax.dynamic_slice(padded, (zero_index, row_start, col_start), (2, PROBE, PROBE))
        patches = jax.vmap(extract)(row_starts, col_starts)
        patch_real = patches[:, 0]
        patch_imag = patches[:, 1]
        measured = magnitudes[tile_row, tile_col]
        wave_real = probe_real * patch_real - probe_imag * patch_imag
        wave_imag = probe_real * patch_imag + probe_imag * patch_real
        far_real, far_imag = transform(wave_real, wave_imag, False)
        modulus = jnp.sqrt(far_real * far_real + far_imag * far_imag)
        factor = measured / jnp.maximum(modulus, modulus_floor) - 1.0
        diff_real, diff_imag = transform(far_real * factor, far_imag * factor, True)
        diff_real = diff_real * live
        diff_imag = diff_imag * live
        grad_real = probe_real * diff_real + probe_imag * diff_imag
        grad_imag = probe_real * diff_imag - probe_imag * diff_real
        pieces = jnp.stack([grad_real, grad_imag, live * power], axis=1)

        def place(slot, total):
            start = (zero_index, row_starts[slot], col_starts[slot])
            current = lax.dynamic_slice(total, start, (3, PROBE, PROBE))
            return lax.dynamic_update_slice(total, current + pieces[slot], start)
        buffer = lax.fori_loop(0, POS_DEV, place, buffer)
        probe_terms = jnp.stack([lax.optimization_barrier(jnp.sum(patch_real * diff_real + patch_imag * diff_imag, 0)), lax.optimization_barrier(jnp.sum(patch_real * diff_imag - patch_imag * diff_real, 0)), lax.optimization_barrier(jnp.sum(live * (patch_real * patch_real + patch_imag * patch_imag), 0))])
        return ((buffer, probe_sums + probe_terms), None)
    start_buffer = jnp.zeros((3, padded.shape[1], padded.shape[2]), jnp.float32)
    start_probe = jnp.zeros((3, PROBE, PROBE), jnp.float32)
    tiles = jnp.arange(grid_rows * grid_cols, dtype=jnp.int32)
    (buffer, probe_sums), unused = lax.scan(tile_step, (start_buffer, start_probe), tiles)
    inner = buffer[:, half:half + specimen.shape[1], half:half + specimen.shape[2]]
    damping = object_damping * jnp.max(power)
    specimen_next = specimen + inner[:2] / (inner[2] + damping)
    weight = probe_sums[2]
    probe_next = probe_field + probe_sums[:2] / (weight + probe_damping * jnp.mean(weight))
    return (specimen_next, probe_next)
```

```python
import math

import jax
import jax.numpy as jnp
from jax import lax
from jax.experimental import pallas as pl
from jax.experimental.pallas import tpu as pltpu
from jax.sharding import PartitionSpec as P

modulus_floor = 0.25
object_damping = 0.1
probe_damping = 0.1


MESH = pl.DeviceIdType.MESH
PEERS = 22


def reduce_kernel(d_ref, probe_ref, out_ref, rp, s0, r1, s1, r2, s2, r3, g, wp, rw, r3w, ps, pr, ss, rs, ws, wr, zs, zr, gs, gr):
    row = lax.axis_index("row")
    col = lax.axis_index("col")
    core = row % 2
    x = (row // 2) % 4
    y = (row // 8) * 2 + col % 2
    z = col // 2

    def device(core_of, x_of, y_of, z_of):
        return ((y_of // 2) * 8 + x_of * 2 + core_of, z_of * 2 + y_of % 2)

    def copy(src, dst, send, recv, where):
        return pltpu.make_async_remote_copy(src_ref=src, dst_ref=dst, send_sem=send, recv_sem=recv, device_id=where, device_id_type=MESH)

    partner = device(1 - core, x, y, z)
    along = (
        [device(core, (x + d) % 4, y, z) for d in range(1, 4)],
        [device(core, x, (y + d) % 4, z) for d in range(1, 4)],
    )
    place = (x, y)

    barrier = pltpu.get_barrier_semaphore()
    pl.semaphore_signal(barrier, inc=1, device_id=partner, device_id_type=MESH)
    for group in along:
        for peer in group:
            pl.semaphore_signal(barrier, inc=1, device_id=peer, device_id_type=MESH)

    def greet(i, carry):
        pl.semaphore_signal(barrier, inc=1, device_id=device(core, x, y, (z + i) % 16), device_id_type=MESH)
        return carry

    lax.fori_loop(1, 16, greet, 0)
    total = d_ref[0, 2]
    for t in range(1, 64):
        total = total + d_ref[t, 2]
    wp[0] = total
    pl.semaphore_wait(barrier, PEERS)

    pending = []
    c = copy(d_ref.at[pl.ds((1 - core) * 32, 32)], rp, ps.at[0], pr.at[0], partner)
    c.start()
    cw = copy(wp.at[0], rw.at[0], ps.at[1], pr.at[1], partner)
    cw.start()
    pending += [c, cw]
    c.wait_recv()
    cw.wait_recv()
    base = core * 32

    def join(t, carry):
        s0[t] = d_ref[base + t] + rp[t]
        return carry

    lax.fori_loop(0, 32, join, 0, unroll=4)
    wp[1] = wp[0] + rw[0]

    stage = []
    for color in range(2):
        for d in range(1, 4):
            to = (place[color] + d) % 4
            c = copy(s0.at[pl.ds(color * 16 + to * 4, 4)], r1.at[color, d - 1], ss.at[0, color, d - 1], rs.at[0, color, d - 1], along[color][d - 1])
            c.start()
            stage.append(c)
    for d in range(1, 4):
        c = copy(wp.at[1], rw.at[d], ws.at[0, d - 1], wr.at[0, d - 1], along[0][d - 1])
        c.start()
        stage.append(c)
    for c in stage:
        c.wait_recv()
    pending += stage
    for color in range(2):
        for b in range(4):
            s1[color, b] = s0[color * 16 + place[color] * 4 + b] + (r1[color, 0, b] + (r1[color, 1, b] + r1[color, 2, b]))
    wp[2] = wp[1] + (rw[1] + (rw[2] + rw[3]))

    stage = []
    for color in range(2):
        other = 1 - color
        for d in range(1, 4):
            to = (place[other] + d) % 4
            c = copy(s1.at[color, to], r2.at[color, d - 1], ss.at[1, color, d - 1], rs.at[1, color, d - 1], along[other][d - 1])
            c.start()
            stage.append(c)
    for d in range(1, 4):
        c = copy(wp.at[2], rw.at[3 + d], ws.at[1, d - 1], wr.at[1, d - 1], along[1][d - 1])
        c.start()
        stage.append(c)
    for c in stage:
        c.wait_recv()
    pending += stage
    for color in range(2):
        s2[color] = s1[color, place[1 - color]] + (r2[color, 0] + (r2[color, 1] + r2[color, 2]))
    wp[3] = wp[2] + (rw[4] + (rw[5] + rw[6]))

    def root(color):
        return 2 + 8 * color + 4 * core

    def slot(color):
        return core * 32 + color * 16 + place[color] * 4 + place[1 - color]

    for color in range(2):
        goal = root(color)

        @pl.when(z != goal)
        def _():
            at = (z - goal + 16) % 16
            copy(s2.at[color], r3.at[at - 1], zs.at[color, 0], zr.at[0], device(core, x, y, goal)).start()
            copy(wp.at[3], r3w.at[at - 1], zs.at[color, 1], zr.at[1], device(core, x, y, goal)).start()

    for color in range(2):

        @pl.when(z == root(color))
        def _():
            pltpu.make_async_copy(r3, r3, zr.at[0]).wait()
            pltpu.make_async_copy(r3w, r3w, zr.at[1]).wait()
            full = s2[color]
            weight = wp[3]
            for i in range(15):
                full = full + r3[i]
                weight = weight + r3w[i]
            mean = jnp.sum(weight) * (1.0 / 65536.0)
            scale = full[2] + 0.1 * mean
            t = slot(color)
            g[t, 0] = probe_ref[t, 0] + full[0] / scale
            g[t, 1] = probe_ref[t, 1] + full[1] / scale

            def send(i, carry):
                copy(g.at[t], g.at[t], gs.at[i - 1], gr.at[color], device(core, x, y, (z + i) % 16)).start()
                return carry

            lax.fori_loop(1, 16, send, 0)

    for color in range(2):

        @pl.when(z != root(color))
        def _():
            t = slot(color)
            pltpu.make_async_copy(g.at[t], g.at[t], gr.at[color]).wait()

    stage = []
    for color in range(2):
        other = 1 - color
        t = slot(color)
        for d in range(1, 4):
            c = copy(g.at[t], g.at[t], ss.at[2, color, d - 1], rs.at[2, color, d - 1], along[other][d - 1])
            c.start()
            stage.append(c)
    for c in stage:
        c.wait_recv()
    pending += stage
    stage = []
    for color in range(2):
        t = core * 32 + color * 16 + place[color] * 4
        for d in range(1, 4):
            c = copy(g.at[pl.ds(t, 4)], g.at[pl.ds(t, 4)], ss.at[3, color, d - 1], rs.at[3, color, d - 1], along[color][d - 1])
            c.start()
            stage.append(c)
    for c in stage:
        c.wait_recv()
    pending += stage
    c = copy(g.at[pl.ds(base, 32)], g.at[pl.ds(base, 32)], ps.at[2], pr.at[2], partner)
    c.start()
    c.wait_recv()
    pending.append(c)
    for lb in range(2):
        for rb in range(32):
            for p in range(2):
                out_ref[p, rb * 8 : rb * 8 + 8, lb * 128 : lb * 128 + 128] = g[lb * 32 + rb, p]
    for c in pending:
        c.wait_send()
    for color in range(2):

        @pl.when(z != root(color))
        def _():
            pltpu.make_async_copy(s2.at[color], s2.at[color], zs.at[color, 0]).wait()
            pltpu.make_async_copy(wp.at[3], wp.at[3], zs.at[color, 1]).wait()

        @pl.when(z == root(color))
        def _():
            t = slot(color)

            def done(i, carry):
                pltpu.make_async_copy(g.at[t], g.at[t], gs.at[i]).wait()
                return carry

            lax.fori_loop(0, 15, done, 0)


def reduce_probe(pieces, probe_tiles):
    tile = (8, 128)
    dma = pltpu.SemaphoreType.DMA
    vmem = pltpu.VMEM
    f32 = jnp.float32
    return pl.pallas_call(
        reduce_kernel,
        out_shape=jax.ShapeDtypeStruct((2, 256, 256), f32),
        in_specs=[pl.BlockSpec(memory_space=pltpu.VMEM)] * 2,
        out_specs=pl.BlockSpec(memory_space=pltpu.VMEM),
        scratch_shapes=[
            vmem((32, 3) + tile, f32),
            vmem((32, 3) + tile, f32),
            vmem((2, 3, 4, 3) + tile, f32),
            vmem((2, 4, 3) + tile, f32),
            vmem((2, 3, 3) + tile, f32),
            vmem((2, 3) + tile, f32),
            vmem((15, 3) + tile, f32),
            vmem((64, 2) + tile, f32),
            vmem((4,) + tile, f32),
            vmem((7,) + tile, f32),
            vmem((15,) + tile, f32),
            dma((3,)),
            dma((3,)),
            dma((4, 2, 3)),
            dma((4, 2, 3)),
            dma((2, 3)),
            dma((2, 3)),
            dma((2, 2)),
            dma((2,)),
            dma((15,)),
            dma((2,)),
        ],
        compiler_params=pltpu.CompilerParams(collective_id=0, has_side_effects=True),
        name="reduce_probe",
    )(pieces, probe_tiles)


def to_tiles(planes):
    count = planes.shape[0]
    return planes.reshape(count, 32, 8, 2, 128).transpose(3, 1, 0, 2, 4).reshape(64, count, 8, 128)


def extended_2(block, sides, width):
    for axis, dim in sides:
        count = lax.axis_size(axis)
        forward = [(i, i + 1) for i in range(count - 1)]
        backward = [(target, source) for source, target in forward]
        low = lax.ppermute(
            lax.slice_in_dim(block, block.shape[dim] - width, None, axis=dim), axis, forward
        )
        high = lax.ppermute(lax.slice_in_dim(block, 0, width, axis=dim), axis, backward)
        block = jnp.concatenate([low, block, high], axis=dim)
    return block


def dft_tables(width):
    counter = jnp.arange(width, dtype=jnp.int32)
    phase = counter[:, None] * counter[None, :] % width
    angle = phase.astype(jnp.float32) * (2.0 * math.pi / width)
    factor = 1.0 / math.sqrt(width)
    return (jnp.cos(angle) * factor, jnp.sin(angle) * factor)


def matmul_right(left, table):
    return jnp.einsum("sjm,ml->sjl", left, table, precision=lax.Precision.HIGHEST)


def matmul_left(table, right):
    return jnp.einsum("kj,sjl->skl", table, right, precision=lax.Precision.HIGHEST)


def transform(wave_real, wave_imag, cosine, sine, direction):
    inner_real = matmul_right(wave_real, cosine) + direction * matmul_right(wave_imag, sine)
    inner_imag = matmul_right(wave_imag, cosine) - direction * matmul_right(wave_real, sine)
    outer_real = matmul_left(cosine, inner_real) + direction * matmul_left(sine, inner_imag)
    outer_imag = matmul_left(cosine, inner_imag) - direction * matmul_left(sine, inner_real)
    return (outer_real, outer_imag)


def fold_rims(wide, tile_r, tile_c, half):
    center = wide[:, 2 * half : 2 * half + tile_r, :]
    center = center.at[:, :half, :].add(wide[:, :half, :])
    center = center.at[:, tile_r - half :, :].add(wide[:, tile_r + 3 * half :, :])
    result = center[:, :, 2 * half : 2 * half + tile_c]
    result = result.at[:, :, :half].add(center[:, :, :half])
    result = result.at[:, :, tile_c - half :].add(center[:, :, tile_c + 3 * half :])
    return result


def shards(specimen, probe_field, scan_offsets, live_counts, magnitudes):
    width = probe_field.shape[1]
    half = width // 2
    tile_r = specimen.shape[1]
    tile_c = specimen.shape[2]
    slots = magnitudes.shape[2]
    row_place = lax.axis_index("row")
    col_place = lax.axis_index("col")
    zero_index = jnp.zeros((), jnp.int32)
    extended = extended_2(specimen, (("row", 1), ("col", 2)), half)
    offsets_here = scan_offsets[row_place, col_place]
    live = (jnp.arange(slots, dtype=jnp.int32) < live_counts[row_place, col_place]).astype(
        jnp.float32
    )[:, None, None]
    row_starts = offsets_here[:, 0] + half
    col_starts = offsets_here[:, 1] + half

    def extract(row_start, col_start):
        return lax.dynamic_slice(extended, (zero_index, row_start, col_start), (2, width, width))

    patches = jax.vmap(extract)(row_starts, col_starts)
    patch_real = patches[:, 0]
    patch_imag = patches[:, 1]
    probe_real = probe_field[0]
    probe_imag = probe_field[1]
    power = probe_real * probe_real + probe_imag * probe_imag
    cosine, sine = dft_tables(width)
    wave_real = probe_real * patch_real - probe_imag * patch_imag
    wave_imag = probe_real * patch_imag + probe_imag * patch_real
    far_real, far_imag = transform(wave_real, wave_imag, cosine, sine, 1.0)
    modulus = jnp.sqrt(far_real * far_real + far_imag * far_imag)
    factor = magnitudes[0, 0] / jnp.maximum(modulus, modulus_floor) - 1.0
    diff_real, diff_imag = transform(far_real * factor, far_imag * factor, cosine, sine, -1.0)
    diff_real = diff_real * live
    diff_imag = diff_imag * live
    grad_real = probe_real * diff_real + probe_imag * diff_imag
    grad_imag = probe_real * diff_imag - probe_imag * diff_real
    pieces = jnp.stack([grad_real, grad_imag, live * power], axis=1)
    layers = pieces.shape[1]

    def place(slot, total):
        start = (zero_index, row_starts[slot], col_starts[slot])
        current = lax.dynamic_slice(total, start, (layers, width, width))
        return lax.dynamic_update_slice(total, current + pieces[slot], start)

    start_total = jnp.zeros((layers, tile_r + 2 * half, tile_c + 2 * half), jnp.float32)
    buffer = lax.fori_loop(0, slots, place, start_total)
    wide = extended_2(buffer, (("row", 1), ("col", 2)), half)
    folded = fold_rims(wide, tile_r, tile_c, half)
    update = folded[:2]
    lighting = folded[2]
    damping = object_damping * jnp.max(power)
    specimen_next = specimen + update / (lighting + damping)
    local_terms = (
        jnp.sum(patch_real * diff_real + patch_imag * diff_imag, 0),
        jnp.sum(patch_real * diff_imag - patch_imag * diff_real, 0),
        jnp.sum(live * (patch_real * patch_real + patch_imag * patch_imag), 0),
    )
    probe_next = reduce_probe(to_tiles(jnp.stack(local_terms)), to_tiles(probe_field))
    return (specimen_next, probe_next)


def solution(mesh):
    return jax.shard_map(
        shards,
        mesh=mesh,
        in_specs=(P(None, "row", "col"), P(), P(), P(), P("row", "col", None, None, None)),
        out_specs=(P(None, "row", "col"), P()),
        check_vma=False,
    )
```

```python
import math

import jax
import jax.numpy as jnp
import numpy as np
from jax import lax
from jax.experimental import pallas as pl
from jax.experimental.pallas import tpu as pltpu
from jax.sharding import PartitionSpec as P

MESH = pl.DeviceIdType.MESH
ROWS = 16
COLS = 32
object_damping = 0.1
probe_damping = 0.1
f32 = jnp.float32
bf16 = jnp.bfloat16
VMEM = pl.BlockSpec(memory_space=pltpu.VMEM)
SMEM = pl.BlockSpec(memory_space=pltpu.SMEM)


def remote(src, dst, send, recv, where):
    return pltpu.make_async_remote_copy(src_ref=src, dst_ref=dst, send_sem=send, recv_sem=recv, device_id=where, device_id_type=MESH)


def greet(barrier, where):
    pl.semaphore_signal(barrier, inc=1, device_id=where, device_id_type=MESH)


def halo_kernel(tile_ref, ext, own, cs, cr, vs, vr):
    row = lax.axis_index("row")
    col = lax.axis_index("col")
    has = {"l": col > 0, "r": col < COLS - 1, "u": row > 0, "d": row < ROWS - 1}
    to = {"l": (row, col - 1), "r": (row, col + 1), "u": (row - 1, col), "d": (row + 1, col)}
    center = [pltpu.make_async_copy(tile_ref.at[:, :, pl.ds(j * 128, 128)], ext.at[:, 1 + j, pl.ds(128, 128), :], own.at[j]) for j in range(2)]
    for c in center:
        c.start()
    barrier = pltpu.get_barrier_semaphore()
    for side in "lrud":

        @pl.when(has[side])
        def _():
            greet(barrier, to[side])

    expected = sum(has[side].astype(jnp.int32) for side in "lrud")

    @pl.when(row == 0)
    def _():
        ext[:, :, 0:128, :] = jnp.zeros((2, 4, 128, 128), f32)

    @pl.when(row == ROWS - 1)
    def _():
        ext[:, :, 256:384, :] = jnp.zeros((2, 4, 128, 128), f32)

    @pl.when(col == 0)
    def _():
        ext[:, 0] = jnp.zeros((2, 384, 128), f32)

    @pl.when(col == COLS - 1)
    def _():
        ext[:, 3] = jnp.zeros((2, 384, 128), f32)

    for c in center:
        c.wait()
    pl.semaphore_wait(barrier, expected)

    def across(p, side):
        mine, theirs = (1, 3) if side == "l" else (2, 0)
        i = 0 if side == "l" else 1
        return remote(ext.at[p, mine, pl.ds(128, 128)], ext.at[p, theirs, pl.ds(128, 128)], cs.at[p, i], cr.at[p, i], to[side])

    def up_down(p, side, part):
        at = (pl.ds(1, 2), 0, 3)[part]
        i, theirs = (0, 256) if side == "u" else (1, 0)
        return remote(ext.at[p, at, pl.ds(128, 128)], ext.at[p, at, pl.ds(theirs, 128)], vs.at[p, part, i], vr.at[p, part, i], to[side])

    for p in range(2):
        for side in "lr":

            @pl.when(has[side])
            def _():
                across(p, side).start()

    for p in range(2):
        for side in "ud":

            @pl.when(has[side])
            def _():
                up_down(p, side, 0).start()

    for p in range(2):
        for side, part in (("l", 1), ("r", 2)):

            @pl.when(has[side])
            def _():
                across(p, "r" if side == "l" else "l").wait_recv()
                for way in "ud":

                    @pl.when(has[way])
                    def _():
                        up_down(p, way, part).start()

    for p in range(2):
        for side in "lr":

            @pl.when(has[side])
            def _():
                across(p, side).wait_send()

        for way, back in (("u", "d"), ("d", "u")):
            for part, need in ((0, None), (1, "l"), (2, "r")):
                cond = has[way] if need is None else jnp.logical_and(has[way], has[need])

                @pl.when(cond)
                def _():
                    up_down(p, way, part).wait_send()
                    up_down(p, back, part).wait_recv()


def halo(tile):
    dma = pltpu.SemaphoreType.DMA
    return pl.pallas_call(
        halo_kernel,
        out_shape=jax.ShapeDtypeStruct((2, 4, 384, 128), f32),
        in_specs=[pl.BlockSpec(memory_space=pl.ANY)],
        out_specs=VMEM,
        scratch_shapes=[dma((2,)), dma((2, 2)), dma((2, 2)), dma((2, 3, 2)), dma((2, 3, 2))],
        compiler_params=pltpu.CompilerParams(collective_id=1, has_side_effects=True),
        name="halo",
    )(tile)


def dft_tables():
    m = np.arange(128)[:, None]
    k = np.arange(128)[None, :]
    tables = []
    for odd in range(2):
        angle = ((m * (2 * k + odd)) % 256) * (2.0 * math.pi / 256)
        c, s = np.cos(angle) / 16, np.sin(angle) / 16
        full = np.block([[c, -s], [s, c]])
        for t in (full, full.T):
            high = t.astype(np.float32).astype(jnp.bfloat16)
            low = (t - high.astype(np.float64)).astype(np.float32).astype(jnp.bfloat16)
            tables += [high, low]
    order = np.concatenate([np.arange(0, 256, 2), np.arange(1, 256, 2)])
    select = (np.arange(256)[:, None] == order[None, :]).astype(jnp.bfloat16)
    return np.stack(tables).reshape(2, 2, 2, 256, 256), select


def split(value):
    high = value.astype(bf16)
    return high, (value - high.astype(f32)).astype(bf16)


def product(a, b):
    def dot(u, v):
        return jnp.dot(u, v, preferred_element_type=f32)

    return dot(a[0], b[0]) + (dot(a[1], b[0]) + dot(a[0], b[1]))


STEP = 64


def tile_kernel(offs, live, ext, probe, mags, tables, select, upd, pieces, den, pat, wave, freq, zb, padded, seen, sems):
    row = lax.axis_index("row")
    col = lax.axis_index("col")

    def table(odd, turned):
        return tables[odd, turned, 0], tables[odd, turned, 1]

    fetch = [[pltpu.make_async_copy(mags.at[0, 0, s, :, pl.ds(j * 128, 128)], seen.at[s, j], sems.at[s, j]) for j in range(2)] for s in range(2)]
    for pair in fetch:
        for c in pair:
            c.start()
    upd[...] = jnp.zeros_like(upd)
    for s in range(2):
        top = offs[(row * 2 + s) * 2, col] + 128
        left = offs[(row * 2 + s) * 2 + 1, col] + 128
        turn, block = left % 128, left // 128
        lane = lax.broadcasted_iota(jnp.int32, (STEP, 128), 1)
        alive = (s < live[row, col]).astype(f32)
        for i in range(0, 256, STEP):
            got = []
            for p in range(2):
                rolled = [pltpu.roll(ext[p, jnp.minimum(block + j, 3), pl.ds(top + i, STEP), :], 128 - turn, 1) for j in range(3)]
                halves = [jnp.where(lane < 128 - turn, rolled[j], rolled[j + 1]) for j in range(2)]
                got.append(jnp.concatenate(halves, 1))
                pat[p, i : i + STEP, :] = got[p]
            pr, pi = probe[0, i : i + STEP, :], probe[1, i : i + STEP, :]
            wr = pr * got[0] - pi * got[1]
            wi = pr * got[1] + pi * got[0]
            for odd in range(2):
                if odd:
                    mixed = [w[:, :128] - w[:, 128:] for w in (wr, wi)]
                else:
                    mixed = [w[:, :128] + w[:, 128:] for w in (wr, wi)]
                out = product(split(jnp.concatenate(mixed, 1)), table(odd, 0))
                for p in range(2):
                    wave[p, i : i + STEP, odd * 128 : odd * 128 + 128] = out[:, p * 128 : p * 128 + 128]
        for odd in range(2):
            if odd:
                mixed = [wave[p, 0:128, :] - wave[p, 128:256, :] for p in range(2)]
            else:
                mixed = [wave[p, 0:128, :] + wave[p, 128:256, :] for p in range(2)]
            freq[odd] = product(table(odd, 1), split(jnp.concatenate(mixed, 0)))
        for c in fetch[s]:
            c.wait()
        for odd in range(2):
            for i in range(0, 128, STEP):
                mh, ml = split(jnp.concatenate([seen[s, j, pl.ds(odd + 2 * i, STEP, stride=2), :] for j in range(2)], 1))
                measured = jnp.dot(mh, select[...], preferred_element_type=f32) + jnp.dot(ml, select[...], preferred_element_type=f32)
                fr = freq[odd, i : i + STEP, :]
                fi = freq[odd, 128 + i : 128 + i + STEP, :]
                factor = measured * lax.rsqrt(jnp.maximum(fr * fr + fi * fi, 0.0625)) - 1.0
                factor = factor * alive
                for p, value in ((0, fr * factor), (1, fi * factor)):
                    high, low = split(value)
                    zb[odd, 0, p * 128 + i : p * 128 + i + STEP, :] = high
                    zb[odd, 1, p * 128 + i : p * 128 + i + STEP, :] = low
        for odd in range(2):
            freq[odd] = product(table(odd, 0), (zb[odd, 0], zb[odd, 1]))
        for p in range(2):
            e = freq[0, p * 128 : p * 128 + 128, :]
            o = freq[1, p * 128 : p * 128 + 128, :]
            wave[p, 0:128, :] = e + o
            wave[p, 128:256, :] = e - o
        for i in range(0, 256, STEP):
            parts = []
            for odd in range(2):
                mixed = [wave[p, i : i + STEP, odd * 128 : odd * 128 + 128] for p in range(2)]
                parts.append(product(split(jnp.concatenate(mixed, 1)), table(odd, 1)))
            diff = []
            for p in range(2):
                e, o = (parts[odd][:, p * 128 : p * 128 + 128] for odd in range(2))
                diff.append(jnp.concatenate([e + o, e - o], 1))
            dr, di = diff
            pr, pi = probe[0, i : i + STEP, :], probe[1, i : i + STEP, :]
            ore, oim = pat[0, i : i + STEP, :], pat[1, i : i + STEP, :]
            for p, grad in ((0, pr * dr + pi * di), (1, pr * di - pi * dr)):
                first, second = (pltpu.roll(grad[:, j * 128 : j * 128 + 128], turn, 1) for j in range(2))
                moved = (jnp.where(lane >= turn, first, 0.0), jnp.where(lane >= turn, second, first), jnp.where(lane < turn, second, 0.0))
                for j in range(3):
                    at = (p, jnp.minimum(block + j, 3), pl.ds(top + i, STEP))
                    upd[at] = upd[at] + moved[j]
            terms = (ore * dr + oim * di, ore * di - oim * dr, (ore * ore + oim * oim) * alive)
            for lb in range(2):
                for rb in range(STEP // 8):
                    t = lb * 32 + i // 8 + rb
                    for p in range(3):
                        value = terms[p][rb * 8 : rb * 8 + 8, lb * 128 : lb * 128 + 128]
                        pieces[t, p] = value if s == 0 else pieces[t, p] + value
    padded[...] = jnp.zeros_like(padded)
    peak = jnp.zeros((8, 128), f32)
    for i in range(0, 256, STEP):
        power = probe[0, i : i + STEP, :] * probe[0, i : i + STEP, :] + probe[1, i : i + STEP, :] * probe[1, i : i + STEP, :]
        for j in range(2):
            padded[2 + j, 128 + i : 128 + i + STEP, :] = power[:, j * 128 : j * 128 + 128]
        for a in range(0, STEP, 8):
            for b in range(0, 256, 128):
                peak = jnp.maximum(peak, power[a : a + 8, b : b + 128])
    den[...] = jnp.full((128, 256), object_damping, f32) * jnp.max(peak)

    def add(n, carry):
        da = n // 6 - 1
        db = (n // 2) % 3 - 1
        s = n % 2
        a = row + da
        b = col + db
        inside = (a >= 0) & (a < ROWS) & (b >= 0) & (b < COLS)
        a = jnp.clip(a, 0, ROWS - 1)
        b = jnp.clip(b, 0, COLS - 1)
        down = da * 128 + offs[(a * 2 + s) * 2, b]
        across = db * 256 + offs[(a * 2 + s) * 2 + 1, b]
        on = inside & (s < live[a, b]) & (across > -256) & (across < 256)

        @pl.when(on)
        def _():
            turn = (across + 256) % 128
            block = 4 - (across + 256) // 128
            lane = lax.broadcasted_iota(jnp.int32, (STEP, 128), 1)
            for i in range(0, 128, STEP):
                rolled = [pltpu.roll(padded[block + j - 1, pl.ds(i + 128 - down, STEP), :], turn, 1) for j in range(3)]
                for j in range(2):
                    den[i : i + STEP, j * 128 : j * 128 + 128] += jnp.where(lane >= turn, rolled[j + 1], rolled[j])

        return carry

    lax.fori_loop(0, 18, add, 0)


def tile_step(offs, live, ext, probe, mags):
    tables, select = dft_tables()
    out = jax.ShapeDtypeStruct
    vmem = pltpu.VMEM
    return pl.pallas_call(
        tile_kernel,
        out_shape=(out((2, 4, 384, 128), f32), out((64, 3, 8, 128), f32), out((128, 256), f32)),
        in_specs=[SMEM, SMEM, VMEM, VMEM, pl.BlockSpec(memory_space=pl.ANY), VMEM, VMEM],
        out_specs=(VMEM,) * 3,
        scratch_shapes=[
            vmem((2, 256, 256), f32),
            vmem((2, 256, 256), f32),
            vmem((2, 256, 256), f32),
            vmem((2, 2, 256, 256), bf16),
            vmem((6, 512, 128), f32),
            vmem((2, 2, 256, 128), f32),
            pltpu.SemaphoreType.DMA((2, 2)),
        ],
        name="tile_step",
    )(offs, live, ext, probe, mags, jnp.asarray(tables), jnp.asarray(select))


def finish_kernel(d_ref, probe_ref, u_ref, den_ref, spec_ref, spec_out, out_ref, fv, side, fc, hs, hr, es, er, rp, s0, r1, s1, r2, s2, r3, g, wp, rw, r3w, ps, pr, ss, rs, ws, wr, zs, zr, gs, gr):
    row = lax.axis_index("row")
    col = lax.axis_index("col")
    core = row % 2
    x = (row // 2) % 4
    y = (row // 8) * 2 + col % 2
    z = col // 2

    def device(core_of, x_of, y_of, z_of):
        return ((y_of // 2) * 8 + x_of * 2 + core_of, z_of * 2 + y_of % 2)

    copy = remote
    partner = device(1 - core, x, y, z)
    along = (
        [device(core, (x + d) % 4, y, z) for d in range(1, 4)],
        [device(core, x, (y + d) % 4, z) for d in range(1, 4)],
    )
    place = (x, y)
    has = {"l": col > 0, "r": col < COLS - 1, "u": row > 0, "d": row < ROWS - 1}
    beside = {"l": (row, col - 1), "r": (row, col + 1), "u": (row - 1, col), "d": (row + 1, col)}

    barrier = pltpu.get_barrier_semaphore()
    pl.semaphore_signal(barrier, inc=1, device_id=partner, device_id_type=MESH)
    for group in along:
        for peer in group:
            pl.semaphore_signal(barrier, inc=1, device_id=peer, device_id_type=MESH)

    def hail(i, carry):
        greet(barrier, device(core, x, y, (z + i) % 16))
        return carry

    lax.fori_loop(1, 16, hail, 0)
    for side_of in "lrud":

        @pl.when(has[side_of])
        def _():
            greet(barrier, beside[side_of])

    expected = 22 + sum(has[side_of].astype(jnp.int32) for side_of in "lrud")

    for i, side_of in enumerate("ud"):

        @pl.when(jnp.logical_not(has[side_of]))
        def _():
            fv[i] = jnp.zeros((2, 4, 128, 128), f32)

    for i, side_of in enumerate("lr"):

        @pl.when(jnp.logical_not(has[side_of]))
        def _():
            fc[i] = jnp.zeros((2, 128, 128), f32)

    total = d_ref[0, 2]
    for t in range(1, 64):
        total = total + d_ref[t, 2]
    wp[0] = total
    pl.semaphore_wait(barrier, expected)

    def vertical(p, part, side_of):
        at = (0, 3, pl.ds(1, 2))[part]
        i, first = (0, 0) if side_of == "u" else (1, 256)
        return copy(u_ref.at[p, at, pl.ds(first, 128)], fv.at[1 - i, p, at], hs.at[p, part, i], hr.at[p, part, 1 - i], beside[side_of])

    def arrival(p, part, side_of):
        at = (0, 3, pl.ds(1, 2))[part]
        i = 0 if side_of == "u" else 1
        return copy(u_ref.at[p, at, pl.ds(0, 128)], fv.at[i, p, at], hs.at[p, part, i], hr.at[p, part, i], beside[side_of])

    def lateral(p, side_of):
        i = 0 if side_of == "l" else 1
        return copy(side.at[i, p], fc.at[1 - i, p], es.at[p, i], er.at[p, 1 - i], beside[side_of])

    def lateral_in(p, side_of):
        i = 0 if side_of == "l" else 1
        return copy(side.at[i, p], fc.at[i, p], es.at[p, i], er.at[p, i], beside[side_of])


    pending = []
    c = copy(d_ref.at[pl.ds((1 - core) * 32, 32)], rp, ps.at[0], pr.at[0], partner)
    c.start()
    cw = copy(wp.at[0], rw.at[0], ps.at[1], pr.at[1], partner)
    cw.start()
    pending += [c, cw]
    c.wait_recv()
    cw.wait_recv()
    base = core * 32

    def join(t, carry):
        s0[t] = d_ref[base + t] + rp[t]
        return carry

    lax.fori_loop(0, 32, join, 0, unroll=4)
    wp[1] = wp[0] + rw[0]

    stage = []
    for color in range(2):
        for d in range(1, 4):
            to = (place[color] + d) % 4
            c = copy(s0.at[pl.ds(color * 16 + to * 4, 4)], r1.at[color, d - 1], ss.at[0, color, d - 1], rs.at[0, color, d - 1], along[color][d - 1])
            c.start()
            stage.append(c)
    for d in range(1, 4):
        c = copy(wp.at[1], rw.at[d], ws.at[0, d - 1], wr.at[0, d - 1], along[0][d - 1])
        c.start()
        stage.append(c)
    for c in stage:
        c.wait_recv()
    pending += stage
    for color in range(2):
        for b in range(4):
            s1[color, b] = s0[color * 16 + place[color] * 4 + b] + (r1[color, 0, b] + (r1[color, 1, b] + r1[color, 2, b]))
    wp[2] = wp[1] + (rw[1] + (rw[2] + rw[3]))

    stage = []
    for color in range(2):
        other = 1 - color
        for d in range(1, 4):
            to = (place[other] + d) % 4
            c = copy(s1.at[color, to], r2.at[color, d - 1], ss.at[1, color, d - 1], rs.at[1, color, d - 1], along[other][d - 1])
            c.start()
            stage.append(c)
    for d in range(1, 4):
        c = copy(wp.at[2], rw.at[3 + d], ws.at[1, d - 1], wr.at[1, d - 1], along[1][d - 1])
        c.start()
        stage.append(c)
    for part in range(3):
        for p in range(2):
            for side_of in "ud":

                @pl.when(has[side_of])
                def _():
                    vertical(p, part, side_of).start()

    for c in stage:
        c.wait_recv()
    pending += stage
    for color in range(2):
        s2[color] = s1[color, place[1 - color]] + (r2[color, 0] + (r2[color, 1] + r2[color, 2]))
    wp[3] = wp[2] + (rw[4] + (rw[5] + rw[6]))

    def root(color):
        return 2 + 8 * color + 4 * core

    def slot(color):
        return core * 32 + color * 16 + place[color] * 4 + place[1 - color]

    for color in range(2):
        goal = root(color)

        @pl.when(z != goal)
        def _():
            at = (z - goal + 16) % 16
            copy(s2.at[color], r3.at[at - 1], zs.at[color, 0], zr.at[0], device(core, x, y, goal)).start()
            copy(wp.at[3], r3w.at[at - 1], zs.at[color, 1], zr.at[1], device(core, x, y, goal)).start()

    for color in range(2):

        @pl.when(z == root(color))
        def _():
            pltpu.make_async_copy(r3, r3, zr.at[0]).wait()
            pltpu.make_async_copy(r3w, r3w, zr.at[1]).wait()
            full = s2[color]
            weight = wp[3]
            for i in range(15):
                full = full + r3[i]
                weight = weight + r3w[i]
            mean = jnp.sum(weight) * (1.0 / 65536.0)
            scale = full[2] + probe_damping * mean
            t = slot(color)
            rows = pl.ds(pl.multiple_of((t % 32) * 8, 8), 8)
            lanes = pl.ds(pl.multiple_of((t // 32) * 128, 128), 128)
            for p in range(2):
                g[t, p] = probe_ref[p, rows, lanes] + full[p] / scale

            def send(i, carry):
                copy(g.at[t], g.at[t], gs.at[i - 1], gr.at[color], device(core, x, y, (z + i) % 16)).start()
                return carry

            lax.fori_loop(1, 16, send, 0)

    for i, (side_of, at) in enumerate((("l", 0), ("r", 3))):
        for p in range(2):
            for way in "ud":

                @pl.when(has[way])
                def _():
                    arrival(p, i, way).wait_recv()

            @pl.when(has[side_of])
            def _():
                side[i, p] = u_ref[p, at, 128:256, :] + (fv[0, p, at] + fv[1, p, at])
                lateral(p, side_of).start()

    for color in range(2):

        @pl.when(z != root(color))
        def _():
            t = slot(color)
            pltpu.make_async_copy(g.at[t], g.at[t], gr.at[color]).wait()

    stage = []
    for color in range(2):
        other = 1 - color
        t = slot(color)
        for d in range(1, 4):
            c = copy(g.at[t], g.at[t], ss.at[2, color, d - 1], rs.at[2, color, d - 1], along[other][d - 1])
            c.start()
            stage.append(c)
    for c in stage:
        c.wait_recv()
    pending += stage
    stage = []
    for color in range(2):
        t = core * 32 + color * 16 + place[color] * 4
        for d in range(1, 4):
            c = copy(g.at[pl.ds(t, 4)], g.at[pl.ds(t, 4)], ss.at[3, color, d - 1], rs.at[3, color, d - 1], along[color][d - 1])
            c.start()
            stage.append(c)
    for c in stage:
        c.wait_recv()
    pending += stage
    c = copy(g.at[pl.ds(base, 32)], g.at[pl.ds(base, 32)], ps.at[2], pr.at[2], partner)
    c.start()
    c.wait_recv()
    pending.append(c)
    for p in range(2):
        for way in "ud":

            @pl.when(has[way])
            def _():
                arrival(p, 2, way).wait_recv()

        for side_of in "lr":

            @pl.when(has[side_of])
            def _():
                lateral_in(p, side_of).wait_recv()

        for i in range(2):
            at = 1 + i
            update = u_ref[p, at, 128:256, :] + (fv[0, p, at] + fv[1, p, at]) + fc[i, p]
            lanes = slice(i * 128, i * 128 + 128)
            spec_out[p, :, lanes] = spec_ref[p, :, lanes] + update / den_ref[:, lanes]
    for lb in range(2):
        for rb in range(32):
            for p in range(2):
                out_ref[p, rb * 8 : rb * 8 + 8, lb * 128 : lb * 128 + 128] = g[lb * 32 + rb, p]
    for c in pending:
        c.wait_send()
    for p in range(2):
        for way in "ud":

            @pl.when(has[way])
            def _():
                for part in range(3):
                    vertical(p, part, way).wait_send()

        for side_of in "lr":

            @pl.when(has[side_of])
            def _():
                lateral(p, side_of).wait_send()

    for color in range(2):

        @pl.when(z != root(color))
        def _():
            pltpu.make_async_copy(s2.at[color], s2.at[color], zs.at[color, 0]).wait()
            pltpu.make_async_copy(wp.at[3], wp.at[3], zs.at[color, 1]).wait()

        @pl.when(z == root(color))
        def _():
            t = slot(color)

            def done(i, carry):
                pltpu.make_async_copy(g.at[t], g.at[t], gs.at[i]).wait()
                return carry

            lax.fori_loop(0, 15, done, 0)


def finish(upd, pieces, den, specimen, probe_field):
    tile = (8, 128)
    dma = pltpu.SemaphoreType.DMA
    vmem = pltpu.VMEM
    return pl.pallas_call(
        finish_kernel,
        out_shape=(jax.ShapeDtypeStruct((2, 128, 256), f32), jax.ShapeDtypeStruct((2, 256, 256), f32)),
        in_specs=[VMEM] * 5,
        out_specs=(VMEM,) * 2,
        scratch_shapes=[
            vmem((2, 2, 4, 128, 128), f32),
            vmem((2, 2, 128, 128), f32),
            vmem((2, 2, 128, 128), f32),
            dma((2, 3, 2)),
            dma((2, 3, 2)),
            dma((2, 2)),
            dma((2, 2)),
            vmem((32, 3) + tile, f32),
            vmem((32, 3) + tile, f32),
            vmem((2, 3, 4, 3) + tile, f32),
            vmem((2, 4, 3) + tile, f32),
            vmem((2, 3, 3) + tile, f32),
            vmem((2, 3) + tile, f32),
            vmem((15, 3) + tile, f32),
            vmem((64, 2) + tile, f32),
            vmem((4,) + tile, f32),
            vmem((7,) + tile, f32),
            vmem((15,) + tile, f32),
            dma((3,)),
            dma((3,)),
            dma((4, 2, 3)),
            dma((4, 2, 3)),
            dma((2, 3)),
            dma((2, 3)),
            dma((2, 2)),
            dma((2,)),
            dma((15,)),
            dma((2,)),
        ],
        compiler_params=pltpu.CompilerParams(collective_id=0, has_side_effects=True),
        name="finish",
    )(pieces, probe_field, upd, den, specimen)


def shards(specimen, probe_field, scan_offsets, live_counts, magnitudes):
    offs = scan_offsets.transpose(0, 2, 3, 1).reshape(ROWS * 4, COLS)
    ext = halo(specimen)
    upd, pieces, den = tile_step(offs, live_counts, ext, probe_field, magnitudes)
    return finish(upd, pieces, den, specimen, probe_field)


def solution(mesh):
    return jax.shard_map(
        shards,
        mesh=mesh,
        in_specs=(P(None, "row", "col"), P(), P(), P(), P("row", "col", None, None, None)),
        out_specs=(P(None, "row", "col"), P()),
        check_vma=False,
    )
```

```python
import math

import jax
import jax.numpy as jnp
import numpy as np
from jax import lax
from jax.experimental import pallas as pl
from jax.experimental.pallas import tpu as pltpu
from jax.sharding import PartitionSpec as P

MESH = pl.DeviceIdType.MESH
ROWS = 16
COLS = 32
object_damping = 0.1
probe_damping = 0.1
f32 = jnp.float32
bf16 = jnp.bfloat16
VMEM = pl.BlockSpec(memory_space=pltpu.VMEM)
HBM = pl.BlockSpec(memory_space=pltpu.MemorySpace.HBM)
SMEM = pl.BlockSpec(memory_space=pltpu.SMEM)


def remote(src, dst, send, recv, where):
    return pltpu.make_async_remote_copy(src_ref=src, dst_ref=dst, send_sem=send, recv_sem=recv, device_id=where, device_id_type=MESH)


def greet(barrier, where):
    pl.semaphore_signal(barrier, inc=1, device_id=where, device_id_type=MESH)

STEP = 64


def halo_kernel(offs_hbm, live_hbm, tile_ref, probe_hbm, mags, ext, den, probe, seen, padded, offs, live, own, fetch, cs, cr, vs, vr):
    row = lax.axis_index("row")
    col = lax.axis_index("col")
    has = {"l": col > 0, "r": col < COLS - 1, "u": row > 0, "d": row < ROWS - 1}
    to = {"l": (row, col - 1), "r": (row, col + 1), "u": (row - 1, col), "d": (row + 1, col)}
    center = [pltpu.make_async_copy(tile_ref.at[:, :, pl.ds(j * 128, 128)], ext.at[:, 1 + j, pl.ds(128, 128), :], own.at[j]) for j in range(2)]
    for c in center:
        c.start()
    small = [pltpu.make_async_copy(a, b, fetch.at[i]) for i, (a, b) in enumerate(((offs_hbm, offs), (live_hbm, live), (probe_hbm, probe)))]
    for c in small:
        c.start()
    shown = [pltpu.make_async_copy(mags.at[0, 0, s, :, pl.ds(j * 128, 128)], seen.at[s, j], fetch.at[3 + 2 * s + j]) for s in range(2) for j in range(2)]
    barrier = pltpu.get_barrier_semaphore()
    for side in "lrud":

        @pl.when(has[side])
        def _():
            greet(barrier, to[side])

    expected = sum(has[side].astype(jnp.int32) for side in "lrud")

    @pl.when(row == 0)
    def _():
        ext[:, :, 0:128, :] = jnp.zeros((2, 4, 128, 128), f32)

    @pl.when(row == ROWS - 1)
    def _():
        ext[:, :, 256:384, :] = jnp.zeros((2, 4, 128, 128), f32)

    @pl.when(col == 0)
    def _():
        ext[:, 0] = jnp.zeros((2, 384, 128), f32)

    @pl.when(col == COLS - 1)
    def _():
        ext[:, 3] = jnp.zeros((2, 384, 128), f32)

    for c in center:
        c.wait()
    pl.semaphore_wait(barrier, expected)

    def across(p, side):
        mine, theirs = (1, 3) if side == "l" else (2, 0)
        i = 0 if side == "l" else 1
        return remote(ext.at[p, mine, pl.ds(128, 128)], ext.at[p, theirs, pl.ds(128, 128)], cs.at[p, i], cr.at[p, i], to[side])

    def up_down(p, side, part):
        at = (pl.ds(1, 2), 0, 3)[part]
        i, theirs = (0, 256) if side == "u" else (1, 0)
        return remote(ext.at[p, at, pl.ds(128, 128)], ext.at[p, at, pl.ds(theirs, 128)], vs.at[p, part, i], vr.at[p, part, i], to[side])

    for p in range(2):
        for side in "lr":

            @pl.when(has[side])
            def _():
                across(p, side).start()

    for p in range(2):
        for side in "ud":

            @pl.when(has[side])
            def _():
                up_down(p, side, 0).start()

    for c in shown:
        c.start()
    for c in small:
        c.wait()
    padded[...] = jnp.zeros_like(padded)
    peak = jnp.zeros((8, 128), f32)
    for i in range(0, 256, STEP):
        power = probe[0, i : i + STEP, :] * probe[0, i : i + STEP, :] + probe[1, i : i + STEP, :] * probe[1, i : i + STEP, :]
        for j in range(2):
            padded[2 + j, 128 + i : 128 + i + STEP, :] = power[:, j * 128 : j * 128 + 128]
        for a in range(0, STEP, 8):
            for b in range(0, 256, 128):
                peak = jnp.maximum(peak, power[a : a + 8, b : b + 128])
    den[...] = jnp.full((128, 256), object_damping, f32) * jnp.max(peak)

    def add(n, carry):
        da = n // 6 - 1
        db = (n // 2) % 3 - 1
        s = n % 2
        a = row + da
        b = col + db
        inside = (a >= 0) & (a < ROWS) & (b >= 0) & (b < COLS)
        a = jnp.clip(a, 0, ROWS - 1)
        b = jnp.clip(b, 0, COLS - 1)
        down = da * 128 + offs[(a * 2 + s) * 2, b]
        across = db * 256 + offs[(a * 2 + s) * 2 + 1, b]
        on = (inside & (s < live[a, b]) & (across > -256) & (across < 256)).astype(f32)
        across = jnp.clip(across, -256, 255)
        turn = (across + 256) % 128
        block = 4 - (across + 256) // 128
        lane = lax.broadcasted_iota(jnp.int32, (STEP, 128), 1)
        for i in range(0, 128, STEP):
            rolled = [pltpu.roll(padded[block + j - 1, pl.ds(i + 128 - down, STEP), :], turn, 1) for j in range(3)]
            for j in range(2):
                den[i : i + STEP, j * 128 : j * 128 + 128] += on * jnp.where(lane >= turn, rolled[j + 1], rolled[j])

        return carry

    lax.fori_loop(0, 18, add, 0)

    for p in range(2):
        for side, part in (("l", 1), ("r", 2)):

            @pl.when(has[side])
            def _():
                across(p, "r" if side == "l" else "l").wait_recv()
                for way in "ud":

                    @pl.when(has[way])
                    def _():
                        up_down(p, way, part).start()

    for p in range(2):
        for side in "lr":

            @pl.when(has[side])
            def _():
                across(p, side).wait_send()

        for way, back in (("u", "d"), ("d", "u")):
            for part, need in ((0, None), (1, "l"), (2, "r")):
                cond = has[way] if need is None else jnp.logical_and(has[way], has[need])

                @pl.when(cond)
                def _():
                    up_down(p, way, part).wait_send()
                    up_down(p, back, part).wait_recv()

    for c in shown:
        c.wait()


def halo(offs, live, tile, probe, mags):
    dma = pltpu.SemaphoreType.DMA
    return pl.pallas_call(
        halo_kernel,
        out_shape=(jax.ShapeDtypeStruct((2, 4, 384, 128), f32), jax.ShapeDtypeStruct((128, 256), f32), jax.ShapeDtypeStruct((2, 256, 256), f32), jax.ShapeDtypeStruct((2, 2, 256, 128), f32)),
        in_specs=[HBM] * 5,
        out_specs=(VMEM,) * 4,
        scratch_shapes=[pltpu.VMEM((6, 512, 128), f32), pltpu.SMEM((ROWS * 4, COLS), jnp.int32), pltpu.SMEM((ROWS, COLS), jnp.int32), dma((2,)), dma((7,)), dma((2, 2)), dma((2, 2)), dma((2, 3, 2)), dma((2, 3, 2))],
        compiler_params=pltpu.CompilerParams(collective_id=1, has_side_effects=True, vmem_limit_bytes=8 << 20),
        cost_estimate=pl.CostEstimate(flops=400000000, bytes_accessed=1 << 20, transcendentals=0),
        name="halo",
    )(*(pltpu.with_memory_space_constraint(a, pltpu.MemorySpace.HBM) for a in (offs, live, tile, probe, mags)))


def dft_tables():
    m = np.arange(128)[:, None]
    k = np.arange(128)[None, :]
    tables = []
    for odd in range(2):
        angle = ((m * (2 * k + odd)) % 256) * (2.0 * math.pi / 256)
        c, s = np.cos(angle) / 16, np.sin(angle) / 16
        full = np.block([[c, -s], [s, c]])
        for t in (full, full.T):
            high = t.astype(np.float32).astype(jnp.bfloat16)
            low = (t - high.astype(np.float64)).astype(np.float32).astype(jnp.bfloat16)
            tables += [high, low]
    order = np.concatenate([np.arange(0, 256, 2), np.arange(1, 256, 2)])
    select = (np.arange(256)[:, None] == order[None, :]).astype(jnp.bfloat16)
    return np.stack(tables).reshape(2, 2, 2, 256, 256), select


def split(value):
    high = value.astype(bf16)
    return high, (value - high.astype(f32)).astype(bf16)


def product(a, b):
    def dot(u, v):
        return jnp.dot(u, v, preferred_element_type=f32)

    return dot(a[0], b[0]) + (dot(a[1], b[0]) + dot(a[0], b[1]))


def tile_kernel(offs_hbm, live_hbm, ext, probe, seen, tables, select, upd, pieces, pat, wave, freq, zb, measured, offs, live, sems):
    row = lax.axis_index("row")
    col = lax.axis_index("col")

    def table(odd, turned):
        return tables[odd, turned, 0], tables[odd, turned, 1]

    fetch = [pltpu.make_async_copy(a, b, sems.at[i]) for i, (a, b) in enumerate(((offs_hbm, offs), (live_hbm, live)))]
    for c in fetch:
        c.start()
    for s in range(2):
        for odd in range(2):
            for i in range(0, 128, STEP):
                mh, ml = split(jnp.concatenate([seen[s, j, pl.ds(odd + 2 * i, STEP, stride=2), :] for j in range(2)], 1))
                measured[s, odd, i : i + STEP, :] = jnp.dot(mh, select[...], preferred_element_type=f32) + jnp.dot(ml, select[...], preferred_element_type=f32)
    upd[...] = jnp.zeros_like(upd)
    for c in fetch:
        c.wait()
    for s in range(2):
        top = offs[(row * 2 + s) * 2, col] + 128
        left = offs[(row * 2 + s) * 2 + 1, col] + 128
        turn, block = left % 128, left // 128
        lane = lax.broadcasted_iota(jnp.int32, (STEP, 128), 1)
        alive = (s < live[row, col]).astype(f32)
        for i in range(0, 256, STEP):
            got = []
            for p in range(2):
                rolled = [pltpu.roll(ext[p, jnp.minimum(block + j, 3), pl.ds(top + i, STEP), :], 128 - turn, 1) for j in range(3)]
                halves = [jnp.where(lane < 128 - turn, rolled[j], rolled[j + 1]) for j in range(2)]
                got.append(jnp.concatenate(halves, 1))
                pat[p, i : i + STEP, :] = got[p]
            pr, pi = probe[0, i : i + STEP, :], probe[1, i : i + STEP, :]
            wr = pr * got[0] - pi * got[1]
            wi = pr * got[1] + pi * got[0]
            for odd in range(2):
                if odd:
                    mixed = [w[:, :128] - w[:, 128:] for w in (wr, wi)]
                else:
                    mixed = [w[:, :128] + w[:, 128:] for w in (wr, wi)]
                out = product(split(jnp.concatenate(mixed, 1)), table(odd, 0))
                for p in range(2):
                    wave[p, i : i + STEP, odd * 128 : odd * 128 + 128] = out[:, p * 128 : p * 128 + 128]
        for odd in range(2):
            if odd:
                mixed = [wave[p, 0:128, :] - wave[p, 128:256, :] for p in range(2)]
            else:
                mixed = [wave[p, 0:128, :] + wave[p, 128:256, :] for p in range(2)]
            freq[odd] = product(table(odd, 1), split(jnp.concatenate(mixed, 0)))
        for odd in range(2):
            for i in range(0, 128, STEP):
                fr = freq[odd, i : i + STEP, :]
                fi = freq[odd, 128 + i : 128 + i + STEP, :]
                factor = measured[s, odd, i : i + STEP, :] * lax.rsqrt(jnp.maximum(fr * fr + fi * fi, 0.0625)) - 1.0
                factor = factor * alive
                for p, value in ((0, fr * factor), (1, fi * factor)):
                    high, low = split(value)
                    zb[odd, 0, p * 128 + i : p * 128 + i + STEP, :] = high
                    zb[odd, 1, p * 128 + i : p * 128 + i + STEP, :] = low
        for odd in range(2):
            freq[odd] = product(table(odd, 0), (zb[odd, 0], zb[odd, 1]))
        for p in range(2):
            e = freq[0, p * 128 : p * 128 + 128, :]
            o = freq[1, p * 128 : p * 128 + 128, :]
            wave[p, 0:128, :] = e + o
            wave[p, 128:256, :] = e - o
        for i in range(0, 256, STEP):
            parts = []
            for odd in range(2):
                mixed = [wave[p, i : i + STEP, odd * 128 : odd * 128 + 128] for p in range(2)]
                parts.append(product(split(jnp.concatenate(mixed, 1)), table(odd, 1)))
            diff = []
            for p in range(2):
                e, o = (parts[odd][:, p * 128 : p * 128 + 128] for odd in range(2))
                diff.append(jnp.concatenate([e + o, e - o], 1))
            dr, di = diff
            pr, pi = probe[0, i : i + STEP, :], probe[1, i : i + STEP, :]
            ore, oim = pat[0, i : i + STEP, :], pat[1, i : i + STEP, :]
            for p, grad in ((0, pr * dr + pi * di), (1, pr * di - pi * dr)):
                first, second = (pltpu.roll(grad[:, j * 128 : j * 128 + 128], turn, 1) for j in range(2))
                moved = (jnp.where(lane >= turn, first, 0.0), jnp.where(lane >= turn, second, first), jnp.where(lane < turn, second, 0.0))
                for j in range(3):
                    at = (p, jnp.minimum(block + j, 3), pl.ds(top + i, STEP))
                    upd[at] = upd[at] + moved[j]
            terms = (ore * dr + oim * di, ore * di - oim * dr, (ore * ore + oim * oim) * alive)
            for lb in range(2):
                for rb in range(STEP // 8):
                    t = lb * 32 + i // 8 + rb
                    for p in range(3):
                        value = terms[p][rb * 8 : rb * 8 + 8, lb * 128 : lb * 128 + 128]
                        pieces[t, p] = value if s == 0 else pieces[t, p] + value


def tile_step(offs, live, ext, probe, seen):
    tables, select = dft_tables()
    out = jax.ShapeDtypeStruct
    vmem = pltpu.VMEM
    return pl.pallas_call(
        tile_kernel,
        out_shape=(out((2, 4, 384, 128), f32), out((64, 3, 8, 128), f32)),
        in_specs=[HBM, HBM] + [VMEM] * 5,
        out_specs=(VMEM,) * 2,
        scratch_shapes=[
            vmem((2, 256, 256), f32),
            vmem((2, 256, 256), f32),
            vmem((2, 256, 256), f32),
            vmem((2, 2, 256, 256), bf16),
            vmem((2, 2, 128, 256), f32),
            pltpu.SMEM((ROWS * 4, COLS), jnp.int32),
            pltpu.SMEM((ROWS, COLS), jnp.int32),
            pltpu.SemaphoreType.DMA((2,)),
        ],
        compiler_params=pltpu.CompilerParams(vmem_limit_bytes=16 << 20),
        cost_estimate=pl.CostEstimate(flops=400000000, bytes_accessed=1 << 20, transcendentals=0),
        name="tile_step",
    )(*(pltpu.with_memory_space_constraint(a, pltpu.MemorySpace.HBM) for a in (offs, live)), ext, probe, seen, jnp.asarray(tables), jnp.asarray(select))


def finish_kernel(d_ref, probe_ref, u_ref, den_ref, spec_ref, spec_out, g, fv, side, fc, rp, s0, r1, s1, r2, s2, r3, wp, rw, r3w, hs, hr, es, er, ps, pr, ss1, rs1, ss2, rs2, ss3, rs3, ss4, rs4, ws, wr, zs, zr, gs, gr, know):
    row = lax.axis_index("row")
    col = lax.axis_index("col")
    core = row % 2
    x = (row // 2) % 4
    y = (row // 8) * 2 + col % 2
    z = col // 2

    def device(core_of, x_of, y_of, z_of):
        return ((y_of // 2) * 8 + x_of * 2 + core_of, z_of * 2 + y_of % 2)

    def peer(axis, d):
        return device(core, jnp.where(axis == 0, (x + d) % 4, x), jnp.where(axis == 0, y, (y + d) % 4), z)

    partner = device(1 - core, x, y, z)
    place = (x, y)
    has = {"l": col > 0, "r": col < COLS - 1, "u": row > 0, "d": row < ROWS - 1}
    beside = {"l": (row, col - 1), "r": (row, col + 1), "u": (row - 1, col), "d": (row + 1, col)}

    barrier = pltpu.get_barrier_semaphore()
    greet(barrier, partner)
    for axis in range(2):
        for d in range(1, 4):
            greet(barrier, peer(axis, d))

    def along(d):
        return device(core, x, y, (z + d) % 16)

    greet(barrier, along(1))
    greet(barrier, along(15))

    def tell(n, d):
        for way in (d, 16 - d):
            pl.semaphore_signal(know.at[n], inc=1, device_id=along(way), device_id_type=MESH)

    for way in "lrud":

        @pl.when(has[way])
        def _():
            greet(barrier, beside[way])

    expected = 9 + sum(has[way].astype(jnp.int32) for way in "lrud")

    for i, way in enumerate("ud"):

        @pl.when(jnp.logical_not(has[way]))
        def _():
            fv[i] = jnp.zeros((2, 4, 128, 128), f32)

    for i, way in enumerate("lr"):

        @pl.when(jnp.logical_not(has[way]))
        def _():
            fc[i] = jnp.zeros((2, 128, 128), f32)

    total = d_ref[0, 2]
    for t in range(1, 64):
        total = total + d_ref[t, 2]
    wp[0] = total
    pl.semaphore_wait(barrier, expected)
    tell(0, 1)

    def vertical(p, part, way, inward=False):
        at = (0, 3, pl.ds(1, 2))[part]
        i = 0 if way == "u" else 1
        there = i if inward else 1 - i
        return remote(u_ref.at[p, at, pl.ds(256 * i, 128)], fv.at[there, p, at], hs.at[p, part, i], hr.at[p, part, there], beside[way])

    def lateral(p, way, inward=False):
        i = 0 if way == "l" else 1
        there = i if inward else 1 - i
        return remote(side.at[i, p], fc.at[there, p], es.at[p, i], er.at[p, there], beside[way])

    base = core * 32
    pending = []

    def go(c):
        c.start()
        pending.append(c)
        return c

    def spot(color, d):
        return color * 16 + ((place[color] + d) % 4) * 4

    near = (2, 1, 3)
    pairs = {}
    for d in near + (0,):
        for color in range(2):
            at = spot(color, d)
            pairs[color, d] = go(remote(d_ref.at[pl.ds((1 - core) * 32 + at, 4)], rp.at[pl.ds(at, 4)], ps.at[color, d], pr.at[color, d], partner))
        if d == 2:
            first = go(remote(wp.at[0], rw.at[0], ws.at[0], wr.at[0], partner))

    pl.semaphore_wait(know.at[0], 2)
    tell(1, 2)

    def join(color, d):
        pairs[color, d].wait_recv()
        at = spot(color, d)
        for b in range(4):
            s0[at + b] = d_ref[base + at + b] + rp[at + b]

    for d in near:
        for color in range(2):
            join(color, d)
    pl.semaphore_wait(know.at[1], 2)
    tell(2, 4)
    one = {}
    for e in near + (0,):
        for d in near:
            for color in range(2):
                b = (place[1 - color] + e) % 4
                one[color, d, e] = go(remote(s0.at[spot(color, d) + b], r1.at[color, d - 1, e], ss1.at[color, d - 1, e], rs1.at[color, d - 1, e], peer(color, d)))
        if e == 2:
            first.wait_recv()
            wp[1] = wp[0] + rw[0]
            waves = [go(remote(wp.at[1], rw.at[d], ws.at[d], wr.at[d], peer(0, d))) for d in range(1, 4)]
    for color in range(2):
        join(color, 0)
    two = {}
    for e in near + (0,):
        for color in range(2):
            b = (place[1 - color] + e) % 4
            for d in near:
                one[color, d, e].wait_recv()
            s1[color, e] = s0[spot(color, 0) + b] + (r1[color, 0, e] + (r1[color, 1, e] + r1[color, 2, e]))
            if e:
                two[color, e] = go(remote(s1.at[color, e], r2.at[color, e - 1], ss2.at[color, e - 1], rs2.at[color, e - 1], peer(1 - color, e)))
        if e == 2:
            for c in waves:
                c.wait_recv()
            wp[2] = wp[1] + (rw[1] + (rw[2] + rw[3]))
            waves = [go(remote(wp.at[2], rw.at[3 + d], ws.at[3 + d], wr.at[3 + d], peer(1, d))) for d in range(1, 4)]
    for part in range(3):
        for p in range(2):
            for way in "ud":

                @pl.when(has[way])
                def _():
                    vertical(p, part, way).start()

    for c in waves:
        c.wait_recv()
    wp[3] = wp[2] + (rw[4] + (rw[5] + rw[6]))
    pl.semaphore_wait(know.at[2], 2)

    def root(color):
        return 2 + 8 * color + 4 * core

    def slot(color):
        return base + color * 16 + jnp.where(color == 0, x * 4 + y, y * 4 + x)

    for color in range(2):
        for e in near:
            two[color, e].wait_recv()
        s2[color] = s1[color, 0] + (r2[color, 0] + (r2[color, 1] + r2[color, 2]))
        goal = root(color)

        @pl.when(z != goal)
        def _():
            at = (z - goal + 16) % 16
            remote(s2.at[color], r3.at[at - 1], zs.at[color, 0], zr.at[0], device(core, x, y, goal)).start()
            remote(wp.at[3], r3w.at[at - 1], zs.at[color, 1], zr.at[1], device(core, x, y, goal)).start()

    for color in range(2):

        @pl.when(z == root(color))
        def _():
            pltpu.make_async_copy(r3, r3, zr.at[0]).wait()
            pltpu.make_async_copy(r3w, r3w, zr.at[1]).wait()
            full = s2[color]
            weight = wp[3]
            for i in range(15):
                full = full + r3[i]
                weight = weight + r3w[i]
            mean = jnp.sum(weight) * (1.0 / 65536.0)
            scale = full[2] + probe_damping * mean
            t = slot(color)
            rows = pl.ds(pl.multiple_of((t % 32) * 8, 8), 8)
            lanes = pl.ds(pl.multiple_of((t // 32) * 128, 128), 128)
            for p in range(2):
                g[t, p] = probe_ref[p, rows, lanes] + full[p] / scale

            def send(i, carry):
                remote(g.at[t], g.at[t], gs.at[i - 1], gr.at[color], device(core, x, y, (z + i) % 16)).start()
                return carry

            lax.fori_loop(1, 16, send, 0)

    for i, (way, at) in enumerate((("l", 0), ("r", 3))):
        for p in range(2):
            for up_down in "ud":

                @pl.when(has[up_down])
                def _():
                    vertical(p, i, up_down, True).wait_recv()

            @pl.when(has[way])
            def _():
                side[i, p] = u_ref[p, at, 128:256, :] + (fv[0, p, at] + fv[1, p, at])
                lateral(p, way).start()

    def away(color):
        d = (z - root(color) + 16) % 16
        return jnp.minimum(d, 16 - d)

    nearer = (away(1) < away(0)).astype(jnp.int32)
    colors = (nearer, 1 - nearer)

    def own(color):
        return jnp.where(color == 0, x, y)

    def cross(color):
        return jnp.where(color == 0, y, x)

    def tile_at(color, a, b):
        return base + color * 16 + (a % 4) * 4 + b % 4

    three = {}
    four = {}
    for n, color in enumerate(colors):
        t = slot(color)

        @pl.when(z != root(color))
        def _():
            pltpu.make_async_copy(g.at[t], g.at[t], gr.at[color]).wait()

        for d in near:
            three[n, d] = go(remote(g.at[t], g.at[t], ss3.at[color, d - 1], rs3.at[color, d - 1], peer(1 - color, d)))
        for d in near:
            four[n, d, 0] = go(remote(g.at[t], g.at[t], ss4.at[color, d - 1, 0], rs4.at[color, d - 1, 0], peer(color, d)))
    last = []
    for n, color in enumerate(colors):
        for e in (1, 3, 2):
            three[n, e].wait_recv()
            t = tile_at(color, own(color), cross(color) - e + 4)
            for d in near:
                four[n, d, e] = go(remote(g.at[t], g.at[t], ss4.at[color, d - 1, e], rs4.at[color, d - 1, e], peer(color, d)))
        group = g.at[pl.ds(tile_at(color, own(color), 0), 4)]
        last.append(go(remote(group, group, ps.at[2 + n, 0], pr.at[2 + n, 0], partner)))
    for n, color in enumerate(colors):
        for d in (1, 3, 2):
            for e in range(4):
                four[n, d, e].wait_recv()
            group = g.at[pl.ds(tile_at(color, own(color) - d + 4, 0), 4)]
            last.append(go(remote(group, group, ps.at[2 + n, d], pr.at[2 + n, d], partner)))
    for p in range(2):
        for way in "ud":

            @pl.when(has[way])
            def _():
                vertical(p, 2, way, True).wait_recv()

        for way in "lr":

            @pl.when(has[way])
            def _():
                lateral(p, way, True).wait_recv()

        for i in range(2):
            at = 1 + i
            update = u_ref[p, at, 128:256, :] + (fv[0, p, at] + fv[1, p, at]) + fc[i, p]
            lanes = slice(i * 128, i * 128 + 128)
            spec_out[p, :, lanes] = spec_ref[p, :, lanes] + update / den_ref[:, lanes]
    for c in last:
        c.wait_recv()
    for c in pending:
        c.wait_send()
    for p in range(2):
        for way in "ud":

            @pl.when(has[way])
            def _():
                for part in range(3):
                    vertical(p, part, way).wait_send()

        for way in "lr":

            @pl.when(has[way])
            def _():
                lateral(p, way).wait_send()

    for color in range(2):

        @pl.when(z != root(color))
        def _():
            pltpu.make_async_copy(s2.at[color], s2.at[color], zs.at[color, 0]).wait()
            pltpu.make_async_copy(wp.at[3], wp.at[3], zs.at[color, 1]).wait()

        @pl.when(z == root(color))
        def _():
            t = slot(color)

            def done(i, carry):
                pltpu.make_async_copy(g.at[t], g.at[t], gs.at[i]).wait()
                return carry

            lax.fori_loop(0, 15, done, 0)


def finish(upd, pieces, den, specimen, probe_field):
    tile = (8, 128)
    dma = pltpu.SemaphoreType.DMA

    def vmem(*shape):
        return pltpu.VMEM(shape, f32)

    return pl.pallas_call(
        finish_kernel,
        out_shape=(jax.ShapeDtypeStruct((2, 128, 256), f32), jax.ShapeDtypeStruct((64, 2, 8, 128), f32)),
        in_specs=[VMEM] * 5,
        out_specs=(VMEM,) * 2,
        scratch_shapes=[
            vmem(2, 2, 4, 128, 128),
            vmem(2, 2, 128, 128),
            vmem(2, 2, 128, 128),
            vmem(32, 3, *tile),
            vmem(32, 3, *tile),
            vmem(2, 3, 4, 3, *tile),
            vmem(2, 4, 3, *tile),
            vmem(2, 3, 3, *tile),
            vmem(2, 3, *tile),
            vmem(15, 3, *tile),
            vmem(4, *tile),
            vmem(7, *tile),
            vmem(15, *tile),
            dma((2, 3, 2)),
            dma((2, 3, 2)),
            dma((2, 2)),
            dma((2, 2)),
            dma((4, 4)),
            dma((4, 4)),
            dma((2, 3, 4)),
            dma((2, 3, 4)),
            dma((2, 3)),
            dma((2, 3)),
            dma((2, 3)),
            dma((2, 3)),
            dma((2, 3, 4)),
            dma((2, 3, 4)),
            dma((7,)),
            dma((7,)),
            dma((2, 2)),
            dma((2,)),
            dma((15,)),
            dma((2,)),
            pltpu.SemaphoreType.REGULAR((3,)),
        ],
        compiler_params=pltpu.CompilerParams(collective_id=0, has_side_effects=True, vmem_limit_bytes=16 << 20),
        cost_estimate=pl.CostEstimate(flops=1000000000, bytes_accessed=1 << 20, transcendentals=0),
        name="finish",
    )(pieces, probe_field, upd, den, specimen)


def write_kernel(spec_ref, g_ref, spec_out, probe_out):
    spec_out[...] = spec_ref[...]
    for lb in range(2):
        for rb in range(32):
            for p in range(2):
                probe_out[p, rb * 8 : rb * 8 + 8, lb * 128 : lb * 128 + 128] = g_ref[lb * 32 + rb, p]


def write(specimen_next, probe_tiles):
    return pl.pallas_call(
        write_kernel,
        out_shape=(jax.ShapeDtypeStruct((2, 128, 256), f32), jax.ShapeDtypeStruct((2, 256, 256), f32)),
        in_specs=[VMEM] * 2,
        out_specs=(VMEM,) * 2,
        compiler_params=pltpu.CompilerParams(vmem_limit_bytes=8 << 20),
        name="write",
    )(specimen_next, probe_tiles)


def shards(specimen, probe_field, scan_offsets, live_counts, magnitudes):
    offs = scan_offsets.transpose(0, 2, 3, 1).reshape(ROWS * 4, COLS)
    ext, den, probe, seen = halo(offs, live_counts, specimen, probe_field, magnitudes)
    upd, pieces = tile_step(offs, live_counts, ext, probe, seen)
    return write(*finish(upd, pieces, den, specimen, probe))


def solution(mesh):
    return jax.shard_map(
        shards,
        mesh=mesh,
        in_specs=(P(None, "row", "col"), P(), P(), P(), P("row", "col", None, None, None)),
        out_specs=(P(None, "row", "col"), P()),
        check_vma=False,
    )
```

```python
import math

import jax
import jax.numpy as jnp
import numpy as np
from jax import lax
from jax.experimental import pallas as pl
from jax.experimental.pallas import tpu as pltpu
from jax.sharding import PartitionSpec as P

MESH = pl.DeviceIdType.MESH
ROWS = 16
COLS = 32
object_damping = 0.1
probe_damping = 0.1
f32 = jnp.float32
bf16 = jnp.bfloat16
VMEM = pl.BlockSpec(memory_space=pltpu.VMEM)
HBM = pl.BlockSpec(memory_space=pltpu.MemorySpace.HBM)
SMEM = pl.BlockSpec(memory_space=pltpu.SMEM)


def remote(src, dst, send, recv, where):
    return pltpu.make_async_remote_copy(src_ref=src, dst_ref=dst, send_sem=send, recv_sem=recv, device_id=where, device_id_type=MESH)


def greet(barrier, where):
    pl.semaphore_signal(barrier, inc=1, device_id=where, device_id_type=MESH)

STEP = 64


def split(value):
    high = value.astype(bf16)
    return high, (value - high.astype(f32)).astype(bf16)


def halo_kernel(offs_hbm, live_hbm, tile_ref, probe_hbm, mags, select_hbm, ext, den, probe, measured, select, padded, seen, offs, live, own, fetch, cs, cr, vs, vr):
    row = lax.axis_index("row")
    col = lax.axis_index("col")
    has = {"l": col > 0, "r": col < COLS - 1, "u": row > 0, "d": row < ROWS - 1}
    to = {"l": (row, col - 1), "r": (row, col + 1), "u": (row - 1, col), "d": (row + 1, col)}
    center = [pltpu.make_async_copy(tile_ref.at[:, :, pl.ds(j * 128, 128)], ext.at[:, 1 + j, pl.ds(128, 128), :], own.at[j]) for j in range(2)]
    for c in center:
        c.start()
    small = [pltpu.make_async_copy(a, b, fetch.at[i]) for i, (a, b) in enumerate(((offs_hbm, offs), (live_hbm, live), (probe_hbm, probe)))]
    for c in small:
        c.start()
    shown = [pltpu.make_async_copy(mags.at[0, 0, s, :, pl.ds(j * 128, 128)], seen.at[s, j], fetch.at[3 + 2 * s + j]) for s in range(2) for j in range(2)]
    shown.append(pltpu.make_async_copy(select_hbm, select, fetch.at[7]))
    barrier = pltpu.get_barrier_semaphore()
    for side in "lrud":

        @pl.when(has[side])
        def _():
            greet(barrier, to[side])

    expected = sum(has[side].astype(jnp.int32) for side in "lrud")

    @pl.when(row == 0)
    def _():
        ext[:, :, 0:128, :] = jnp.zeros((2, 4, 128, 128), f32)

    @pl.when(row == ROWS - 1)
    def _():
        ext[:, :, 256:384, :] = jnp.zeros((2, 4, 128, 128), f32)

    @pl.when(col == 0)
    def _():
        ext[:, 0] = jnp.zeros((2, 384, 128), f32)

    @pl.when(col == COLS - 1)
    def _():
        ext[:, 3] = jnp.zeros((2, 384, 128), f32)

    for c in center:
        c.wait()
    pl.semaphore_wait(barrier, expected)

    def across(p, side):
        mine, theirs = (1, 3) if side == "l" else (2, 0)
        i = 0 if side == "l" else 1
        return remote(ext.at[p, mine, pl.ds(128, 128)], ext.at[p, theirs, pl.ds(128, 128)], cs.at[p, i], cr.at[p, i], to[side])

    def up_down(p, side, part):
        at = (pl.ds(1, 2), 0, 3)[part]
        i, theirs = (0, 256) if side == "u" else (1, 0)
        return remote(ext.at[p, at, pl.ds(128, 128)], ext.at[p, at, pl.ds(theirs, 128)], vs.at[p, part, i], vr.at[p, part, i], to[side])

    for p in range(2):
        for side in "lr":

            @pl.when(has[side])
            def _():
                across(p, side).start()

    for p in range(2):
        for side in "ud":

            @pl.when(has[side])
            def _():
                up_down(p, side, 0).start()

    for c in shown:
        c.start()
    for c in small:
        c.wait()
    padded[...] = jnp.zeros_like(padded)
    peak = jnp.zeros((8, 128), f32)
    for i in range(0, 256, STEP):
        power = probe[0, i : i + STEP, :] * probe[0, i : i + STEP, :] + probe[1, i : i + STEP, :] * probe[1, i : i + STEP, :]
        for j in range(2):
            padded[2 + j, 128 + i : 128 + i + STEP, :] = power[:, j * 128 : j * 128 + 128]
        for a in range(0, STEP, 8):
            for b in range(0, 256, 128):
                peak = jnp.maximum(peak, power[a : a + 8, b : b + 128])
    den[...] = jnp.full((128, 256), object_damping, f32) * jnp.max(peak)

    def add(n, carry):
        da = n // 6 - 1
        db = (n // 2) % 3 - 1
        s = n % 2
        a = row + da
        b = col + db
        inside = (a >= 0) & (a < ROWS) & (b >= 0) & (b < COLS)
        a = jnp.clip(a, 0, ROWS - 1)
        b = jnp.clip(b, 0, COLS - 1)
        down = da * 128 + offs[(a * 2 + s) * 2, b]
        across = db * 256 + offs[(a * 2 + s) * 2 + 1, b]
        on = (inside & (s < live[a, b]) & (across > -256) & (across < 256)).astype(f32)
        across = jnp.clip(across, -256, 255)
        turn = (across + 256) % 128
        block = 4 - (across + 256) // 128
        lane = lax.broadcasted_iota(jnp.int32, (STEP, 128), 1)
        for i in range(0, 128, STEP):
            rolled = [pltpu.roll(padded[block + j - 1, pl.ds(i + 128 - down, STEP), :], turn, 1) for j in range(3)]
            for j in range(2):
                den[i : i + STEP, j * 128 : j * 128 + 128] += on * jnp.where(lane >= turn, rolled[j + 1], rolled[j])

        return carry

    lax.fori_loop(0, 18, add, 0)
    for c in shown:
        c.wait()
    for s in range(2):
        for odd in range(2):
            for i in range(0, 128, STEP):
                mh, ml = split(jnp.concatenate([seen[s, j, pl.ds(odd + 2 * i, STEP, stride=2), :] for j in range(2)], 1))
                measured[s, odd, i : i + STEP, :] = jnp.dot(mh, select[...], preferred_element_type=f32) + jnp.dot(ml, select[...], preferred_element_type=f32)

    for p in range(2):
        for side, part in (("l", 1), ("r", 2)):

            @pl.when(has[side])
            def _():
                across(p, "r" if side == "l" else "l").wait_recv()
                for way in "ud":

                    @pl.when(has[way])
                    def _():
                        up_down(p, way, part).start()

    for p in range(2):
        for side in "lr":

            @pl.when(has[side])
            def _():
                across(p, side).wait_send()

        for way, back in (("u", "d"), ("d", "u")):
            for part, need in ((0, None), (1, "l"), (2, "r")):
                cond = has[way] if need is None else jnp.logical_and(has[way], has[need])

                @pl.when(cond)
                def _():
                    up_down(p, way, part).wait_send()
                    up_down(p, back, part).wait_recv()


def halo(offs, live, tile, probe, mags, select):
    dma = pltpu.SemaphoreType.DMA
    return pl.pallas_call(
        halo_kernel,
        out_shape=(jax.ShapeDtypeStruct((2, 4, 384, 128), f32), jax.ShapeDtypeStruct((128, 256), f32), jax.ShapeDtypeStruct((2, 256, 256), f32), jax.ShapeDtypeStruct((2, 2, 128, 256), f32)),
        in_specs=[HBM] * 6,
        out_specs=(VMEM,) * 4,
        scratch_shapes=[pltpu.VMEM((256, 256), bf16), pltpu.VMEM((6, 512, 128), f32), pltpu.VMEM((2, 2, 256, 128), f32), pltpu.SMEM((ROWS * 4, COLS), jnp.int32), pltpu.SMEM((ROWS, COLS), jnp.int32), dma((2,)), dma((8,)), dma((2, 2)), dma((2, 2)), dma((2, 3, 2)), dma((2, 3, 2))],
        compiler_params=pltpu.CompilerParams(collective_id=1, has_side_effects=True, vmem_limit_bytes=8 << 20),
        cost_estimate=pl.CostEstimate(flops=400000000, bytes_accessed=1 << 20, transcendentals=0),
        name="halo",
    )(*(pltpu.with_memory_space_constraint(a, pltpu.MemorySpace.HBM) for a in (offs, live, tile, probe, mags, select)))


def dft_tables():
    m = np.arange(128)[:, None]
    k = np.arange(128)[None, :]
    tables = []
    for odd in range(2):
        angle = ((m * (2 * k + odd)) % 256) * (2.0 * math.pi / 256)
        c, s = np.cos(angle) / 16, np.sin(angle) / 16
        full = np.block([[c, -s], [s, c]])
        for t in (full, full.T):
            high = t.astype(np.float32).astype(jnp.bfloat16)
            low = (t - high.astype(np.float64)).astype(np.float32).astype(jnp.bfloat16)
            tables += [high, low]
    order = np.concatenate([np.arange(0, 256, 2), np.arange(1, 256, 2)])
    select = (np.arange(256)[:, None] == order[None, :]).astype(jnp.bfloat16)
    return np.stack(tables).reshape(2, 2, 2, 256, 256), select


def product(a, b):
    def dot(u, v):
        return jnp.dot(u, v, preferred_element_type=f32)

    return dot(a[0], b[0]) + (dot(a[1], b[0]) + dot(a[0], b[1]))


def tile_work(offs, live, ext, probe, measured, tables, upd, pieces, pat, wave, freq, zb, placed):
    row = lax.axis_index("row")
    col = lax.axis_index("col")
    lane = lax.broadcasted_iota(jnp.int32, (STEP, 128), 1)

    def table(odd, turned):
        return tables[odd, turned, 0], tables[odd, turned, 1]

    top = [offs[(row * 2 + s) * 2, col] + 128 for s in range(2)]
    left = [offs[(row * 2 + s) * 2 + 1, col] + 128 for s in range(2)]
    turn = [a % 128 for a in left]
    block = [a // 128 for a in left]
    alive = [(s < live[row, col]).astype(f32) for s in range(2)]
    for s in range(2):
        for i in range(0, 256, STEP):
            got = []
            for p in range(2):
                rolled = [pltpu.roll(ext[p, jnp.minimum(block[s] + j, 3), pl.ds(top[s] + i, STEP), :], 128 - turn[s], 1) for j in range(3)]
                halves = [jnp.where(lane < 128 - turn[s], rolled[j], rolled[j + 1]) for j in range(2)]
                got.append(jnp.concatenate(halves, 1))
                pat[s, p, i : i + STEP, :] = got[p]
            pr, pi = probe[0, i : i + STEP, :], probe[1, i : i + STEP, :]
            wr = pr * got[0] - pi * got[1]
            wi = pr * got[1] + pi * got[0]
            for odd in range(2):
                if odd:
                    mixed = [w[:, :128] - w[:, 128:] for w in (wr, wi)]
                else:
                    mixed = [w[:, :128] + w[:, 128:] for w in (wr, wi)]
                out = product(split(jnp.concatenate(mixed, 1)), table(odd, 0))
                for p in range(2):
                    wave[s, p, i : i + STEP, odd * 128 : odd * 128 + 128] = out[:, p * 128 : p * 128 + 128]
    for odd in range(2):
        for s in range(2):
            if odd:
                mixed = [wave[s, p, 0:128, :] - wave[s, p, 128:256, :] for p in range(2)]
            else:
                mixed = [wave[s, p, 0:128, :] + wave[s, p, 128:256, :] for p in range(2)]
            freq[s, odd] = product(table(odd, 1), split(jnp.concatenate(mixed, 0)))
    for odd in range(2):
        for s in range(2):
            for i in range(0, 128, STEP):
                fr = freq[s, odd, i : i + STEP, :]
                fi = freq[s, odd, 128 + i : 128 + i + STEP, :]
                factor = measured[s, odd, i : i + STEP, :] * lax.rsqrt(jnp.maximum(fr * fr + fi * fi, 0.0625)) - 1.0
                factor = factor * alive[s]
                for p, value in ((0, fr * factor), (1, fi * factor)):
                    high, low = split(value)
                    zb[s, odd, 0, p * 128 + i : p * 128 + i + STEP, :] = high
                    zb[s, odd, 1, p * 128 + i : p * 128 + i + STEP, :] = low
    for odd in range(2):
        for s in range(2):
            freq[s, odd] = product(table(odd, 0), (zb[s, odd, 0], zb[s, odd, 1]))
    for s in range(2):
        for p in range(2):
            e = freq[s, 0, p * 128 : p * 128 + 128, :]
            o = freq[s, 1, p * 128 : p * 128 + 128, :]
            wave[s, p, 0:128, :] = e + o
            wave[s, p, 128:256, :] = e - o
    for s in range(2):
        for i in range(0, 256, STEP):
            parts = []
            for odd in range(2):
                mixed = [wave[s, p, i : i + STEP, odd * 128 : odd * 128 + 128] for p in range(2)]
                parts.append(product(split(jnp.concatenate(mixed, 1)), table(odd, 1)))
            diff = []
            for p in range(2):
                e, o = (parts[odd][:, p * 128 : p * 128 + 128] for odd in range(2))
                diff.append(jnp.concatenate([e + o, e - o], 1))
            dr, di = diff
            pr, pi = probe[0, i : i + STEP, :], probe[1, i : i + STEP, :]
            ore, oim = pat[s, 0, i : i + STEP, :], pat[s, 1, i : i + STEP, :]
            for p, grad in ((0, pr * dr + pi * di), (1, pr * di - pi * dr)):
                first, second = (pltpu.roll(grad[:, j * 128 : j * 128 + 128], turn[s], 1) for j in range(2))
                moved = (jnp.where(lane >= turn[s], first, 0.0), jnp.where(lane >= turn[s], second, first), jnp.where(lane < turn[s], second, 0.0))
                for j in range(3):
                    placed[s, p, j, 128 + i : 128 + i + STEP, :] = moved[j]
            terms = (ore * dr + oim * di, ore * di - oim * dr, (ore * ore + oim * oim) * alive[s])
            for lb in range(2):
                for rb in range(STEP // 8):
                    t = lb * 32 + i // 8 + rb
                    for p in range(3):
                        value = terms[p][rb * 8 : rb * 8 + 8, lb * 128 : lb * 128 + 128]
                        pieces[t, p] = value if s == 0 else pieces[t, p] + value
    for k in range(4):
        here = [k - block[s] for s in range(2)]
        weight = [((a >= 0) & (a <= 2)).astype(f32) for a in here]
        here = [jnp.clip(a, 0, 2) for a in here]
        for p in range(2):
            for i in range(0, 384, STEP):
                got = [placed[s, p, here[s], pl.ds(128 + i - top[s], STEP), :] * weight[s] for s in range(2)]
                upd[p, k, i : i + STEP, :] = got[0] + got[1]


def finish_kernel(offs_hbm, live_hbm, ext, probe_ref, measured, tables, den_ref, spec_ref, spec_out, g, d_ref, u_ref, pat, wave, freq, zb, placed, offs, live, fetch, fv, side, fc, rp, s0, r1, s1, r2, s2, r3, wp, rw, r3w, hs, hr, es, er, ps, pr, ss1, rs1, ss2, rs2, ss3, rs3, ss4, rs4, ws, wr, zs, zr, gs, gr, know):
    row = lax.axis_index("row")
    col = lax.axis_index("col")
    core = row % 2
    x = (row // 2) % 4
    y = (row // 8) * 2 + col % 2
    z = col // 2

    def device(core_of, x_of, y_of, z_of):
        return ((y_of // 2) * 8 + x_of * 2 + core_of, z_of * 2 + y_of % 2)

    def peer(axis, d):
        return device(core, jnp.where(axis == 0, (x + d) % 4, x), jnp.where(axis == 0, y, (y + d) % 4), z)

    partner = device(1 - core, x, y, z)
    place = (x, y)
    has = {"l": col > 0, "r": col < COLS - 1, "u": row > 0, "d": row < ROWS - 1}
    beside = {"l": (row, col - 1), "r": (row, col + 1), "u": (row - 1, col), "d": (row + 1, col)}

    small = [pltpu.make_async_copy(a, b, fetch.at[i]) for i, (a, b) in enumerate(((offs_hbm, offs), (live_hbm, live)))]
    for c in small:
        c.start()
    barrier = pltpu.get_barrier_semaphore()
    greet(barrier, partner)
    for axis in range(2):
        for d in range(1, 4):
            greet(barrier, peer(axis, d))

    def along(d):
        return device(core, x, y, (z + d) % 16)

    greet(barrier, along(1))
    greet(barrier, along(15))

    def tell(n, d):
        for way in (d, 16 - d):
            pl.semaphore_signal(know.at[n], inc=1, device_id=along(way), device_id_type=MESH)

    for way in "lrud":

        @pl.when(has[way])
        def _():
            greet(barrier, beside[way])

    expected = 9 + sum(has[way].astype(jnp.int32) for way in "lrud")

    for i, way in enumerate("ud"):

        @pl.when(jnp.logical_not(has[way]))
        def _():
            fv[i] = jnp.zeros((2, 4, 128, 128), f32)

    for i, way in enumerate("lr"):

        @pl.when(jnp.logical_not(has[way]))
        def _():
            fc[i] = jnp.zeros((2, 128, 128), f32)

    placed[:, :, :, 0:128, :] = jnp.zeros((2, 2, 3, 128, 128), f32)
    placed[:, :, :, 384:512, :] = jnp.zeros((2, 2, 3, 128, 128), f32)
    for c in small:
        c.wait()
    tile_work(offs, live, ext, probe_ref, measured, tables, u_ref, d_ref, pat, wave, freq, zb, placed)
    total = d_ref[0, 2]
    for t in range(1, 64):
        total = total + d_ref[t, 2]
    wp[0] = total
    pl.semaphore_wait(barrier, expected)
    tell(0, 1)

    def vertical(p, part, way, inward=False):
        at = (0, 3, pl.ds(1, 2))[part]
        i = 0 if way == "u" else 1
        there = i if inward else 1 - i
        return remote(u_ref.at[p, at, pl.ds(256 * i, 128)], fv.at[there, p, at], hs.at[p, part, i], hr.at[p, part, there], beside[way])

    def lateral(p, way, inward=False):
        i = 0 if way == "l" else 1
        there = i if inward else 1 - i
        return remote(side.at[i, p], fc.at[there, p], es.at[p, i], er.at[p, there], beside[way])

    base = core * 32
    pending = []

    def go(c):
        c.start()
        pending.append(c)
        return c

    def spot(color, d):
        return color * 16 + ((place[color] + d) % 4) * 4

    near = (2, 1, 3)
    pairs = {}
    for d in near + (0,):
        for color in range(2):
            at = spot(color, d)
            pairs[color, d] = go(remote(d_ref.at[pl.ds((1 - core) * 32 + at, 4)], rp.at[pl.ds(at, 4)], ps.at[color, d], pr.at[color, d], partner))
        if d == 2:
            first = go(remote(wp.at[0], rw.at[0], ws.at[0], wr.at[0], partner))

    pl.semaphore_wait(know.at[0], 2)
    tell(1, 2)

    def join(color, d):
        pairs[color, d].wait_recv()
        at = spot(color, d)
        for b in range(4):
            s0[at + b] = d_ref[base + at + b] + rp[at + b]

    for d in near:
        for color in range(2):
            join(color, d)
    pl.semaphore_wait(know.at[1], 2)
    tell(2, 4)
    one = {}
    for e in near + (0,):
        for d in near:
            for color in range(2):
                b = (place[1 - color] + e) % 4
                one[color, d, e] = go(remote(s0.at[spot(color, d) + b], r1.at[color, d - 1, e], ss1.at[color, d - 1, e], rs1.at[color, d - 1, e], peer(color, d)))
        if e == 2:
            first.wait_recv()
            wp[1] = wp[0] + rw[0]
            waves = [go(remote(wp.at[1], rw.at[d], ws.at[d], wr.at[d], peer(0, d))) for d in range(1, 4)]
    for color in range(2):
        join(color, 0)
    two = {}
    for e in near + (0,):
        for color in range(2):
            b = (place[1 - color] + e) % 4
            for d in near:
                one[color, d, e].wait_recv()
            s1[color, e] = s0[spot(color, 0) + b] + (r1[color, 0, e] + (r1[color, 1, e] + r1[color, 2, e]))
            if e:
                two[color, e] = go(remote(s1.at[color, e], r2.at[color, e - 1], ss2.at[color, e - 1], rs2.at[color, e - 1], peer(1 - color, e)))
        if e == 2:
            for c in waves:
                c.wait_recv()
            wp[2] = wp[1] + (rw[1] + (rw[2] + rw[3]))
            waves = [go(remote(wp.at[2], rw.at[3 + d], ws.at[3 + d], wr.at[3 + d], peer(1, d))) for d in range(1, 4)]
    for part in range(3):
        for p in range(2):
            for way in "ud":

                @pl.when(has[way])
                def _():
                    vertical(p, part, way).start()

    for c in waves:
        c.wait_recv()
    wp[3] = wp[2] + (rw[4] + (rw[5] + rw[6]))
    pl.semaphore_wait(know.at[2], 2)

    def root(color):
        return 2 + 8 * color + 4 * core

    def slot(color):
        return base + color * 16 + jnp.where(color == 0, x * 4 + y, y * 4 + x)

    for color in range(2):
        for e in near:
            two[color, e].wait_recv()
        s2[color] = s1[color, 0] + (r2[color, 0] + (r2[color, 1] + r2[color, 2]))
        goal = root(color)

        @pl.when(z != goal)
        def _():
            at = (z - goal + 16) % 16
            remote(s2.at[color], r3.at[at - 1], zs.at[color, 0], zr.at[0], device(core, x, y, goal)).start()
            remote(wp.at[3], r3w.at[at - 1], zs.at[color, 1], zr.at[1], device(core, x, y, goal)).start()

    for color in range(2):

        @pl.when(z == root(color))
        def _():
            pltpu.make_async_copy(r3, r3, zr.at[0]).wait()
            pltpu.make_async_copy(r3w, r3w, zr.at[1]).wait()
            full = s2[color]
            weight = wp[3]
            for i in range(15):
                full = full + r3[i]
                weight = weight + r3w[i]
            mean = jnp.sum(weight) * (1.0 / 65536.0)
            scale = full[2] + probe_damping * mean
            t = slot(color)
            rows = pl.ds(pl.multiple_of((t % 32) * 8, 8), 8)
            lanes = pl.ds(pl.multiple_of((t // 32) * 128, 128), 128)
            for p in range(2):
                g[t, p] = probe_ref[p, rows, lanes] + full[p] / scale

            def send(i, carry):
                remote(g.at[t], g.at[t], gs.at[i - 1], gr.at[color], device(core, x, y, (z + i) % 16)).start()
                return carry

            lax.fori_loop(1, 16, send, 0)

    for i, (way, at) in enumerate((("l", 0), ("r", 3))):
        for p in range(2):
            for up_down in "ud":

                @pl.when(has[up_down])
                def _():
                    vertical(p, i, up_down, True).wait_recv()

            @pl.when(has[way])
            def _():
                side[i, p] = u_ref[p, at, 128:256, :] + (fv[0, p, at] + fv[1, p, at])
                lateral(p, way).start()

    def away(color):
        d = (z - root(color) + 16) % 16
        return jnp.minimum(d, 16 - d)

    nearer = (away(1) < away(0)).astype(jnp.int32)
    colors = (nearer, 1 - nearer)

    def own(color):
        return jnp.where(color == 0, x, y)

    def cross(color):
        return jnp.where(color == 0, y, x)

    def tile_at(color, a, b):
        return base + color * 16 + (a % 4) * 4 + b % 4

    three = {}
    four = {}
    for n, color in enumerate(colors):
        t = slot(color)

        @pl.when(z != root(color))
        def _():
            pltpu.make_async_copy(g.at[t], g.at[t], gr.at[color]).wait()

        for d in near:
            three[n, d] = go(remote(g.at[t], g.at[t], ss3.at[color, d - 1], rs3.at[color, d - 1], peer(1 - color, d)))
        for d in near:
            four[n, d, 0] = go(remote(g.at[t], g.at[t], ss4.at[color, d - 1, 0], rs4.at[color, d - 1, 0], peer(color, d)))
    last = []
    for n, color in enumerate(colors):
        for e in (1, 3, 2):
            three[n, e].wait_recv()
            t = tile_at(color, own(color), cross(color) - e + 4)
            for d in near:
                four[n, d, e] = go(remote(g.at[t], g.at[t], ss4.at[color, d - 1, e], rs4.at[color, d - 1, e], peer(color, d)))
        group = g.at[pl.ds(tile_at(color, own(color), 0), 4)]
        last.append(go(remote(group, group, ps.at[2 + n, 0], pr.at[2 + n, 0], partner)))
    for n, color in enumerate(colors):
        for d in (1, 3, 2):
            for e in range(4):
                four[n, d, e].wait_recv()
            group = g.at[pl.ds(tile_at(color, own(color) - d + 4, 0), 4)]
            last.append(go(remote(group, group, ps.at[2 + n, d], pr.at[2 + n, d], partner)))
    for p in range(2):
        for way in "ud":

            @pl.when(has[way])
            def _():
                vertical(p, 2, way, True).wait_recv()

        for way in "lr":

            @pl.when(has[way])
            def _():
                lateral(p, way, True).wait_recv()

        for i in range(2):
            at = 1 + i
            update = u_ref[p, at, 128:256, :] + (fv[0, p, at] + fv[1, p, at]) + fc[i, p]
            lanes = slice(i * 128, i * 128 + 128)
            spec_out[p, :, lanes] = spec_ref[p, :, lanes] + update / den_ref[:, lanes]
    for c in last:
        c.wait_recv()
    for c in pending:
        c.wait_send()
    for p in range(2):
        for way in "ud":

            @pl.when(has[way])
            def _():
                for part in range(3):
                    vertical(p, part, way).wait_send()

        for way in "lr":

            @pl.when(has[way])
            def _():
                lateral(p, way).wait_send()

    for color in range(2):

        @pl.when(z != root(color))
        def _():
            pltpu.make_async_copy(s2.at[color], s2.at[color], zs.at[color, 0]).wait()
            pltpu.make_async_copy(wp.at[3], wp.at[3], zs.at[color, 1]).wait()

        @pl.when(z == root(color))
        def _():
            t = slot(color)

            def done(i, carry):
                pltpu.make_async_copy(g.at[t], g.at[t], gs.at[i]).wait()
                return carry

            lax.fori_loop(0, 15, done, 0)


def finish(offs, live, ext, probe, measured, tables, den, specimen):
    tile = (8, 128)
    dma = pltpu.SemaphoreType.DMA

    def vmem(*shape):
        return pltpu.VMEM(shape, f32)

    return pl.pallas_call(
        finish_kernel,
        out_shape=(jax.ShapeDtypeStruct((2, 128, 256), f32), jax.ShapeDtypeStruct((64, 2, 8, 128), f32)),
        in_specs=[HBM] * 2 + [VMEM] * 6,
        out_specs=(VMEM,) * 2,
        scratch_shapes=[
            vmem(64, 3, *tile),
            vmem(2, 4, 384, 128),
            vmem(2, 2, 256, 256),
            vmem(2, 2, 256, 256),
            vmem(2, 2, 256, 256),
            pltpu.VMEM((2, 2, 2, 256, 256), bf16),
            vmem(2, 2, 3, 512, 128),
            pltpu.SMEM((ROWS * 4, COLS), jnp.int32),
            pltpu.SMEM((ROWS, COLS), jnp.int32),
            dma((2,)),
            vmem(2, 2, 4, 128, 128),
            vmem(2, 2, 128, 128),
            vmem(2, 2, 128, 128),
            vmem(32, 3, *tile),
            vmem(32, 3, *tile),
            vmem(2, 3, 4, 3, *tile),
            vmem(2, 4, 3, *tile),
            vmem(2, 3, 3, *tile),
            vmem(2, 3, *tile),
            vmem(15, 3, *tile),
            vmem(4, *tile),
            vmem(7, *tile),
            vmem(15, *tile),
            dma((2, 3, 2)),
            dma((2, 3, 2)),
            dma((2, 2)),
            dma((2, 2)),
            dma((4, 4)),
            dma((4, 4)),
            dma((2, 3, 4)),
            dma((2, 3, 4)),
            dma((2, 3)),
            dma((2, 3)),
            dma((2, 3)),
            dma((2, 3)),
            dma((2, 3, 4)),
            dma((2, 3, 4)),
            dma((7,)),
            dma((7,)),
            dma((2, 2)),
            dma((2,)),
            dma((15,)),
            dma((2,)),
            pltpu.SemaphoreType.REGULAR((3,)),
        ],
        compiler_params=pltpu.CompilerParams(collective_id=0, has_side_effects=True, vmem_limit_bytes=32 << 20),
        cost_estimate=pl.CostEstimate(flops=1000000000, bytes_accessed=1 << 20, transcendentals=0),
        name="finish",
    )(*(pltpu.with_memory_space_constraint(a, pltpu.MemorySpace.HBM) for a in (offs, live)), ext, probe, measured, tables, den, specimen)


def write_kernel(spec_ref, g_ref, spec_out, probe_out):
    spec_out[...] = spec_ref[...]
    for lb in range(2):
        for rb in range(32):
            for p in range(2):
                probe_out[p, rb * 8 : rb * 8 + 8, lb * 128 : lb * 128 + 128] = g_ref[lb * 32 + rb, p]


def write(specimen_next, probe_tiles):
    return pl.pallas_call(
        write_kernel,
        out_shape=(jax.ShapeDtypeStruct((2, 128, 256), f32), jax.ShapeDtypeStruct((2, 256, 256), f32)),
        in_specs=[VMEM] * 2,
        out_specs=(VMEM,) * 2,
        compiler_params=pltpu.CompilerParams(vmem_limit_bytes=8 << 20),
        name="write",
    )(specimen_next, probe_tiles)


def shards(specimen, probe_field, scan_offsets, live_counts, magnitudes):
    offs = scan_offsets.transpose(0, 2, 3, 1).reshape(ROWS * 4, COLS)
    tables, select = (jnp.asarray(a) for a in dft_tables())
    ext, den, probe, measured = halo(offs, live_counts, specimen, probe_field, magnitudes, select)
    return write(*finish(offs, live_counts, ext, probe, measured, tables, den, specimen))


def solution(mesh):
    return jax.shard_map(
        shards,
        mesh=mesh,
        in_specs=(P(None, "row", "col"), P(), P(), P(), P("row", "col", None, None, None)),
        out_specs=(P(None, "row", "col"), P()),
        check_vma=False,
    )
```

```python
import math

import jax
import jax.numpy as jnp
import numpy as np
from jax import lax
from jax.experimental import pallas as pl
from jax.experimental.pallas import tpu as pltpu
from jax.sharding import PartitionSpec as P

MESH = pl.DeviceIdType.MESH
ROWS = 16
COLS = 32
object_damping = 0.1
probe_damping = 0.1
f32 = jnp.float32
bf16 = jnp.bfloat16
VMEM = pl.BlockSpec(memory_space=pltpu.VMEM)
HBM = pl.BlockSpec(memory_space=pltpu.MemorySpace.HBM)
SMEM = pl.BlockSpec(memory_space=pltpu.SMEM)


def remote(src, dst, send, recv, where):
    return pltpu.make_async_remote_copy(src_ref=src, dst_ref=dst, send_sem=send, recv_sem=recv, device_id=where, device_id_type=MESH)


def greet(barrier, where):
    pl.semaphore_signal(barrier, inc=1, device_id=where, device_id_type=MESH)

STEP = 64


def split(value):
    high = value.astype(bf16)
    return high, (value - high.astype(f32)).astype(bf16)


def halo_kernel(offs_hbm, live_hbm, tile_ref, probe_hbm, mags, select_hbm, ext, den, probe, measured, select, padded, seen, offs, live, own, fetch, cs, cr, vs, vr):
    row = lax.axis_index("row")
    col = lax.axis_index("col")
    has = {"l": col > 0, "r": col < COLS - 1, "u": row > 0, "d": row < ROWS - 1}
    to = {"l": (row, col - 1), "r": (row, col + 1), "u": (row - 1, col), "d": (row + 1, col)}
    center = [pltpu.make_async_copy(tile_ref.at[:, :, pl.ds(j * 128, 128)], ext.at[:, 1 + j, pl.ds(128, 128), :], own.at[j]) for j in range(2)]
    for c in center:
        c.start()
    small = [pltpu.make_async_copy(a, b, fetch.at[i]) for i, (a, b) in enumerate(((offs_hbm, offs), (live_hbm, live), (probe_hbm, probe)))]
    for c in small:
        c.start()
    shown = [pltpu.make_async_copy(mags.at[0, 0, s, :, pl.ds(j * 128, 128)], seen.at[s, j], fetch.at[3 + 2 * s + j]) for s in range(2) for j in range(2)]
    shown.append(pltpu.make_async_copy(select_hbm, select, fetch.at[7]))
    barrier = pltpu.get_barrier_semaphore()
    for side in "lrud":

        @pl.when(has[side])
        def _():
            greet(barrier, to[side])

    expected = sum(has[side].astype(jnp.int32) for side in "lrud")

    @pl.when(row == 0)
    def _():
        ext[:, :, 0:128, :] = jnp.zeros((2, 4, 128, 128), f32)

    @pl.when(row == ROWS - 1)
    def _():
        ext[:, :, 256:384, :] = jnp.zeros((2, 4, 128, 128), f32)

    @pl.when(col == 0)
    def _():
        ext[:, 0] = jnp.zeros((2, 384, 128), f32)

    @pl.when(col == COLS - 1)
    def _():
        ext[:, 3] = jnp.zeros((2, 384, 128), f32)

    for c in center:
        c.wait()
    pl.semaphore_wait(barrier, expected)

    def across(p, side):
        mine, theirs = (1, 3) if side == "l" else (2, 0)
        i = 0 if side == "l" else 1
        return remote(ext.at[p, mine, pl.ds(128, 128)], ext.at[p, theirs, pl.ds(128, 128)], cs.at[p, i], cr.at[p, i], to[side])

    def up_down(p, side, part):
        at = (pl.ds(1, 2), 0, 3)[part]
        i, theirs = (0, 256) if side == "u" else (1, 0)
        return remote(ext.at[p, at, pl.ds(128, 128)], ext.at[p, at, pl.ds(theirs, 128)], vs.at[p, part, i], vr.at[p, part, i], to[side])

    for p in range(2):
        for side in "lr":

            @pl.when(has[side])
            def _():
                across(p, side).start()

    for p in range(2):
        for side in "ud":

            @pl.when(has[side])
            def _():
                up_down(p, side, 0).start()

    for c in shown:
        c.start()
    for c in small:
        c.wait()
    padded[...] = jnp.zeros_like(padded)
    peak = jnp.zeros((8, 128), f32)
    for i in range(0, 256, STEP):
        power = probe[0, i : i + STEP, :] * probe[0, i : i + STEP, :] + probe[1, i : i + STEP, :] * probe[1, i : i + STEP, :]
        for j in range(2):
            padded[2 + j, 128 + i : 128 + i + STEP, :] = power[:, j * 128 : j * 128 + 128]
        for a in range(0, STEP, 8):
            for b in range(0, 256, 128):
                peak = jnp.maximum(peak, power[a : a + 8, b : b + 128])
    den[...] = jnp.full((128, 256), object_damping, f32) * jnp.max(peak)

    def add(n, carry):
        da = n // 6 - 1
        db = (n // 2) % 3 - 1
        s = n % 2
        a = row + da
        b = col + db
        inside = (a >= 0) & (a < ROWS) & (b >= 0) & (b < COLS)
        a = jnp.clip(a, 0, ROWS - 1)
        b = jnp.clip(b, 0, COLS - 1)
        down = da * 128 + offs[(a * 2 + s) * 2, b]
        across = db * 256 + offs[(a * 2 + s) * 2 + 1, b]
        on = (inside & (s < live[a, b]) & (across > -256) & (across < 256)).astype(f32)
        across = jnp.clip(across, -256, 255)
        turn = (across + 256) % 128
        block = 4 - (across + 256) // 128
        lane = lax.broadcasted_iota(jnp.int32, (STEP, 128), 1)
        for i in range(0, 128, STEP):
            rolled = [pltpu.roll(padded[block + j - 1, pl.ds(i + 128 - down, STEP), :], turn, 1) for j in range(3)]
            for j in range(2):
                den[i : i + STEP, j * 128 : j * 128 + 128] += on * jnp.where(lane >= turn, rolled[j + 1], rolled[j])

        return carry

    lax.fori_loop(0, 18, add, 0)
    for c in shown:
        c.wait()
    for s in range(2):
        for odd in range(2):
            for i in range(0, 128, STEP):
                mh, ml = split(jnp.concatenate([seen[s, j, pl.ds(odd + 2 * i, STEP, stride=2), :] for j in range(2)], 1))
                measured[s, odd, i : i + STEP, :] = jnp.dot(mh, select[...], preferred_element_type=f32) + jnp.dot(ml, select[...], preferred_element_type=f32)

    for p in range(2):
        for side, part in (("l", 1), ("r", 2)):

            @pl.when(has[side])
            def _():
                across(p, "r" if side == "l" else "l").wait_recv()
                for way in "ud":

                    @pl.when(has[way])
                    def _():
                        up_down(p, way, part).start()

    for p in range(2):
        for side in "lr":

            @pl.when(has[side])
            def _():
                across(p, side).wait_send()

        for way, back in (("u", "d"), ("d", "u")):
            for part, need in ((0, None), (1, "l"), (2, "r")):
                cond = has[way] if need is None else jnp.logical_and(has[way], has[need])

                @pl.when(cond)
                def _():
                    up_down(p, way, part).wait_send()
                    up_down(p, back, part).wait_recv()


def halo(offs, live, tile, probe, mags, select):
    dma = pltpu.SemaphoreType.DMA
    return pl.pallas_call(
        halo_kernel,
        out_shape=(jax.ShapeDtypeStruct((2, 4, 384, 128), f32), jax.ShapeDtypeStruct((128, 256), f32), jax.ShapeDtypeStruct((2, 256, 256), f32), jax.ShapeDtypeStruct((2, 2, 128, 256), f32)),
        in_specs=[HBM] * 6,
        out_specs=(VMEM,) * 4,
        scratch_shapes=[pltpu.VMEM((256, 256), bf16), pltpu.VMEM((6, 512, 128), f32), pltpu.VMEM((2, 2, 256, 128), f32), pltpu.SMEM((ROWS * 4, COLS), jnp.int32), pltpu.SMEM((ROWS, COLS), jnp.int32), dma((2,)), dma((8,)), dma((2, 2)), dma((2, 2)), dma((2, 3, 2)), dma((2, 3, 2))],
        compiler_params=pltpu.CompilerParams(collective_id=1, has_side_effects=True, vmem_limit_bytes=8 << 20),
        cost_estimate=pl.CostEstimate(flops=400000000, bytes_accessed=1 << 20, transcendentals=0),
        name="halo",
    )(*(pltpu.with_memory_space_constraint(a, pltpu.MemorySpace.HBM) for a in (offs, live, tile, probe, mags, select)))


def dft_tables():
    m = np.arange(128)[:, None]
    k = np.arange(128)[None, :]
    tables = []
    for odd in range(2):
        angle = ((m * (2 * k + odd)) % 256) * (2.0 * math.pi / 256)
        c, s = np.cos(angle) / 16, np.sin(angle) / 16
        full = np.block([[c, -s], [s, c]])
        for t in (full, full.T):
            high = t.astype(np.float32).astype(jnp.bfloat16)
            low = (t - high.astype(np.float64)).astype(np.float32).astype(jnp.bfloat16)
            tables += [high, low]
    order = np.concatenate([np.arange(0, 256, 2), np.arange(1, 256, 2)])
    select = (np.arange(256)[:, None] == order[None, :]).astype(jnp.bfloat16)
    return np.stack(tables).reshape(2, 2, 2, 256, 256), select


def product(a, b):
    def dot(u, v):
        return jnp.dot(u, v, preferred_element_type=f32)

    return dot(a[0], b[0]) + (dot(a[1], b[0]) + dot(a[0], b[1]))


def tile_work(offs, live, ext, probe, measured, tables, upd, pieces, pat, wave, freq, zb, placed):
    row = lax.axis_index("row")
    col = lax.axis_index("col")
    lane = lax.broadcasted_iota(jnp.int32, (STEP, 128), 1)

    def table(odd, turned):
        return tables[odd, turned, 0], tables[odd, turned, 1]

    top = [offs[(row * 2 + s) * 2, col] + 128 for s in range(2)]
    left = [offs[(row * 2 + s) * 2 + 1, col] + 128 for s in range(2)]
    turn = [a % 128 for a in left]
    block = [a // 128 for a in left]
    alive = [(s < live[row, col]).astype(f32) for s in range(2)]
    for s in range(2):
        for i in range(0, 256, STEP):
            got = []
            for p in range(2):
                rolled = [pltpu.roll(ext[p, jnp.minimum(block[s] + j, 3), pl.ds(top[s] + i, STEP), :], 128 - turn[s], 1) for j in range(3)]
                halves = [jnp.where(lane < 128 - turn[s], rolled[j], rolled[j + 1]) for j in range(2)]
                got.append(jnp.concatenate(halves, 1))
                pat[s, p, i : i + STEP, :] = got[p]
            pr, pi = probe[0, i : i + STEP, :], probe[1, i : i + STEP, :]
            wr = pr * got[0] - pi * got[1]
            wi = pr * got[1] + pi * got[0]
            for odd in range(2):
                if odd:
                    mixed = [w[:, :128] - w[:, 128:] for w in (wr, wi)]
                else:
                    mixed = [w[:, :128] + w[:, 128:] for w in (wr, wi)]
                out = product(split(jnp.concatenate(mixed, 1)), table(odd, 0))
                for p in range(2):
                    wave[s, p, i : i + STEP, odd * 128 : odd * 128 + 128] = out[:, p * 128 : p * 128 + 128]
    for odd in range(2):
        for s in range(2):
            if odd:
                mixed = [wave[s, p, 0:128, :] - wave[s, p, 128:256, :] for p in range(2)]
            else:
                mixed = [wave[s, p, 0:128, :] + wave[s, p, 128:256, :] for p in range(2)]
            freq[s, odd] = product(table(odd, 1), split(jnp.concatenate(mixed, 0)))
    for odd in range(2):
        for s in range(2):
            for i in range(0, 128, STEP):
                fr = freq[s, odd, i : i + STEP, :]
                fi = freq[s, odd, 128 + i : 128 + i + STEP, :]
                factor = measured[s, odd, i : i + STEP, :] * lax.rsqrt(jnp.maximum(fr * fr + fi * fi, 0.0625)) - 1.0
                factor = factor * alive[s]
                for p, value in ((0, fr * factor), (1, fi * factor)):
                    high, low = split(value)
                    zb[s, odd, 0, p * 128 + i : p * 128 + i + STEP, :] = high
                    zb[s, odd, 1, p * 128 + i : p * 128 + i + STEP, :] = low
    for odd in range(2):
        for s in range(2):
            freq[s, odd] = product(table(odd, 0), (zb[s, odd, 0], zb[s, odd, 1]))
    for s in range(2):
        for p in range(2):
            e = freq[s, 0, p * 128 : p * 128 + 128, :]
            o = freq[s, 1, p * 128 : p * 128 + 128, :]
            wave[s, p, 0:128, :] = e + o
            wave[s, p, 128:256, :] = e - o
    for s in range(2):
        for i in range(0, 256, STEP):
            parts = []
            for odd in range(2):
                mixed = [wave[s, p, i : i + STEP, odd * 128 : odd * 128 + 128] for p in range(2)]
                parts.append(product(split(jnp.concatenate(mixed, 1)), table(odd, 1)))
            diff = []
            for p in range(2):
                e, o = (parts[odd][:, p * 128 : p * 128 + 128] for odd in range(2))
                diff.append(jnp.concatenate([e + o, e - o], 1))
            dr, di = diff
            pr, pi = probe[0, i : i + STEP, :], probe[1, i : i + STEP, :]
            ore, oim = pat[s, 0, i : i + STEP, :], pat[s, 1, i : i + STEP, :]
            for p, grad in ((0, pr * dr + pi * di), (1, pr * di - pi * dr)):
                first, second = (pltpu.roll(grad[:, j * 128 : j * 128 + 128], turn[s], 1) for j in range(2))
                moved = (jnp.where(lane >= turn[s], first, 0.0), jnp.where(lane >= turn[s], second, first), jnp.where(lane < turn[s], second, 0.0))
                for j in range(3):
                    placed[s, p, j, 128 + i : 128 + i + STEP, :] = moved[j]
            terms = (ore * dr + oim * di, ore * di - oim * dr, (ore * ore + oim * oim) * alive[s])
            for lb in range(2):
                for rb in range(STEP // 8):
                    t = lb * 32 + i // 8 + rb
                    for p in range(3):
                        value = terms[p][rb * 8 : rb * 8 + 8, lb * 128 : lb * 128 + 128]
                        pieces[t, p] = value if s == 0 else pieces[t, p] + value
    for k in range(4):
        here = [k - block[s] for s in range(2)]
        weight = [((a >= 0) & (a <= 2)).astype(f32) for a in here]
        here = [jnp.clip(a, 0, 2) for a in here]
        for p in range(2):
            for i in range(0, 384, STEP):
                got = [placed[s, p, here[s], pl.ds(128 + i - top[s], STEP), :] * weight[s] for s in range(2)]
                upd[p, k, i : i + STEP, :] = got[0] + got[1]


def finish_kernel(offs_hbm, live_hbm, ext, probe_ref, measured, tables, den_ref, spec_ref, spec_out, g, d_ref, u_ref, pat, wave, freq, zb, placed, offs, live, fetch, fv, side, fc, rp, s0, r1, s1, r2, s2, r3, wp, rw, r3w, hs, hr, es, er, ps, pr, ss1, rs1, ss2, rs2, ss3, rs3, ss4, rs4, ws, wr, zs, zr, gs, gr, know):
    row = lax.axis_index("row")
    col = lax.axis_index("col")
    core = row % 2
    x = (row // 2) % 4
    y = (row // 8) * 2 + col % 2
    z = col // 2

    def device(core_of, x_of, y_of, z_of):
        return ((y_of // 2) * 8 + x_of * 2 + core_of, z_of * 2 + y_of % 2)

    def peer(axis, d):
        return device(core, jnp.where(axis == 0, (x + d) % 4, x), jnp.where(axis == 0, y, (y + d) % 4), z)

    partner = device(1 - core, x, y, z)
    place = (x, y)
    has = {"l": col > 0, "r": col < COLS - 1, "u": row > 0, "d": row < ROWS - 1}
    beside = {"l": (row, col - 1), "r": (row, col + 1), "u": (row - 1, col), "d": (row + 1, col)}

    small = [pltpu.make_async_copy(a, b, fetch.at[i]) for i, (a, b) in enumerate(((offs_hbm, offs), (live_hbm, live)))]
    for c in small:
        c.start()
    barrier = pltpu.get_barrier_semaphore()
    greet(barrier, partner)
    for axis in range(2):
        for d in range(1, 4):
            greet(barrier, peer(axis, d))

    def along(d):
        return device(core, x, y, (z + d) % 16)

    for d in range(1, 5):
        greet(barrier, along(d))
        greet(barrier, along(16 - d))

    for way in "lrud":

        @pl.when(has[way])
        def _():
            greet(barrier, beside[way])

    expected = 15 + sum(has[way].astype(jnp.int32) for way in "lrud")

    for i, way in enumerate("ud"):

        @pl.when(jnp.logical_not(has[way]))
        def _():
            fv[i] = jnp.zeros((2, 4, 128, 128), f32)

    for i, way in enumerate("lr"):

        @pl.when(jnp.logical_not(has[way]))
        def _():
            fc[i] = jnp.zeros((2, 128, 128), f32)

    placed[:, :, :, 0:128, :] = jnp.zeros((2, 2, 3, 128, 128), f32)
    placed[:, :, :, 384:512, :] = jnp.zeros((2, 2, 3, 128, 128), f32)
    for c in small:
        c.wait()
    tile_work(offs, live, ext, probe_ref, measured, tables, u_ref, d_ref, pat, wave, freq, zb, placed)
    total = d_ref[0, 2]
    for t in range(1, 64):
        total = total + d_ref[t, 2]
    wp[0] = total
    pl.semaphore_wait(barrier, expected)
    for d in (4, 12):
        pl.semaphore_signal(know, inc=1, device_id=along(d), device_id_type=MESH)

    def vertical(p, part, way, inward=False):
        at = (0, 3, pl.ds(1, 2))[part]
        i = 0 if way == "u" else 1
        there = i if inward else 1 - i
        return remote(u_ref.at[p, at, pl.ds(256 * i, 128)], fv.at[there, p, at], hs.at[p, part, i], hr.at[p, part, there], beside[way])

    def lateral(p, way, inward=False):
        i = 0 if way == "l" else 1
        there = i if inward else 1 - i
        return remote(side.at[i, p], fc.at[there, p], es.at[p, i], er.at[p, there], beside[way])

    base = core * 32
    pending = []

    def go(c):
        c.start()
        pending.append(c)
        return c

    def spot(color, d):
        return color * 16 + ((place[color] + d) % 4) * 4

    near = (2, 1, 3)
    pairs = {}
    for d in near + (0,):
        for color in range(2):
            at = spot(color, d)
            pairs[color, d] = go(remote(d_ref.at[pl.ds((1 - core) * 32 + at, 4)], rp.at[pl.ds(at, 4)], ps.at[color, d], pr.at[color, d], partner))
        if d == 2:
            first = go(remote(wp.at[0], rw.at[0], ws.at[0], wr.at[0], partner))


    def join(color, d):
        pairs[color, d].wait_recv()
        at = spot(color, d)
        for b in range(4):
            s0[at + b] = d_ref[base + at + b] + rp[at + b]

    for d in near:
        for color in range(2):
            join(color, d)
    one = {}
    for e in near + (0,):
        for d in near:
            for color in range(2):
                b = (place[1 - color] + e) % 4
                one[color, d, e] = go(remote(s0.at[spot(color, d) + b], r1.at[color, d - 1, e], ss1.at[color, d - 1, e], rs1.at[color, d - 1, e], peer(color, d)))
        if e == 2:
            first.wait_recv()
            wp[1] = wp[0] + rw[0]
            waves = [go(remote(wp.at[1], rw.at[d], ws.at[d], wr.at[d], peer(0, d))) for d in range(1, 4)]
    for color in range(2):
        join(color, 0)
    two = {}
    for e in near + (0,):
        for color in range(2):
            b = (place[1 - color] + e) % 4
            for d in near:
                one[color, d, e].wait_recv()
            s1[color, e] = s0[spot(color, 0) + b] + (r1[color, 0, e] + (r1[color, 1, e] + r1[color, 2, e]))
            if e:
                two[color, e] = go(remote(s1.at[color, e], r2.at[color, e - 1], ss2.at[color, e - 1], rs2.at[color, e - 1], peer(1 - color, e)))
        if e == 2:
            for c in waves:
                c.wait_recv()
            wp[2] = wp[1] + (rw[1] + (rw[2] + rw[3]))
            waves = [go(remote(wp.at[2], rw.at[3 + d], ws.at[3 + d], wr.at[3 + d], peer(1, d))) for d in range(1, 4)]
    for part in range(3):
        for p in range(2):
            for way in "ud":

                @pl.when(has[way])
                def _():
                    vertical(p, part, way).start()

    for c in waves:
        c.wait_recv()
    wp[3] = wp[2] + (rw[4] + (rw[5] + rw[6]))
    pl.semaphore_wait(know, 2)

    def root(color):
        return 4 * color + 2 * core

    def slot(color):
        return base + color * 16 + jnp.where(color == 0, x * 4 + y, y * 4 + x)

    for color in range(2):
        for e in near:
            two[color, e].wait_recv()
        s2[color] = s1[color, 0] + (r2[color, 0] + (r2[color, 1] + r2[color, 2]))
        for n in range(2):
            goal = root(color) + 8 * n

            @pl.when(z != goal)
            def _():
                remote(s2.at[color], r3.at[z], zs.at[color, n, 0], zr.at[0], device(core, x, y, goal)).start()
                remote(wp.at[3], r3w.at[z], zs.at[color, n, 1], zr.at[1], device(core, x, y, goal)).start()

    for color in range(2):

        @pl.when(z % 8 == root(color))
        def _():
            r3[z] = s2[color]
            r3w[z] = wp[3]
            pltpu.make_async_copy(r3.at[pl.ds(0, 15)], r3.at[pl.ds(0, 15)], zr.at[0]).wait()
            pltpu.make_async_copy(r3w.at[pl.ds(0, 15)], r3w.at[pl.ds(0, 15)], zr.at[1]).wait()
            full = r3[0]
            weight = r3w[0]
            for i in range(1, 16):
                full = full + r3[i]
                weight = weight + r3w[i]
            mean = jnp.sum(weight) * (1.0 / 65536.0)
            scale = full[2] + probe_damping * mean
            t = slot(color)
            rows = pl.ds(pl.multiple_of((t % 32) * 8, 8), 8)
            lanes = pl.ds(pl.multiple_of((t // 32) * 128, 128), 128)
            for p in range(2):
                g[t, p] = probe_ref[p, rows, lanes] + full[p] / scale
            for i in (4, 3, 13, 2, 14, 1, 15):
                remote(g.at[t], g.at[t], gs.at[i % 8], gr.at[color], along(i)).start()

    for i, (way, at) in enumerate((("l", 0), ("r", 3))):
        for p in range(2):
            for up_down in "ud":

                @pl.when(has[up_down])
                def _():
                    vertical(p, i, up_down, True).wait_recv()

            @pl.when(has[way])
            def _():
                side[i, p] = u_ref[p, at, 128:256, :] + (fv[0, p, at] + fv[1, p, at])
                lateral(p, way).start()

    def away(color):
        d = (z - root(color) + 16) % 8
        return jnp.minimum(d, 8 - d)

    nearer = (away(1) < away(0)).astype(jnp.int32)
    colors = (nearer, 1 - nearer)

    def own(color):
        return jnp.where(color == 0, x, y)

    def cross(color):
        return jnp.where(color == 0, y, x)

    def tile_at(color, a, b):
        return base + color * 16 + (a % 4) * 4 + b % 4

    three = {}
    four = {}
    for n, color in enumerate(colors):
        t = slot(color)

        @pl.when(z % 8 != root(color))
        def _():
            pltpu.make_async_copy(g.at[t], g.at[t], gr.at[color]).wait()

        for d in near:
            three[n, d] = go(remote(g.at[t], g.at[t], ss3.at[color, d - 1], rs3.at[color, d - 1], peer(1 - color, d)))
        for d in near:
            four[n, d, 0] = go(remote(g.at[t], g.at[t], ss4.at[color, d - 1, 0], rs4.at[color, d - 1, 0], peer(color, d)))
    last = []
    for n, color in enumerate(colors):
        for e in (1, 3, 2):
            three[n, e].wait_recv()
            t = tile_at(color, own(color), cross(color) - e + 4)
            for d in near:
                four[n, d, e] = go(remote(g.at[t], g.at[t], ss4.at[color, d - 1, e], rs4.at[color, d - 1, e], peer(color, d)))
        group = g.at[pl.ds(tile_at(color, own(color), 0), 4)]
        last.append(go(remote(group, group, ps.at[2 + n, 0], pr.at[2 + n, 0], partner)))
    for n, color in enumerate(colors):
        for d in (1, 3, 2):
            for e in range(4):
                four[n, d, e].wait_recv()
            group = g.at[pl.ds(tile_at(color, own(color) - d + 4, 0), 4)]
            last.append(go(remote(group, group, ps.at[2 + n, d], pr.at[2 + n, d], partner)))
    for p in range(2):
        for way in "ud":

            @pl.when(has[way])
            def _():
                vertical(p, 2, way, True).wait_recv()

        for way in "lr":

            @pl.when(has[way])
            def _():
                lateral(p, way, True).wait_recv()

        for i in range(2):
            at = 1 + i
            update = u_ref[p, at, 128:256, :] + (fv[0, p, at] + fv[1, p, at]) + fc[i, p]
            lanes = slice(i * 128, i * 128 + 128)
            spec_out[p, :, lanes] = spec_ref[p, :, lanes] + update / den_ref[:, lanes]
    for c in last:
        c.wait_recv()
    for c in pending:
        c.wait_send()
    for p in range(2):
        for way in "ud":

            @pl.when(has[way])
            def _():
                for part in range(3):
                    vertical(p, part, way).wait_send()

        for way in "lr":

            @pl.when(has[way])
            def _():
                lateral(p, way).wait_send()

    for color in range(2):

        for n in range(2):

            @pl.when(z != root(color) + 8 * n)
            def _():
                pltpu.make_async_copy(s2.at[color], s2.at[color], zs.at[color, n, 0]).wait()
                pltpu.make_async_copy(wp.at[3], wp.at[3], zs.at[color, n, 1]).wait()

        @pl.when(z % 8 == root(color))
        def _():
            t = slot(color)
            for i in (4, 3, 5, 2, 6, 1, 7):
                pltpu.make_async_copy(g.at[t], g.at[t], gs.at[i]).wait()


def finish(offs, live, ext, probe, measured, tables, den, specimen):
    tile = (8, 128)
    dma = pltpu.SemaphoreType.DMA

    def vmem(*shape):
        return pltpu.VMEM(shape, f32)

    return pl.pallas_call(
        finish_kernel,
        out_shape=(jax.ShapeDtypeStruct((2, 128, 256), f32), jax.ShapeDtypeStruct((64, 2, 8, 128), f32)),
        in_specs=[HBM] * 2 + [VMEM] * 6,
        out_specs=(VMEM,) * 2,
        scratch_shapes=[
            vmem(64, 3, *tile),
            vmem(2, 4, 384, 128),
            vmem(2, 2, 256, 256),
            vmem(2, 2, 256, 256),
            vmem(2, 2, 256, 256),
            pltpu.VMEM((2, 2, 2, 256, 256), bf16),
            vmem(2, 2, 3, 512, 128),
            pltpu.SMEM((ROWS * 4, COLS), jnp.int32),
            pltpu.SMEM((ROWS, COLS), jnp.int32),
            dma((2,)),
            vmem(2, 2, 4, 128, 128),
            vmem(2, 2, 128, 128),
            vmem(2, 2, 128, 128),
            vmem(32, 3, *tile),
            vmem(32, 3, *tile),
            vmem(2, 3, 4, 3, *tile),
            vmem(2, 4, 3, *tile),
            vmem(2, 3, 3, *tile),
            vmem(2, 3, *tile),
            vmem(16, 3, *tile),
            vmem(4, *tile),
            vmem(7, *tile),
            vmem(16, *tile),
            dma((2, 3, 2)),
            dma((2, 3, 2)),
            dma((2, 2)),
            dma((2, 2)),
            dma((4, 4)),
            dma((4, 4)),
            dma((2, 3, 4)),
            dma((2, 3, 4)),
            dma((2, 3)),
            dma((2, 3)),
            dma((2, 3)),
            dma((2, 3)),
            dma((2, 3, 4)),
            dma((2, 3, 4)),
            dma((7,)),
            dma((7,)),
            dma((2, 2, 2)),
            dma((2,)),
            dma((8,)),
            dma((2,)),
            pltpu.SemaphoreType.REGULAR,
        ],
        compiler_params=pltpu.CompilerParams(collective_id=0, has_side_effects=True, vmem_limit_bytes=32 << 20),
        cost_estimate=pl.CostEstimate(flops=1000000000, bytes_accessed=1 << 20, transcendentals=0),
        name="finish",
    )(*(pltpu.with_memory_space_constraint(a, pltpu.MemorySpace.HBM) for a in (offs, live)), ext, probe, measured, tables, den, specimen)


def write_kernel(spec_ref, g_ref, spec_out, probe_out):
    spec_out[...] = spec_ref[...]
    for lb in range(2):
        for rb in range(32):
            for p in range(2):
                probe_out[p, rb * 8 : rb * 8 + 8, lb * 128 : lb * 128 + 128] = g_ref[lb * 32 + rb, p]


def write(specimen_next, probe_tiles):
    return pl.pallas_call(
        write_kernel,
        out_shape=(jax.ShapeDtypeStruct((2, 128, 256), f32), jax.ShapeDtypeStruct((2, 256, 256), f32)),
        in_specs=[VMEM] * 2,
        out_specs=(VMEM,) * 2,
        compiler_params=pltpu.CompilerParams(vmem_limit_bytes=8 << 20),
        name="write",
    )(specimen_next, probe_tiles)


def shards(specimen, probe_field, scan_offsets, live_counts, magnitudes):
    offs = scan_offsets.transpose(0, 2, 3, 1).reshape(ROWS * 4, COLS)
    tables, select = (jnp.asarray(a) for a in dft_tables())
    ext, den, probe, measured = halo(offs, live_counts, specimen, probe_field, magnitudes, select)
    return write(*finish(offs, live_counts, ext, probe, measured, tables, den, specimen))


def solution(mesh):
    return jax.shard_map(
        shards,
        mesh=mesh,
        in_specs=(P(None, "row", "col"), P(), P(), P(), P("row", "col", None, None, None)),
        out_specs=(P(None, "row", "col"), P()),
        check_vma=False,
    )
```

```python
import math

import jax
import jax.numpy as jnp
import numpy as np
from jax import lax
from jax.experimental import pallas as pl
from jax.experimental.pallas import tpu as pltpu
from jax.sharding import PartitionSpec as P

MESH = pl.DeviceIdType.MESH
ROWS = 16
COLS = 32
object_damping = 0.1
probe_damping = 0.1
f32 = jnp.float32
bf16 = jnp.bfloat16
VMEM = pl.BlockSpec(memory_space=pltpu.VMEM)
HBM = pl.BlockSpec(memory_space=pltpu.MemorySpace.HBM)
SMEM = pl.BlockSpec(memory_space=pltpu.SMEM)


def remote(src, dst, send, recv, where):
    return pltpu.make_async_remote_copy(src_ref=src, dst_ref=dst, send_sem=send, recv_sem=recv, device_id=where, device_id_type=MESH)


def greet(barrier, where):
    pl.semaphore_signal(barrier, inc=1, device_id=where, device_id_type=MESH)

STEP = 64


def split(value):
    high = value.astype(bf16)
    return high, (value - high.astype(f32)).astype(bf16)


def halo_kernel(offs_hbm, live_hbm, tile_ref, probe_hbm, mags, select_hbm, ext, den, probe, measured, select, padded, seen, offs, live, own, fetch, cs, cr, vs, vr):
    row = lax.axis_index("row")
    col = lax.axis_index("col")
    has = {"l": col > 0, "r": col < COLS - 1, "u": row > 0, "d": row < ROWS - 1}
    to = {"l": (row, col - 1), "r": (row, col + 1), "u": (row - 1, col), "d": (row + 1, col)}
    center = [pltpu.make_async_copy(tile_ref.at[:, :, pl.ds(j * 128, 128)], ext.at[:, 1 + j, pl.ds(128, 128), :], own.at[j]) for j in range(2)]
    for c in center:
        c.start()
    small = [pltpu.make_async_copy(a, b, fetch.at[i]) for i, (a, b) in enumerate(((offs_hbm, offs), (live_hbm, live), (probe_hbm, probe)))]
    for c in small:
        c.start()
    shown = [pltpu.make_async_copy(mags.at[0, 0, s, :, pl.ds(j * 128, 128)], seen.at[s, j], fetch.at[3 + 2 * s + j]) for s in range(2) for j in range(2)]
    shown.append(pltpu.make_async_copy(select_hbm, select, fetch.at[7]))
    barrier = pltpu.get_barrier_semaphore()
    for side in "lrud":

        @pl.when(has[side])
        def _():
            greet(barrier, to[side])

    expected = sum(has[side].astype(jnp.int32) for side in "lrud")

    @pl.when(row == 0)
    def _():
        ext[:, :, 0:128, :] = jnp.zeros((2, 4, 128, 128), f32)

    @pl.when(row == ROWS - 1)
    def _():
        ext[:, :, 256:384, :] = jnp.zeros((2, 4, 128, 128), f32)

    @pl.when(col == 0)
    def _():
        ext[:, 0] = jnp.zeros((2, 384, 128), f32)

    @pl.when(col == COLS - 1)
    def _():
        ext[:, 3] = jnp.zeros((2, 384, 128), f32)

    for c in center:
        c.wait()
    pl.semaphore_wait(barrier, expected)

    def across(p, side):
        mine, theirs = (1, 3) if side == "l" else (2, 0)
        i = 0 if side == "l" else 1
        return remote(ext.at[p, mine, pl.ds(128, 128)], ext.at[p, theirs, pl.ds(128, 128)], cs.at[p, i], cr.at[p, i], to[side])

    def up_down(p, side, part):
        at = (pl.ds(1, 2), 0, 3)[part]
        i, theirs = (0, 256) if side == "u" else (1, 0)
        return remote(ext.at[p, at, pl.ds(128, 128)], ext.at[p, at, pl.ds(theirs, 128)], vs.at[p, part, i], vr.at[p, part, i], to[side])

    for p in range(2):
        for side in "lr":

            @pl.when(has[side])
            def _():
                across(p, side).start()

    for p in range(2):
        for side in "ud":

            @pl.when(has[side])
            def _():
                up_down(p, side, 0).start()

    for c in shown:
        c.start()
    for c in small:
        c.wait()
    padded[...] = jnp.zeros_like(padded)
    peak = jnp.zeros((8, 128), f32)
    for i in range(0, 256, STEP):
        power = probe[0, i : i + STEP, :] * probe[0, i : i + STEP, :] + probe[1, i : i + STEP, :] * probe[1, i : i + STEP, :]
        for j in range(2):
            padded[2 + j, 128 + i : 128 + i + STEP, :] = power[:, j * 128 : j * 128 + 128]
        for a in range(0, STEP, 8):
            for b in range(0, 256, 128):
                peak = jnp.maximum(peak, power[a : a + 8, b : b + 128])
    den[...] = jnp.full((128, 256), object_damping, f32) * jnp.max(peak)

    def add(n, carry):
        da = n // 6 - 1
        db = (n // 2) % 3 - 1
        s = n % 2
        a = row + da
        b = col + db
        inside = (a >= 0) & (a < ROWS) & (b >= 0) & (b < COLS)
        a = jnp.clip(a, 0, ROWS - 1)
        b = jnp.clip(b, 0, COLS - 1)
        down = da * 128 + offs[(a * 2 + s) * 2, b]
        across = db * 256 + offs[(a * 2 + s) * 2 + 1, b]
        on = (inside & (s < live[a, b]) & (across > -256) & (across < 256)).astype(f32)
        across = jnp.clip(across, -256, 255)
        turn = (across + 256) % 128
        block = 4 - (across + 256) // 128
        lane = lax.broadcasted_iota(jnp.int32, (STEP, 128), 1)
        for i in range(0, 128, STEP):
            rolled = [pltpu.roll(padded[block + j - 1, pl.ds(i + 128 - down, STEP), :], turn, 1) for j in range(3)]
            for j in range(2):
                den[i : i + STEP, j * 128 : j * 128 + 128] += on * jnp.where(lane >= turn, rolled[j + 1], rolled[j])

        return carry

    lax.fori_loop(0, 18, add, 0)
    for p in range(2):
        for side, part in (("l", 1), ("r", 2)):

            @pl.when(has[side])
            def _():
                across(p, "r" if side == "l" else "l").wait_recv()
                for way in "ud":

                    @pl.when(has[way])
                    def _():
                        up_down(p, way, part).start()

    for c in shown:
        c.wait()
    for s in range(2):
        for odd in range(2):
            for i in range(0, 128, STEP):
                mh, ml = split(jnp.concatenate([seen[s, j, pl.ds(odd + 2 * i, STEP, stride=2), :] for j in range(2)], 1))
                measured[s, odd, i : i + STEP, :] = jnp.dot(mh, select[...], preferred_element_type=f32) + jnp.dot(ml, select[...], preferred_element_type=f32)

    for p in range(2):
        for side in "lr":

            @pl.when(has[side])
            def _():
                across(p, side).wait_send()

        for way, back in (("u", "d"), ("d", "u")):
            for part, need in ((0, None), (1, "l"), (2, "r")):
                cond = has[way] if need is None else jnp.logical_and(has[way], has[need])

                @pl.when(cond)
                def _():
                    up_down(p, way, part).wait_send()
                    up_down(p, back, part).wait_recv()


def halo(offs, live, tile, probe, mags, select):
    dma = pltpu.SemaphoreType.DMA
    return pl.pallas_call(
        halo_kernel,
        out_shape=(jax.ShapeDtypeStruct((2, 4, 384, 128), f32), jax.ShapeDtypeStruct((128, 256), f32), jax.ShapeDtypeStruct((2, 256, 256), f32), jax.ShapeDtypeStruct((2, 2, 128, 256), f32)),
        in_specs=[HBM] * 6,
        out_specs=(VMEM,) * 4,
        scratch_shapes=[pltpu.VMEM((256, 256), bf16), pltpu.VMEM((6, 512, 128), f32), pltpu.VMEM((2, 2, 256, 128), f32), pltpu.SMEM((ROWS * 4, COLS), jnp.int32), pltpu.SMEM((ROWS, COLS), jnp.int32), dma((2,)), dma((8,)), dma((2, 2)), dma((2, 2)), dma((2, 3, 2)), dma((2, 3, 2))],
        compiler_params=pltpu.CompilerParams(collective_id=1, has_side_effects=True, vmem_limit_bytes=8 << 20),
        cost_estimate=pl.CostEstimate(flops=400000000, bytes_accessed=1 << 20, transcendentals=0),
        name="halo",
    )(*(pltpu.with_memory_space_constraint(a, pltpu.MemorySpace.HBM) for a in (offs, live, tile, probe, mags, select)))


def dft_tables():
    m = np.arange(128)[:, None]
    k = np.arange(128)[None, :]
    tables = []
    for odd in range(2):
        angle = ((m * (2 * k + odd)) % 256) * (2.0 * math.pi / 256)
        c, s = np.cos(angle) / 16, np.sin(angle) / 16
        full = np.block([[c, -s], [s, c]])
        for t in (full, full.T):
            high = t.astype(np.float32).astype(jnp.bfloat16)
            low = (t - high.astype(np.float64)).astype(np.float32).astype(jnp.bfloat16)
            tables += [high, low]
    order = np.concatenate([np.arange(0, 256, 2), np.arange(1, 256, 2)])
    select = (np.arange(256)[:, None] == order[None, :]).astype(jnp.bfloat16)
    return np.stack(tables).reshape(2, 2, 2, 256, 256), select


def product(a, b):
    def dot(u, v):
        return jnp.dot(u, v, preferred_element_type=f32)

    return dot(a[0], b[0]) + (dot(a[1], b[0]) + dot(a[0], b[1]))


def tile_work(offs, live, ext, probe, measured, tables, upd, pieces, pat, wave, freq, zb, placed):
    row = lax.axis_index("row")
    col = lax.axis_index("col")
    lane = lax.broadcasted_iota(jnp.int32, (STEP, 128), 1)

    def table(odd, turned):
        return tables[odd, turned, 0], tables[odd, turned, 1]

    top = [offs[(row * 2 + s) * 2, col] + 128 for s in range(2)]
    left = [offs[(row * 2 + s) * 2 + 1, col] + 128 for s in range(2)]
    turn = [a % 128 for a in left]
    block = [a // 128 for a in left]
    alive = [(s < live[row, col]).astype(f32) for s in range(2)]
    for s in range(2):
        for i in range(0, 256, STEP):
            got = []
            for p in range(2):
                rolled = [pltpu.roll(ext[p, jnp.minimum(block[s] + j, 3), pl.ds(top[s] + i, STEP), :], 128 - turn[s], 1) for j in range(3)]
                halves = [jnp.where(lane < 128 - turn[s], rolled[j], rolled[j + 1]) for j in range(2)]
                got.append(jnp.concatenate(halves, 1))
                pat[s, p, i : i + STEP, :] = got[p]
            pr, pi = probe[0, i : i + STEP, :], probe[1, i : i + STEP, :]
            wr = pr * got[0] - pi * got[1]
            wi = pr * got[1] + pi * got[0]
            for odd in range(2):
                if odd:
                    mixed = [w[:, :128] - w[:, 128:] for w in (wr, wi)]
                else:
                    mixed = [w[:, :128] + w[:, 128:] for w in (wr, wi)]
                high, low = split(jnp.concatenate(mixed, 1))
                zb[s, odd, 0, i : i + STEP, :] = high
                zb[s, odd, 1, i : i + STEP, :] = low
        for odd in range(2):
            out = product((zb[s, odd, 0], zb[s, odd, 1]), table(odd, 0))
            for p in range(2):
                wave[s, p, :, odd * 128 : odd * 128 + 128] = out[:, p * 128 : p * 128 + 128]
    for odd in range(2):
        for s in range(2):
            if odd:
                mixed = [wave[s, p, 0:128, :] - wave[s, p, 128:256, :] for p in range(2)]
            else:
                mixed = [wave[s, p, 0:128, :] + wave[s, p, 128:256, :] for p in range(2)]
            freq[s, odd] = product(table(odd, 1), split(jnp.concatenate(mixed, 0)))
    for odd in range(2):
        for s in range(2):
            for i in range(0, 128, STEP):
                fr = freq[s, odd, i : i + STEP, :]
                fi = freq[s, odd, 128 + i : 128 + i + STEP, :]
                factor = measured[s, odd, i : i + STEP, :] * lax.rsqrt(jnp.maximum(fr * fr + fi * fi, 0.0625)) - 1.0
                factor = factor * alive[s]
                for p, value in ((0, fr * factor), (1, fi * factor)):
                    high, low = split(value)
                    zb[s, odd, 0, p * 128 + i : p * 128 + i + STEP, :] = high
                    zb[s, odd, 1, p * 128 + i : p * 128 + i + STEP, :] = low
    for odd in range(2):
        for s in range(2):
            freq[s, odd] = product(table(odd, 0), (zb[s, odd, 0], zb[s, odd, 1]))
    for s in range(2):
        for p in range(2):
            e = freq[s, 0, p * 128 : p * 128 + 128, :]
            o = freq[s, 1, p * 128 : p * 128 + 128, :]
            wave[s, p, 0:128, :] = e + o
            wave[s, p, 128:256, :] = e - o
    for s in range(2):
        for odd in range(2):
            for i in range(0, 256, STEP):
                high, low = split(jnp.concatenate([wave[s, p, i : i + STEP, odd * 128 : odd * 128 + 128] for p in range(2)], 1))
                zb[s, odd, 0, i : i + STEP, :] = high
                zb[s, odd, 1, i : i + STEP, :] = low
            freq[s, odd] = product((zb[s, odd, 0], zb[s, odd, 1]), table(odd, 1))
    for s in range(2):
        for i in range(0, 256, STEP):
            diff = []
            for p in range(2):
                e, o = (freq[s, odd, i : i + STEP, p * 128 : p * 128 + 128] for odd in range(2))
                diff.append(jnp.concatenate([e + o, e - o], 1))
            dr, di = diff
            pr, pi = probe[0, i : i + STEP, :], probe[1, i : i + STEP, :]
            ore, oim = pat[s, 0, i : i + STEP, :], pat[s, 1, i : i + STEP, :]
            for p, grad in ((0, pr * dr + pi * di), (1, pr * di - pi * dr)):
                first, second = (pltpu.roll(grad[:, j * 128 : j * 128 + 128], turn[s], 1) for j in range(2))
                moved = (jnp.where(lane >= turn[s], first, 0.0), jnp.where(lane >= turn[s], second, first), jnp.where(lane < turn[s], second, 0.0))
                for j in range(3):
                    placed[s, p, j, 128 + i : 128 + i + STEP, :] = moved[j]
            terms = (ore * dr + oim * di, ore * di - oim * dr, (ore * ore + oim * oim) * alive[s])
            for lb in range(2):
                for rb in range(STEP // 8):
                    t = lb * 32 + i // 8 + rb
                    for p in range(3):
                        value = terms[p][rb * 8 : rb * 8 + 8, lb * 128 : lb * 128 + 128]
                        pieces[t, p] = value if s == 0 else pieces[t, p] + value
    for k in range(4):
        here = [k - block[s] for s in range(2)]
        weight = [((a >= 0) & (a <= 2)).astype(f32) for a in here]
        here = [jnp.clip(a, 0, 2) for a in here]
        for p in range(2):
            for i in range(0, 384, STEP):
                got = [placed[s, p, here[s], pl.ds(128 + i - top[s], STEP), :] * weight[s] for s in range(2)]
                upd[p, k, i : i + STEP, :] = got[0] + got[1]


def finish_kernel(offs_hbm, live_hbm, ext, probe_ref, measured, tables, den_ref, spec_ref, spec_out, g, d_ref, u_ref, pat, wave, freq, zb, placed, offs, live, fetch, fv, side, fc, rp, s0, r1, s1, r2, s2, r3, wp, rw, r3w, hs, hr, es, er, ps, pr, ss1, rs1, ss2, rs2, ss3, rs3, ss4, rs4, ws, wr, zs, zr, gs, gr, know):
    row = lax.axis_index("row")
    col = lax.axis_index("col")
    core = row % 2
    x = (row // 2) % 4
    y = (row // 8) * 2 + col % 2
    z = col // 2

    def device(core_of, x_of, y_of, z_of):
        return ((y_of // 2) * 8 + x_of * 2 + core_of, z_of * 2 + y_of % 2)

    def peer(axis, d):
        return device(core, jnp.where(axis == 0, (x + d) % 4, x), jnp.where(axis == 0, y, (y + d) % 4), z)

    partner = device(1 - core, x, y, z)
    place = (x, y)
    has = {"l": col > 0, "r": col < COLS - 1, "u": row > 0, "d": row < ROWS - 1}
    beside = {"l": (row, col - 1), "r": (row, col + 1), "u": (row - 1, col), "d": (row + 1, col)}

    small = [pltpu.make_async_copy(a, b, fetch.at[i]) for i, (a, b) in enumerate(((offs_hbm, offs), (live_hbm, live)))]
    for c in small:
        c.start()
    barrier = pltpu.get_barrier_semaphore()
    greet(barrier, partner)
    for axis in range(2):
        for d in range(1, 4):
            greet(barrier, peer(axis, d))

    def along(d):
        return device(core, x, y, (z + d) % 16)

    for d in range(1, 5):
        greet(barrier, along(d))
        greet(barrier, along(16 - d))

    for way in "lrud":

        @pl.when(has[way])
        def _():
            greet(barrier, beside[way])

    expected = 15 + sum(has[way].astype(jnp.int32) for way in "lrud")

    for i, way in enumerate("ud"):

        @pl.when(jnp.logical_not(has[way]))
        def _():
            fv[i] = jnp.zeros((2, 4, 128, 128), f32)

    for i, way in enumerate("lr"):

        @pl.when(jnp.logical_not(has[way]))
        def _():
            fc[i] = jnp.zeros((2, 128, 128), f32)

    placed[:, :, :, 0:128, :] = jnp.zeros((2, 2, 3, 128, 128), f32)
    placed[:, :, :, 384:512, :] = jnp.zeros((2, 2, 3, 128, 128), f32)
    for c in small:
        c.wait()
    tile_work(offs, live, ext, probe_ref, measured, tables, u_ref, d_ref, pat, wave, freq, zb, placed)
    total = d_ref[0, 2]
    for t in range(1, 64):
        total = total + d_ref[t, 2]
    wp[0] = total
    pl.semaphore_wait(barrier, expected)
    for d in (4, 12):
        pl.semaphore_signal(know, inc=1, device_id=along(d), device_id_type=MESH)

    def vertical(p, part, way, inward=False):
        at = (0, 3, pl.ds(1, 2))[part]
        i = 0 if way == "u" else 1
        there = i if inward else 1 - i
        return remote(u_ref.at[p, at, pl.ds(256 * i, 128)], fv.at[there, p, at], hs.at[p, part, i], hr.at[p, part, there], beside[way])

    def lateral(p, way, inward=False):
        i = 0 if way == "l" else 1
        there = i if inward else 1 - i
        return remote(side.at[i, p], fc.at[there, p], es.at[p, i], er.at[p, there], beside[way])

    base = core * 32
    pending = []

    def go(c):
        c.start()
        pending.append(c)
        return c

    def spot(color, d):
        return color * 16 + ((place[color] + d) % 4) * 4

    near = (2, 1, 3)
    pairs = {}
    for d in near + (0,):
        for color in range(2):
            at = spot(color, d)
            pairs[color, d] = go(remote(d_ref.at[pl.ds((1 - core) * 32 + at, 4)], rp.at[pl.ds(at, 4)], ps.at[color, d], pr.at[color, d], partner))
        if d == 2:
            first = go(remote(wp.at[0], rw.at[0], ws.at[0], wr.at[0], partner))


    def join(color, d):
        pairs[color, d].wait_recv()
        at = spot(color, d)
        for b in range(4):
            s0[at + b] = d_ref[base + at + b] + rp[at + b]

    for d in near:
        for color in range(2):
            join(color, d)
    one = {}
    for e in near + (0,):
        for d in near:
            for color in range(2):
                b = (place[1 - color] + e) % 4
                one[color, d, e] = go(remote(s0.at[spot(color, d) + b], r1.at[color, d - 1, e], ss1.at[color, d - 1, e], rs1.at[color, d - 1, e], peer(color, d)))
        if e == 2:
            first.wait_recv()
            wp[1] = wp[0] + rw[0]
            waves = [go(remote(wp.at[1], rw.at[d], ws.at[d], wr.at[d], peer(0, d))) for d in range(1, 4)]
    for color in range(2):
        join(color, 0)
    two = {}
    for e in near + (0,):
        for color in range(2):
            b = (place[1 - color] + e) % 4
            for d in near:
                one[color, d, e].wait_recv()
            s1[color, e] = s0[spot(color, 0) + b] + (r1[color, 0, e] + (r1[color, 1, e] + r1[color, 2, e]))
            if e:
                two[color, e] = go(remote(s1.at[color, e], r2.at[color, e - 1], ss2.at[color, e - 1], rs2.at[color, e - 1], peer(1 - color, e)))
        if e == 2:
            for c in waves:
                c.wait_recv()
            wp[2] = wp[1] + (rw[1] + (rw[2] + rw[3]))
            waves = [go(remote(wp.at[2], rw.at[3 + d], ws.at[3 + d], wr.at[3 + d], peer(1, d))) for d in range(1, 4)]
    for part in range(3):
        for p in range(2):
            for way in "ud":

                @pl.when(has[way])
                def _():
                    vertical(p, part, way).start()

    for c in waves:
        c.wait_recv()
    wp[3] = wp[2] + (rw[4] + (rw[5] + rw[6]))
    pl.semaphore_wait(know, 2)

    def root(color):
        return 4 * color + 2 * core

    def slot(color):
        return base + color * 16 + jnp.where(color == 0, x * 4 + y, y * 4 + x)

    for color in range(2):
        for e in near:
            two[color, e].wait_recv()
        s2[color] = s1[color, 0] + (r2[color, 0] + (r2[color, 1] + r2[color, 2]))
        for n in range(2):
            goal = root(color) + 8 * n

            @pl.when(z != goal)
            def _():
                remote(s2.at[color], r3.at[z], zs.at[color, n, 0], zr.at[0], device(core, x, y, goal)).start()
                remote(wp.at[3], r3w.at[z], zs.at[color, n, 1], zr.at[1], device(core, x, y, goal)).start()

    for color in range(2):

        @pl.when(z % 8 == root(color))
        def _():
            r3[z] = s2[color]
            r3w[z] = wp[3]
            pltpu.make_async_copy(r3.at[pl.ds(0, 15)], r3.at[pl.ds(0, 15)], zr.at[0]).wait()
            pltpu.make_async_copy(r3w.at[pl.ds(0, 15)], r3w.at[pl.ds(0, 15)], zr.at[1]).wait()
            full = r3[0]
            weight = r3w[0]
            for i in range(1, 16):
                full = full + r3[i]
                weight = weight + r3w[i]
            mean = jnp.sum(weight) * (1.0 / 65536.0)
            scale = full[2] + probe_damping * mean
            t = slot(color)
            rows = pl.ds(pl.multiple_of((t % 32) * 8, 8), 8)
            lanes = pl.ds(pl.multiple_of((t // 32) * 128, 128), 128)
            for p in range(2):
                g[t, p] = probe_ref[p, rows, lanes] + full[p] / scale
            for i in (4, 3, 13, 2, 14, 1, 15):
                remote(g.at[t], g.at[t], gs.at[i % 8], gr.at[color], along(i)).start()

    for i, (way, at) in enumerate((("l", 0), ("r", 3))):
        for p in range(2):
            for up_down in "ud":

                @pl.when(has[up_down])
                def _():
                    vertical(p, i, up_down, True).wait_recv()

            @pl.when(has[way])
            def _():
                side[i, p] = u_ref[p, at, 128:256, :] + (fv[0, p, at] + fv[1, p, at])
                lateral(p, way).start()

    def away(color):
        d = (z - root(color) + 16) % 8
        return jnp.minimum(d, 8 - d)

    nearer = (away(1) < away(0)).astype(jnp.int32)
    colors = (nearer, 1 - nearer)

    def own(color):
        return jnp.where(color == 0, x, y)

    def cross(color):
        return jnp.where(color == 0, y, x)

    def tile_at(color, a, b):
        return base + color * 16 + (a % 4) * 4 + b % 4

    three = {}
    four = {}
    for n, color in enumerate(colors):
        t = slot(color)

        @pl.when(z % 8 != root(color))
        def _():
            pltpu.make_async_copy(g.at[t], g.at[t], gr.at[color]).wait()

        for d in near:
            three[n, d] = go(remote(g.at[t], g.at[t], ss3.at[color, d - 1], rs3.at[color, d - 1], peer(1 - color, d)))
        for d in near:
            four[n, d, 0] = go(remote(g.at[t], g.at[t], ss4.at[color, d - 1, 0], rs4.at[color, d - 1, 0], peer(color, d)))
    last = []
    for n, color in enumerate(colors):
        for e in (1, 3, 2):
            three[n, e].wait_recv()
            t = tile_at(color, own(color), cross(color) - e + 4)
            for d in near:
                four[n, d, e] = go(remote(g.at[t], g.at[t], ss4.at[color, d - 1, e], rs4.at[color, d - 1, e], peer(color, d)))
        group = g.at[pl.ds(tile_at(color, own(color), 0), 4)]
        last.append(go(remote(group, group, ps.at[2 + n, 0], pr.at[2 + n, 0], partner)))
    for n, color in enumerate(colors):
        for d in (1, 3, 2):
            for e in range(4):
                four[n, d, e].wait_recv()
            group = g.at[pl.ds(tile_at(color, own(color) - d + 4, 0), 4)]
            last.append(go(remote(group, group, ps.at[2 + n, d], pr.at[2 + n, d], partner)))
    for p in range(2):
        for way in "ud":

            @pl.when(has[way])
            def _():
                vertical(p, 2, way, True).wait_recv()

        for way in "lr":

            @pl.when(has[way])
            def _():
                lateral(p, way, True).wait_recv()

        for i in range(2):
            at = 1 + i
            update = u_ref[p, at, 128:256, :] + (fv[0, p, at] + fv[1, p, at]) + fc[i, p]
            lanes = slice(i * 128, i * 128 + 128)
            spec_out[p, :, lanes] = spec_ref[p, :, lanes] + update / den_ref[:, lanes]
    for c in last:
        c.wait_recv()
    for c in pending:
        c.wait_send()
    for p in range(2):
        for way in "ud":

            @pl.when(has[way])
            def _():
                for part in range(3):
                    vertical(p, part, way).wait_send()

        for way in "lr":

            @pl.when(has[way])
            def _():
                lateral(p, way).wait_send()

    for color in range(2):

        for n in range(2):

            @pl.when(z != root(color) + 8 * n)
            def _():
                pltpu.make_async_copy(s2.at[color], s2.at[color], zs.at[color, n, 0]).wait()
                pltpu.make_async_copy(wp.at[3], wp.at[3], zs.at[color, n, 1]).wait()

        @pl.when(z % 8 == root(color))
        def _():
            t = slot(color)
            for i in (4, 3, 5, 2, 6, 1, 7):
                pltpu.make_async_copy(g.at[t], g.at[t], gs.at[i]).wait()


def finish(offs, live, ext, probe, measured, tables, den, specimen):
    tile = (8, 128)
    dma = pltpu.SemaphoreType.DMA

    def vmem(*shape):
        return pltpu.VMEM(shape, f32)

    return pl.pallas_call(
        finish_kernel,
        out_shape=(jax.ShapeDtypeStruct((2, 128, 256), f32), jax.ShapeDtypeStruct((64, 2, 8, 128), f32)),
        in_specs=[HBM] * 2 + [VMEM] * 6,
        out_specs=(VMEM,) * 2,
        scratch_shapes=[
            vmem(64, 3, *tile),
            vmem(2, 4, 384, 128),
            vmem(2, 2, 256, 256),
            vmem(2, 2, 256, 256),
            vmem(2, 2, 256, 256),
            pltpu.VMEM((2, 2, 2, 256, 256), bf16),
            vmem(2, 2, 3, 512, 128),
            pltpu.SMEM((ROWS * 4, COLS), jnp.int32),
            pltpu.SMEM((ROWS, COLS), jnp.int32),
            dma((2,)),
            vmem(2, 2, 4, 128, 128),
            vmem(2, 2, 128, 128),
            vmem(2, 2, 128, 128),
            vmem(32, 3, *tile),
            vmem(32, 3, *tile),
            vmem(2, 3, 4, 3, *tile),
            vmem(2, 4, 3, *tile),
            vmem(2, 3, 3, *tile),
            vmem(2, 3, *tile),
            vmem(16, 3, *tile),
            vmem(4, *tile),
            vmem(7, *tile),
            vmem(16, *tile),
            dma((2, 3, 2)),
            dma((2, 3, 2)),
            dma((2, 2)),
            dma((2, 2)),
            dma((4, 4)),
            dma((4, 4)),
            dma((2, 3, 4)),
            dma((2, 3, 4)),
            dma((2, 3)),
            dma((2, 3)),
            dma((2, 3)),
            dma((2, 3)),
            dma((2, 3, 4)),
            dma((2, 3, 4)),
            dma((7,)),
            dma((7,)),
            dma((2, 2, 2)),
            dma((2,)),
            dma((8,)),
            dma((2,)),
            pltpu.SemaphoreType.REGULAR,
        ],
        compiler_params=pltpu.CompilerParams(collective_id=0, has_side_effects=True, vmem_limit_bytes=32 << 20),
        cost_estimate=pl.CostEstimate(flops=1000000000, bytes_accessed=1 << 20, transcendentals=0),
        name="finish",
    )(*(pltpu.with_memory_space_constraint(a, pltpu.MemorySpace.HBM) for a in (offs, live)), ext, probe, measured, tables, den, specimen)


def write_kernel(spec_ref, g_ref, spec_out, probe_out):
    spec_out[...] = spec_ref[...]
    for lb in range(2):
        for rb in range(32):
            for p in range(2):
                probe_out[p, rb * 8 : rb * 8 + 8, lb * 128 : lb * 128 + 128] = g_ref[lb * 32 + rb, p]


def write(specimen_next, probe_tiles):
    return pl.pallas_call(
        write_kernel,
        out_shape=(jax.ShapeDtypeStruct((2, 128, 256), f32), jax.ShapeDtypeStruct((2, 256, 256), f32)),
        in_specs=[VMEM] * 2,
        out_specs=(VMEM,) * 2,
        compiler_params=pltpu.CompilerParams(vmem_limit_bytes=8 << 20),
        name="write",
    )(specimen_next, probe_tiles)


def shards(specimen, probe_field, scan_offsets, live_counts, magnitudes):
    offs = scan_offsets.transpose(0, 2, 3, 1).reshape(ROWS * 4, COLS)
    tables, select = (jnp.asarray(a) for a in dft_tables())
    ext, den, probe, measured = halo(offs, live_counts, specimen, probe_field, magnitudes, select)
    return write(*finish(offs, live_counts, ext, probe, measured, tables, den, specimen))


def solution(mesh):
    return jax.shard_map(
        shards,
        mesh=mesh,
        in_specs=(P(None, "row", "col"), P(), P(), P(), P("row", "col", None, None, None)),
        out_specs=(P(None, "row", "col"), P()),
        check_vma=False,
    )
```

```python
import math

import jax
import jax.numpy as jnp
import numpy as np
from jax import lax
from jax.experimental import pallas as pl
from jax.experimental.pallas import tpu as pltpu
from jax.sharding import PartitionSpec as P

MESH = pl.DeviceIdType.MESH
ROWS = 16
COLS = 32
object_damping = 0.1
probe_damping = 0.1
f32 = jnp.float32
bf16 = jnp.bfloat16
VMEM = pl.BlockSpec(memory_space=pltpu.VMEM)
HBM = pl.BlockSpec(memory_space=pltpu.MemorySpace.HBM)
SMEM = pl.BlockSpec(memory_space=pltpu.SMEM)


def remote(src, dst, send, recv, where):
    return pltpu.make_async_remote_copy(src_ref=src, dst_ref=dst, send_sem=send, recv_sem=recv, device_id=where, device_id_type=MESH)


def greet(barrier, where):
    pl.semaphore_signal(barrier, inc=1, device_id=where, device_id_type=MESH)

STEP = 64


def split(value):
    high = value.astype(bf16)
    return high, (value - high.astype(f32)).astype(bf16)


def halo_kernel(offs_hbm, live_hbm, tile_ref, probe_hbm, mags, select_hbm, pat, den, probe, measured, ext, select, padded, seen, offs, live, own, fetch, cs, cr, vs, vr):
    row = lax.axis_index("row")
    col = lax.axis_index("col")
    has = {"l": col > 0, "r": col < COLS - 1, "u": row > 0, "d": row < ROWS - 1}
    to = {"l": (row, col - 1), "r": (row, col + 1), "u": (row - 1, col), "d": (row + 1, col)}
    center = [pltpu.make_async_copy(tile_ref.at[:, :, pl.ds(j * 128, 128)], ext.at[:, 1 + j, pl.ds(128, 128), :], own.at[j]) for j in range(2)]
    for c in center:
        c.start()
    small = [pltpu.make_async_copy(a, b, fetch.at[i]) for i, (a, b) in enumerate(((offs_hbm, offs), (live_hbm, live), (probe_hbm, probe)))]
    for c in small:
        c.start()
    shown = [pltpu.make_async_copy(mags.at[0, 0, s, :, pl.ds(j * 128, 128)], seen.at[s, j], fetch.at[3 + 2 * s + j]) for s in range(2) for j in range(2)]
    shown.append(pltpu.make_async_copy(select_hbm, select, fetch.at[7]))
    barrier = pltpu.get_barrier_semaphore()
    for side in "lrud":

        @pl.when(has[side])
        def _():
            greet(barrier, to[side])

    expected = sum(has[side].astype(jnp.int32) for side in "lrud")

    @pl.when(row == 0)
    def _():
        ext[:, :, 0:128, :] = jnp.zeros((2, 4, 128, 128), f32)

    @pl.when(row == ROWS - 1)
    def _():
        ext[:, :, 256:384, :] = jnp.zeros((2, 4, 128, 128), f32)

    @pl.when(col == 0)
    def _():
        ext[:, 0] = jnp.zeros((2, 384, 128), f32)

    @pl.when(col == COLS - 1)
    def _():
        ext[:, 3] = jnp.zeros((2, 384, 128), f32)

    for c in center:
        c.wait()
    pl.semaphore_wait(barrier, expected)

    def across(p, side):
        mine, theirs = (1, 3) if side == "l" else (2, 0)
        i = 0 if side == "l" else 1
        return remote(ext.at[p, mine, pl.ds(128, 128)], ext.at[p, theirs, pl.ds(128, 128)], cs.at[p, i], cr.at[p, i], to[side])

    def up_down(p, side, part):
        at = (pl.ds(1, 2), 0, 3)[part]
        i, theirs = (0, 256) if side == "u" else (1, 0)
        return remote(ext.at[p, at, pl.ds(128, 128)], ext.at[p, at, pl.ds(theirs, 128)], vs.at[p, part, i], vr.at[p, part, i], to[side])

    for p in range(2):
        for side in "lr":

            @pl.when(has[side])
            def _():
                across(p, side).start()

    for p in range(2):
        for side in "ud":

            @pl.when(has[side])
            def _():
                up_down(p, side, 0).start()

    for c in shown:
        c.start()
    for c in small:
        c.wait()
    padded[...] = jnp.zeros_like(padded)
    peak = jnp.zeros((8, 128), f32)
    for i in range(0, 256, STEP):
        power = probe[0, i : i + STEP, :] * probe[0, i : i + STEP, :] + probe[1, i : i + STEP, :] * probe[1, i : i + STEP, :]
        for j in range(2):
            padded[2 + j, 128 + i : 128 + i + STEP, :] = power[:, j * 128 : j * 128 + 128]
        for a in range(0, STEP, 8):
            for b in range(0, 256, 128):
                peak = jnp.maximum(peak, power[a : a + 8, b : b + 128])
    den[...] = jnp.full((128, 256), object_damping, f32) * jnp.max(peak)

    def add(n, carry):
        da = n // 6 - 1
        db = (n // 2) % 3 - 1
        s = n % 2
        a = row + da
        b = col + db
        inside = (a >= 0) & (a < ROWS) & (b >= 0) & (b < COLS)
        a = jnp.clip(a, 0, ROWS - 1)
        b = jnp.clip(b, 0, COLS - 1)
        down = da * 128 + jnp.clip(offs[(a * 2 + s) * 2, b], -128, 0)
        across = db * 256 + offs[(a * 2 + s) * 2 + 1, b]
        on = (inside & (s < live[a, b]) & (across > -256) & (across < 256)).astype(f32)
        across = jnp.clip(across, -256, 255)
        turn = (across + 256) % 128
        block = 4 - (across + 256) // 128
        lane = lax.broadcasted_iota(jnp.int32, (STEP, 128), 1)
        for i in range(0, 128, STEP):
            rolled = [pltpu.roll(padded[block + j - 1, pl.ds(i + 128 - down, STEP), :], turn, 1) for j in range(3)]
            for j in range(2):
                den[i : i + STEP, j * 128 : j * 128 + 128] += on * jnp.where(lane >= turn, rolled[j + 1], rolled[j])

        return carry

    lax.fori_loop(0, 18, add, 0)
    for p in range(2):
        for side, part in (("l", 1), ("r", 2)):

            @pl.when(has[side])
            def _():
                across(p, "r" if side == "l" else "l").wait_recv()
                for way in "ud":

                    @pl.when(has[way])
                    def _():
                        up_down(p, way, part).start()

    for c in shown:
        c.wait()
    for s in range(2):
        for odd in range(2):
            for i in range(0, 128, STEP):
                mh, ml = split(jnp.concatenate([seen[s, j, pl.ds(odd + 2 * i, STEP, stride=2), :] for j in range(2)], 1))
                measured[s, odd, i : i + STEP, :] = jnp.dot(mh, select[...], preferred_element_type=f32) + jnp.dot(ml, select[...], preferred_element_type=f32)

    for p in range(2):
        for side in "lr":

            @pl.when(has[side])
            def _():
                across(p, side).wait_send()

        for way, back in (("u", "d"), ("d", "u")):
            for part, need in ((0, None), (1, "l"), (2, "r")):
                cond = has[way] if need is None else jnp.logical_and(has[way], has[need])

                @pl.when(cond)
                def _():
                    up_down(p, way, part).wait_send()
                    up_down(p, back, part).wait_recv()

    lane = lax.broadcasted_iota(jnp.int32, (STEP, 128), 1)
    for s in range(2):
        top = jnp.clip(offs[(row * 2 + s) * 2, col] + 128, 0, 128)
        left = jnp.clip(offs[(row * 2 + s) * 2 + 1, col] + 128, 0, 256)
        turn, block = left % 128, left // 128
        for i in range(0, 256, STEP):
            for p in range(2):
                rolled = [pltpu.roll(ext[p, jnp.minimum(block + j, 3), pl.ds(top + i, STEP), :], 128 - turn, 1) for j in range(3)]
                for j in range(2):
                    pat[s, p, i : i + STEP, j * 128 : j * 128 + 128] = jnp.where(lane < 128 - turn, rolled[j], rolled[j + 1])


def halo(offs, live, tile, probe, mags, select):
    dma = pltpu.SemaphoreType.DMA
    return pl.pallas_call(
        halo_kernel,
        out_shape=(jax.ShapeDtypeStruct((2, 2, 256, 256), f32), jax.ShapeDtypeStruct((128, 256), f32), jax.ShapeDtypeStruct((2, 256, 256), f32), jax.ShapeDtypeStruct((2, 2, 128, 256), f32)),
        in_specs=[HBM] * 6,
        out_specs=(VMEM,) * 4,
        scratch_shapes=[pltpu.VMEM((2, 4, 384, 128), f32), pltpu.VMEM((256, 256), bf16), pltpu.VMEM((6, 512, 128), f32), pltpu.VMEM((2, 2, 256, 128), f32), pltpu.SMEM((ROWS * 4, COLS), jnp.int32), pltpu.SMEM((ROWS, COLS), jnp.int32), dma((2,)), dma((8,)), dma((2, 2)), dma((2, 2)), dma((2, 3, 2)), dma((2, 3, 2))],
        compiler_params=pltpu.CompilerParams(collective_id=1, has_side_effects=True, vmem_limit_bytes=8 << 20),
        cost_estimate=pl.CostEstimate(flops=400000000, bytes_accessed=1 << 20, transcendentals=0),
        name="halo",
    )(*(pltpu.with_memory_space_constraint(a, pltpu.MemorySpace.HBM) for a in (offs, live, tile, probe, mags, select)))


def dft_tables():
    m = np.arange(128)[:, None]
    k = np.arange(128)[None, :]
    tables = []
    for odd in range(2):
        angle = ((m * (2 * k + odd)) % 256) * (2.0 * math.pi / 256)
        c, s = np.cos(angle) / 16, np.sin(angle) / 16
        full = np.block([[c, -s], [s, c]])
        for t in (full, full.T):
            high = t.astype(np.float32).astype(jnp.bfloat16)
            low = (t - high.astype(np.float64)).astype(np.float32).astype(jnp.bfloat16)
            tables += [high, low]
    order = np.concatenate([np.arange(0, 256, 2), np.arange(1, 256, 2)])
    select = (np.arange(256)[:, None] == order[None, :]).astype(jnp.bfloat16)
    return np.stack(tables).reshape(2, 2, 2, 256, 256), select


def product(a, b):
    def dot(u, v):
        return jnp.dot(u, v, preferred_element_type=f32)

    return dot(a[0], b[0]) + (dot(a[1], b[0]) + dot(a[0], b[1]))


def tile_work(small, offs, live, probe, measured, tables, upd, pieces, pat, wave, freq, zb, placed):
    row = lax.axis_index("row")
    col = lax.axis_index("col")
    lane = lax.broadcasted_iota(jnp.int32, (STEP, 128), 1)

    def table(odd, turned):
        return tables[odd, turned, 0], tables[odd, turned, 1]

    for s in range(2):
        for i in range(0, 256, STEP):
            got = [pat[s, p, i : i + STEP, :] for p in range(2)]
            pr, pi = probe[0, i : i + STEP, :], probe[1, i : i + STEP, :]
            wr = pr * got[0] - pi * got[1]
            wi = pr * got[1] + pi * got[0]
            for odd in range(2):
                if odd:
                    mixed = [w[:, :128] - w[:, 128:] for w in (wr, wi)]
                else:
                    mixed = [w[:, :128] + w[:, 128:] for w in (wr, wi)]
                high, low = split(jnp.concatenate(mixed, 1))
                zb[s, odd, 0, i : i + STEP, :] = high
                zb[s, odd, 1, i : i + STEP, :] = low
        for odd in range(2):
            out = product((zb[s, odd, 0], zb[s, odd, 1]), table(odd, 0))
            for p in range(2):
                wave[s, p, :, odd * 128 : odd * 128 + 128] = out[:, p * 128 : p * 128 + 128]
    for odd in range(2):
        for s in range(2):
            if odd:
                mixed = [wave[s, p, 0:128, :] - wave[s, p, 128:256, :] for p in range(2)]
            else:
                mixed = [wave[s, p, 0:128, :] + wave[s, p, 128:256, :] for p in range(2)]
            freq[s, odd] = product(table(odd, 1), split(jnp.concatenate(mixed, 0)))
    for c in small:
        c.wait()
    top = [jnp.clip(offs[(row * 2 + s) * 2, col] + 128, 0, 128) for s in range(2)]
    left = [jnp.clip(offs[(row * 2 + s) * 2 + 1, col] + 128, 0, 256) for s in range(2)]
    turn = [a % 128 for a in left]
    block = [a // 128 for a in left]
    alive = [(s < live[row, col]).astype(f32) for s in range(2)]
    for odd in range(2):
        for s in range(2):
            for i in range(0, 128, STEP):
                fr = freq[s, odd, i : i + STEP, :]
                fi = freq[s, odd, 128 + i : 128 + i + STEP, :]
                factor = measured[s, odd, i : i + STEP, :] * lax.rsqrt(jnp.maximum(fr * fr + fi * fi, 0.0625)) - 1.0
                factor = factor * alive[s]
                for p, value in ((0, fr * factor), (1, fi * factor)):
                    high, low = split(value)
                    zb[s, odd, 0, p * 128 + i : p * 128 + i + STEP, :] = high
                    zb[s, odd, 1, p * 128 + i : p * 128 + i + STEP, :] = low
    for odd in range(2):
        for s in range(2):
            freq[s, odd] = product(table(odd, 0), (zb[s, odd, 0], zb[s, odd, 1]))
    for s in range(2):
        for p in range(2):
            e = freq[s, 0, p * 128 : p * 128 + 128, :]
            o = freq[s, 1, p * 128 : p * 128 + 128, :]
            wave[s, p, 0:128, :] = e + o
            wave[s, p, 128:256, :] = e - o
    for s in range(2):
        for odd in range(2):
            for i in range(0, 256, STEP):
                high, low = split(jnp.concatenate([wave[s, p, i : i + STEP, odd * 128 : odd * 128 + 128] for p in range(2)], 1))
                zb[s, odd, 0, i : i + STEP, :] = high
                zb[s, odd, 1, i : i + STEP, :] = low
            freq[s, odd] = product((zb[s, odd, 0], zb[s, odd, 1]), table(odd, 1))
    for s in range(2):
        for i in range(0, 256, STEP):
            diff = []
            for p in range(2):
                e, o = (freq[s, odd, i : i + STEP, p * 128 : p * 128 + 128] for odd in range(2))
                diff.append(jnp.concatenate([e + o, e - o], 1))
            dr, di = diff
            pr, pi = probe[0, i : i + STEP, :], probe[1, i : i + STEP, :]
            ore, oim = pat[s, 0, i : i + STEP, :], pat[s, 1, i : i + STEP, :]
            for p, grad in ((0, pr * dr + pi * di), (1, pr * di - pi * dr)):
                first, second = (pltpu.roll(grad[:, j * 128 : j * 128 + 128], turn[s], 1) for j in range(2))
                moved = (jnp.where(lane >= turn[s], first, 0.0), jnp.where(lane >= turn[s], second, first), jnp.where(lane < turn[s], second, 0.0))
                for j in range(3):
                    placed[s, p, j, 128 + i : 128 + i + STEP, :] = moved[j]
            terms = (ore * dr + oim * di, ore * di - oim * dr, (ore * ore + oim * oim) * alive[s])
            for lb in range(2):
                for rb in range(STEP // 8):
                    t = lb * 32 + i // 8 + rb
                    for p in range(3):
                        value = terms[p][rb * 8 : rb * 8 + 8, lb * 128 : lb * 128 + 128]
                        pieces[t, p] = value if s == 0 else pieces[t, p] + value
    for k in range(4):
        here = [k - block[s] for s in range(2)]
        weight = [((a >= 0) & (a <= 2)).astype(f32) for a in here]
        here = [jnp.clip(a, 0, 2) for a in here]
        for p in range(2):
            for i in range(0, 384, STEP):
                got = [placed[s, p, here[s], pl.ds(128 + i - top[s], STEP), :] * weight[s] for s in range(2)]
                upd[p, k, i : i + STEP, :] = got[0] + got[1]


def finish_kernel(offs_hbm, live_hbm, pat, probe_ref, measured, tables, den_ref, spec_ref, spec_out, g, d_ref, u_ref, wave, freq, zb, placed, offs, live, fetch, fv, side, fc, rp, s0, r1, s1, r2, s2, r3, wp, rw, r3w, hs, hr, es, er, ps, pr, ss1, rs1, ss2, rs2, ss3, rs3, ss4, rs4, ws, wr, zs, zr, gs, gr, know):
    row = lax.axis_index("row")
    col = lax.axis_index("col")
    core = row % 2
    x = (row // 2) % 4
    y = (row // 8) * 2 + col % 2
    z = col // 2

    def device(core_of, x_of, y_of, z_of):
        return ((y_of // 2) * 8 + x_of * 2 + core_of, z_of * 2 + y_of % 2)

    def peer(axis, d):
        return device(core, jnp.where(axis == 0, (x + d) % 4, x), jnp.where(axis == 0, y, (y + d) % 4), z)

    partner = device(1 - core, x, y, z)
    place = (x, y)
    has = {"l": col > 0, "r": col < COLS - 1, "u": row > 0, "d": row < ROWS - 1}
    beside = {"l": (row, col - 1), "r": (row, col + 1), "u": (row - 1, col), "d": (row + 1, col)}

    small = [pltpu.make_async_copy(a, b, fetch.at[i]) for i, (a, b) in enumerate(((offs_hbm, offs), (live_hbm, live)))]
    for c in small:
        c.start()
    barrier = pltpu.get_barrier_semaphore()
    greet(barrier, partner)
    for axis in range(2):
        for d in range(1, 4):
            greet(barrier, peer(axis, d))

    def along(d):
        return device(core, x, y, (z + d) % 16)

    for d in range(1, 5):
        greet(barrier, along(d))
        greet(barrier, along(16 - d))

    for way in "lrud":

        @pl.when(has[way])
        def _():
            greet(barrier, beside[way])

    expected = 15 + sum(has[way].astype(jnp.int32) for way in "lrud")

    for i, way in enumerate("ud"):

        @pl.when(jnp.logical_not(has[way]))
        def _():
            fv[i] = jnp.zeros((2, 4, 128, 128), f32)

    for i, way in enumerate("lr"):

        @pl.when(jnp.logical_not(has[way]))
        def _():
            fc[i] = jnp.zeros((2, 128, 128), f32)

    placed[:, :, :, 0:128, :] = jnp.zeros((2, 2, 3, 128, 128), f32)
    placed[:, :, :, 384:512, :] = jnp.zeros((2, 2, 3, 128, 128), f32)
    tile_work(small, offs, live, probe_ref, measured, tables, u_ref, d_ref, pat, wave, freq, zb, placed)
    total = d_ref[0, 2]
    for t in range(1, 64):
        total = total + d_ref[t, 2]
    wp[0] = total
    pl.semaphore_wait(barrier, expected)
    for d in (4, 12):
        pl.semaphore_signal(know, inc=1, device_id=along(d), device_id_type=MESH)

    def vertical(p, part, way, inward=False):
        at = (0, 3, pl.ds(1, 2))[part]
        i = 0 if way == "u" else 1
        there = i if inward else 1 - i
        return remote(u_ref.at[p, at, pl.ds(256 * i, 128)], fv.at[there, p, at], hs.at[p, part, i], hr.at[p, part, there], beside[way])

    def lateral(p, way, inward=False):
        i = 0 if way == "l" else 1
        there = i if inward else 1 - i
        return remote(side.at[i, p], fc.at[there, p], es.at[p, i], er.at[p, there], beside[way])

    base = core * 32
    pending = []

    def go(c):
        c.start()
        pending.append(c)
        return c

    def spot(color, d):
        return color * 16 + ((place[color] + d) % 4) * 4

    near = (2, 1, 3)
    pairs = {}
    for d in near + (0,):
        for color in range(2):
            at = spot(color, d)
            pairs[color, d] = go(remote(d_ref.at[pl.ds((1 - core) * 32 + at, 4)], rp.at[pl.ds(at, 4)], ps.at[color, d], pr.at[color, d], partner))
        if d == 2:
            first = go(remote(wp.at[0], rw.at[0], ws.at[0], wr.at[0], partner))


    def join(color, d):
        pairs[color, d].wait_recv()
        at = spot(color, d)
        for b in range(4):
            s0[at + b] = d_ref[base + at + b] + rp[at + b]

    for d in near:
        for color in range(2):
            join(color, d)
    one = {}
    for e in near + (0,):
        for d in near:
            for color in range(2):
                b = (place[1 - color] + e) % 4
                one[color, d, e] = go(remote(s0.at[spot(color, d) + b], r1.at[color, d - 1, e], ss1.at[color, d - 1, e], rs1.at[color, d - 1, e], peer(color, d)))
        if e == 2:
            first.wait_recv()
            wp[1] = wp[0] + rw[0]
            waves = [go(remote(wp.at[1], rw.at[d], ws.at[d], wr.at[d], peer(0, d))) for d in range(1, 4)]
    for color in range(2):
        join(color, 0)
    two = {}
    for e in near + (0,):
        for color in range(2):
            b = (place[1 - color] + e) % 4
            for d in near:
                one[color, d, e].wait_recv()
            s1[color, e] = s0[spot(color, 0) + b] + (r1[color, 0, e] + (r1[color, 1, e] + r1[color, 2, e]))
            if e:
                two[color, e] = go(remote(s1.at[color, e], r2.at[color, e - 1], ss2.at[color, e - 1], rs2.at[color, e - 1], peer(1 - color, e)))
        if e == 2:
            for c in waves:
                c.wait_recv()
            wp[2] = wp[1] + (rw[1] + (rw[2] + rw[3]))
            waves = [go(remote(wp.at[2], rw.at[3 + d], ws.at[3 + d], wr.at[3 + d], peer(1, d))) for d in range(1, 4)]
    for part in range(3):
        for p in range(2):
            for way in "ud":

                @pl.when(has[way])
                def _():
                    vertical(p, part, way).start()

    for c in waves:
        c.wait_recv()
    wp[3] = wp[2] + (rw[4] + (rw[5] + rw[6]))
    pl.semaphore_wait(know, 2)

    def root(color):
        return 4 * color + 2 * core

    def slot(color):
        return base + color * 16 + jnp.where(color == 0, x * 4 + y, y * 4 + x)

    for color in range(2):
        for e in near:
            two[color, e].wait_recv()
        s2[color] = s1[color, 0] + (r2[color, 0] + (r2[color, 1] + r2[color, 2]))
        for n in range(2):
            goal = root(color) + 8 * n

            @pl.when(z != goal)
            def _():
                remote(s2.at[color], r3.at[z], zs.at[color, n, 0], zr.at[0], device(core, x, y, goal)).start()
                remote(wp.at[3], r3w.at[z], zs.at[color, n, 1], zr.at[1], device(core, x, y, goal)).start()

    for color in range(2):

        @pl.when(z % 8 == root(color))
        def _():
            r3[z] = s2[color]
            r3w[z] = wp[3]
            pltpu.make_async_copy(r3.at[pl.ds(0, 15)], r3.at[pl.ds(0, 15)], zr.at[0]).wait()
            pltpu.make_async_copy(r3w.at[pl.ds(0, 15)], r3w.at[pl.ds(0, 15)], zr.at[1]).wait()
            full = r3[0]
            weight = r3w[0]
            for i in range(1, 16):
                full = full + r3[i]
                weight = weight + r3w[i]
            mean = jnp.sum(weight) * (1.0 / 65536.0)
            scale = full[2] + probe_damping * mean
            t = slot(color)
            rows = pl.ds(pl.multiple_of((t % 32) * 8, 8), 8)
            lanes = pl.ds(pl.multiple_of((t // 32) * 128, 128), 128)
            for p in range(2):
                g[t, p] = probe_ref[p, rows, lanes] + full[p] / scale
            for i in (4, 3, 13, 2, 14, 1, 15):
                remote(g.at[t], g.at[t], gs.at[i % 8], gr.at[color], along(i)).start()

    for i, (way, at) in enumerate((("l", 0), ("r", 3))):
        for p in range(2):
            for up_down in "ud":

                @pl.when(has[up_down])
                def _():
                    vertical(p, i, up_down, True).wait_recv()

            @pl.when(has[way])
            def _():
                side[i, p] = u_ref[p, at, 128:256, :] + (fv[0, p, at] + fv[1, p, at])
                lateral(p, way).start()

    def away(color):
        d = (z - root(color) + 16) % 8
        return jnp.minimum(d, 8 - d)

    nearer = (away(1) < away(0)).astype(jnp.int32)
    colors = (nearer, 1 - nearer)

    def own(color):
        return jnp.where(color == 0, x, y)

    def cross(color):
        return jnp.where(color == 0, y, x)

    def tile_at(color, a, b):
        return base + color * 16 + (a % 4) * 4 + b % 4

    three = {}
    four = {}
    for n, color in enumerate(colors):
        t = slot(color)

        @pl.when(z % 8 != root(color))
        def _():
            pltpu.make_async_copy(g.at[t], g.at[t], gr.at[color]).wait()

        for d in near:
            three[n, d] = go(remote(g.at[t], g.at[t], ss3.at[color, d - 1], rs3.at[color, d - 1], peer(1 - color, d)))
        for d in near:
            four[n, d, 0] = go(remote(g.at[t], g.at[t], ss4.at[color, d - 1, 0], rs4.at[color, d - 1, 0], peer(color, d)))
    last = []
    for n, color in enumerate(colors):
        for e in (1, 3, 2):
            three[n, e].wait_recv()
            t = tile_at(color, own(color), cross(color) - e + 4)
            for d in near:
                four[n, d, e] = go(remote(g.at[t], g.at[t], ss4.at[color, d - 1, e], rs4.at[color, d - 1, e], peer(color, d)))
        group = g.at[pl.ds(tile_at(color, own(color), 0), 4)]
        last.append(go(remote(group, group, ps.at[2 + n, 0], pr.at[2 + n, 0], partner)))
    for n, color in enumerate(colors):
        for d in (1, 3, 2):
            for e in range(4):
                four[n, d, e].wait_recv()
            group = g.at[pl.ds(tile_at(color, own(color) - d + 4, 0), 4)]
            last.append(go(remote(group, group, ps.at[2 + n, d], pr.at[2 + n, d], partner)))
    for p in range(2):
        for way in "ud":

            @pl.when(has[way])
            def _():
                vertical(p, 2, way, True).wait_recv()

        for way in "lr":

            @pl.when(has[way])
            def _():
                lateral(p, way, True).wait_recv()

        for i in range(2):
            at = 1 + i
            update = u_ref[p, at, 128:256, :] + (fv[0, p, at] + fv[1, p, at]) + fc[i, p]
            lanes = slice(i * 128, i * 128 + 128)
            spec_out[p, :, lanes] = spec_ref[p, :, lanes] + update / den_ref[:, lanes]
    for c in last:
        c.wait_recv()
    for c in pending:
        c.wait_send()
    for p in range(2):
        for way in "ud":

            @pl.when(has[way])
            def _():
                for part in range(3):
                    vertical(p, part, way).wait_send()

        for way in "lr":

            @pl.when(has[way])
            def _():
                lateral(p, way).wait_send()

    for color in range(2):

        for n in range(2):

            @pl.when(z != root(color) + 8 * n)
            def _():
                pltpu.make_async_copy(s2.at[color], s2.at[color], zs.at[color, n, 0]).wait()
                pltpu.make_async_copy(wp.at[3], wp.at[3], zs.at[color, n, 1]).wait()

        @pl.when(z % 8 == root(color))
        def _():
            t = slot(color)
            for i in (4, 3, 5, 2, 6, 1, 7):
                pltpu.make_async_copy(g.at[t], g.at[t], gs.at[i]).wait()


def finish(offs, live, pat, probe, measured, tables, den, specimen):
    tile = (8, 128)
    dma = pltpu.SemaphoreType.DMA

    def vmem(*shape):
        return pltpu.VMEM(shape, f32)

    return pl.pallas_call(
        finish_kernel,
        out_shape=(jax.ShapeDtypeStruct((2, 128, 256), f32), jax.ShapeDtypeStruct((64, 2, 8, 128), f32)),
        in_specs=[HBM] * 2 + [VMEM] * 6,
        out_specs=(VMEM,) * 2,
        scratch_shapes=[
            vmem(64, 3, *tile),
            vmem(2, 4, 384, 128),
            vmem(2, 2, 256, 256),
            vmem(2, 2, 256, 256),
            pltpu.VMEM((2, 2, 2, 256, 256), bf16),
            vmem(2, 2, 3, 512, 128),
            pltpu.SMEM((ROWS * 4, COLS), jnp.int32),
            pltpu.SMEM((ROWS, COLS), jnp.int32),
            dma((2,)),
            vmem(2, 2, 4, 128, 128),
            vmem(2, 2, 128, 128),
            vmem(2, 2, 128, 128),
            vmem(32, 3, *tile),
            vmem(32, 3, *tile),
            vmem(2, 3, 4, 3, *tile),
            vmem(2, 4, 3, *tile),
            vmem(2, 3, 3, *tile),
            vmem(2, 3, *tile),
            vmem(16, 3, *tile),
            vmem(4, *tile),
            vmem(7, *tile),
            vmem(16, *tile),
            dma((2, 3, 2)),
            dma((2, 3, 2)),
            dma((2, 2)),
            dma((2, 2)),
            dma((4, 4)),
            dma((4, 4)),
            dma((2, 3, 4)),
            dma((2, 3, 4)),
            dma((2, 3)),
            dma((2, 3)),
            dma((2, 3)),
            dma((2, 3)),
            dma((2, 3, 4)),
            dma((2, 3, 4)),
            dma((7,)),
            dma((7,)),
            dma((2, 2, 2)),
            dma((2,)),
            dma((8,)),
            dma((2,)),
            pltpu.SemaphoreType.REGULAR,
        ],
        compiler_params=pltpu.CompilerParams(collective_id=0, has_side_effects=True, vmem_limit_bytes=32 << 20),
        cost_estimate=pl.CostEstimate(flops=1000000000, bytes_accessed=1 << 20, transcendentals=0),
        name="finish",
    )(*(pltpu.with_memory_space_constraint(a, pltpu.MemorySpace.HBM) for a in (offs, live)), pat, probe, measured, tables, den, specimen)


def write_kernel(spec_ref, g_ref, spec_out, probe_out):
    spec_out[...] = spec_ref[...]
    for lb in range(2):
        for rb in range(32):
            for p in range(2):
                probe_out[p, rb * 8 : rb * 8 + 8, lb * 128 : lb * 128 + 128] = g_ref[lb * 32 + rb, p]


def write(specimen_next, probe_tiles):
    return pl.pallas_call(
        write_kernel,
        out_shape=(jax.ShapeDtypeStruct((2, 128, 256), f32), jax.ShapeDtypeStruct((2, 256, 256), f32)),
        in_specs=[VMEM] * 2,
        out_specs=(VMEM,) * 2,
        compiler_params=pltpu.CompilerParams(vmem_limit_bytes=8 << 20),
        name="write",
    )(specimen_next, probe_tiles)


def shards(specimen, probe_field, scan_offsets, live_counts, magnitudes):
    offs = scan_offsets.transpose(0, 2, 3, 1).reshape(ROWS * 4, COLS)
    tables, select = (jnp.asarray(a) for a in dft_tables())
    pat, den, probe, measured = halo(offs, live_counts, specimen, probe_field, magnitudes, select)
    return write(*finish(offs, live_counts, pat, probe, measured, tables, den, specimen))


def solution(mesh):
    return jax.shard_map(
        shards,
        mesh=mesh,
        in_specs=(P(None, "row", "col"), P(), P(), P(), P("row", "col", None, None, None)),
        out_specs=(P(None, "row", "col"), P()),
        check_vma=False,
    )
```
